32 devices in a mesh: hp: 4 (over z), cp: 8 (over y, x, core).
Axes of the slice: x: 2, y: 2, z: 4, core: 2. Of those that a mesh axis runs over, the one named last changes fastest.
Arguments:
- hidden: bfloat16 [4096, 3072], P(('cp', 'hp'))
- grad_out: bfloat16 [4096, 3072], P(('cp', 'hp'))
- positions: int32 [4096], P(('cp', 'hp'))
- norm_gain: bfloat16 [3072], replicated
- w_q: bfloat16 [3072, 3072], replicated
- w_k: bfloat16 [3072, 1024], replicated
- w_v: bfloat16 [3072, 1024], replicated
- w_o: bfloat16 [3072, 3072], replicated
- inv_freq: float32 [64], replicated
Outputs:
- output 1: bfloat16 [4096, 3072], P(('cp', 'hp'))
- output 2: bfloat16 [4096, 3072], P(('cp', 'hp'))
- output 3: float32 [3072, 3072], replicated
- output 4: float32 [3072, 1024], replicated
- output 5: float32 [3072, 1024], replicated
- output 6: float32 [3072, 3072], replicated
- output 7: float32 [3072], replicated
All inputs are finite; a program needn't handle non-finite values.
Results may differ from the reference program's by a relative error of at most 0.0123283.
Values are sent between devices in bfloat16 or wider.
A program may use at most 1 GiB of HBM per device.

```python
import math
import jax
import jax.numpy as jnp
from jax import lax

D_MODEL = 3072
Q_HEADS = 24
KV_HEADS = 8
HEAD_DIM = 128
TOKENS_DEV = 128
CP_SIZE = 8
HP_SIZE = 4

SEQ_LEN = TOKENS_DEV * CP_SIZE * HP_SIZE
NORM_EPS = 1e-5


def true_index():
    block_len = SEQ_LEN // (2 * CP_SIZE)
    rows_idx = jnp.arange(SEQ_LEN, dtype=jnp.int32)
    pair_id = rows_idx // (2 * block_len)
    within = rows_idx % (2 * block_len)
    return jnp.where(within < block_len, pair_id * block_len + within, (2 * CP_SIZE - 1 - pair_id) * block_len + within - block_len)


def draw_positions(key):
    doc_starts = jax.random.randint(key, (8,), 1, SEQ_LEN)
    seq_idx = jnp.arange(SEQ_LEN, dtype=jnp.int32)
    start_flags = jnp.zeros((SEQ_LEN,), jnp.int32).at[doc_starts].set(1)
    start_marks = jnp.where(start_flags > 0, seq_idx, 0)
    return (seq_idx - lax.cummax(start_marks, axis=0))[true_index()]


def setup_inputs(seed: int = 0) -> dict:
    key_list = jax.random.split(jax.random.key(seed), 10)
    half_dim = HEAD_DIM // 2
    in_scale = D_MODEL ** -0.5
    hidden = jax.random.normal(key_list[0], (SEQ_LEN, D_MODEL), jnp.float32).astype(jnp.bfloat16)
    grad_out = jax.random.normal(key_list[1], (SEQ_LEN, D_MODEL), jnp.float32).astype(jnp.bfloat16)
    positions = draw_positions(key_list[2])
    norm_gain = (1.0 + 0.3 * jax.random.normal(key_list[3], (D_MODEL,), jnp.float32)).astype(jnp.bfloat16)
    w_q = (jax.random.normal(key_list[4], (D_MODEL, Q_HEADS * HEAD_DIM), jnp.float32) * in_scale).astype(jnp.bfloat16)
    w_k = (jax.random.normal(key_list[5], (D_MODEL, KV_HEADS * HEAD_DIM), jnp.float32) * in_scale).astype(jnp.bfloat16)
    w_v = (jax.random.normal(key_list[6], (D_MODEL, KV_HEADS * HEAD_DIM), jnp.float32) * in_scale).astype(jnp.bfloat16)
    w_o = (jax.random.normal(key_list[7], (Q_HEADS * HEAD_DIM, D_MODEL), jnp.float32) * (Q_HEADS * HEAD_DIM) ** -0.5).astype(jnp.bfloat16)
    rope_base = jnp.exp(jax.random.uniform(key_list[8], (), jnp.float32, math.log(1.0e4), math.log(5.0e5)))
    jitter = jax.random.uniform(key_list[9], (half_dim,), jnp.float32, 0.7, 1.3)
    inv_freq = rope_base ** (-jnp.arange(half_dim, dtype=jnp.float32) / half_dim) * jitter
    return dict(hidden=hidden, grad_out=grad_out, positions=positions, norm_gain=norm_gain, w_q=w_q, w_k=w_k, w_v=w_v, w_o=w_o, inv_freq=inv_freq)


def rope_apply(vectors, cos_t, sin_t):
    half_dim = vectors.shape[-1] // 2
    lo_half = vectors[..., :half_dim]
    hi_half = vectors[..., half_dim:]
    return jnp.concatenate([lo_half * cos_t - hi_half * sin_t, hi_half * cos_t + lo_half * sin_t], axis=-1)


def rope_undo(vectors, cos_t, sin_t):
    half_dim = vectors.shape[-1] // 2
    lo_half = vectors[..., :half_dim]
    hi_half = vectors[..., half_dim:]
    return jnp.concatenate([lo_half * cos_t + hi_half * sin_t, hi_half * cos_t - lo_half * sin_t], axis=-1)


def reference(hidden, grad_out, positions, norm_gain, w_q, w_k, w_v, w_o, inv_freq):
    group_size = Q_HEADS // KV_HEADS
    score_scale = HEAD_DIM ** -0.5
    q_block = min(TOKENS_DEV, 64)
    n_blocks = SEQ_LEN // q_block
    x_f32 = hidden.astype(jnp.float32)
    inv_rms = lax.rsqrt(jnp.mean(x_f32 * x_f32, axis=-1, keepdims=True) + NORM_EPS)
    x_hat = x_f32 * inv_rms
    normed = (x_hat * norm_gain.astype(jnp.float32)).astype(jnp.bfloat16)
    angles = positions.astype(jnp.float32)[:, None] * inv_freq[None, :]
    cos_t = jnp.cos(angles)[:, None, :]
    sin_t = jnp.sin(angles)[:, None, :]
    q_rot = rope_apply(jnp.dot(normed, w_q, preferred_element_type=jnp.float32).reshape(SEQ_LEN, Q_HEADS, HEAD_DIM), cos_t, sin_t).astype(jnp.bfloat16)
    k_rot = rope_apply(jnp.dot(normed, w_k, preferred_element_type=jnp.float32).reshape(SEQ_LEN, KV_HEADS, HEAD_DIM), cos_t, sin_t).astype(jnp.bfloat16)
    v_val = jnp.dot(normed, w_v, preferred_element_type=jnp.float32).astype(jnp.bfloat16).reshape(SEQ_LEN, KV_HEADS, HEAD_DIM)
    d_out = jnp.dot(grad_out, w_o.T, preferred_element_type=jnp.float32).astype(jnp.bfloat16)
    seq_idx = true_index()
    k_f32 = k_rot.astype(jnp.float32)
    v_f32 = v_val.astype(jnp.float32)
    q_blocks = q_rot.reshape(n_blocks, q_block, KV_HEADS, group_size, HEAD_DIM)
    do_blocks = d_out.reshape(n_blocks, q_block, KV_HEADS, group_size, HEAD_DIM)
    idx_blocks = seq_idx.reshape(n_blocks, q_block)

    def block_step(acc_pair, block_in):
        dk_acc, dv_acc = acc_pair
        q_part, do_part, idx_part = block_in
        q_f32 = q_part.astype(jnp.float32)
        do_f32 = do_part.astype(jnp.float32)
        scores = jnp.einsum('qkgd,tkd->kgqt', q_f32, k_f32) * score_scale
        visible = idx_part[:, None] >= seq_idx[None, :]
        scores = jnp.where(visible, scores, -1e30)
        prob_f32 = jnp.exp(scores - jnp.max(scores, axis=-1, keepdims=True))
        prob_f32 = prob_f32 / jnp.sum(prob_f32, axis=-1, keepdims=True)
        prob_b16 = prob_f32.astype(jnp.bfloat16).astype(jnp.float32)
        out_part = jnp.einsum('kgqt,tkd->qkgd', prob_b16, v_f32).astype(jnp.bfloat16)
        row_delta = jnp.einsum('qkgd,qkgd->kgq', do_f32, out_part.astype(jnp.float32))
        d_prob = jnp.einsum('qkgd,tkd->kgqt', do_f32, v_f32)
        d_score = (prob_f32 * (d_prob - row_delta[..., None])).astype(jnp.bfloat16).astype(jnp.float32)
        dq_part = (jnp.einsum('kgqt,tkd->qkgd', d_score, k_f32) * score_scale).astype(jnp.bfloat16)
        dk_acc = dk_acc + jnp.einsum('kgqt,qkgd->tkd', d_score, q_f32) * score_scale
        dv_acc = dv_acc + jnp.einsum('kgqt,qkgd->tkd', prob_b16, do_f32)
        return (dk_acc, dv_acc), (out_part, dq_part)

    zeros_kv = jnp.zeros((SEQ_LEN, KV_HEADS, HEAD_DIM), jnp.float32)
    (dk_sum, dv_sum), (out_blocks, dq_blocks) = lax.scan(block_step, (zeros_kv, zeros_kv), (q_blocks, do_blocks, idx_blocks))
    attn_out = out_blocks.reshape(SEQ_LEN, Q_HEADS * HEAD_DIM)
    output = (x_f32 + jnp.dot(attn_out, w_o, preferred_element_type=jnp.float32)).astype(jnp.bfloat16)
    grad_wo = jnp.dot(attn_out.T, grad_out, preferred_element_type=jnp.float32)
    g_q = rope_undo(dq_blocks.reshape(SEQ_LEN, Q_HEADS, HEAD_DIM).astype(jnp.float32), cos_t, sin_t).astype(jnp.bfloat16).reshape(SEQ_LEN, Q_HEADS * HEAD_DIM)
    g_k = rope_undo(dk_sum.astype(jnp.bfloat16).astype(jnp.float32), cos_t, sin_t).astype(jnp.bfloat16).reshape(SEQ_LEN, KV_HEADS * HEAD_DIM)
    g_v = dv_sum.astype(jnp.bfloat16).reshape(SEQ_LEN, KV_HEADS * HEAD_DIM)
    grad_wq = jnp.dot(normed.T, g_q, preferred_element_type=jnp.float32)
    grad_wk = jnp.dot(normed.T, g_k, preferred_element_type=jnp.float32)
    grad_wv = jnp.dot(normed.T, g_v, preferred_element_type=jnp.float32)
    d_norm = jnp.dot(g_q, w_q.T, preferred_element_type=jnp.float32) + jnp.dot(g_k, w_k.T, preferred_element_type=jnp.float32) + jnp.dot(g_v, w_v.T, preferred_element_type=jnp.float32)
    grad_gain = jnp.sum(d_norm * x_hat, axis=0)
    d_hat = d_norm * norm_gain.astype(jnp.float32)
    grad_hidden = (grad_out.astype(jnp.float32) + inv_rms * (d_hat - x_hat * jnp.mean(d_hat * x_hat, axis=-1, keepdims=True))).astype(jnp.bfloat16)
    return (output, grad_hidden, grad_wq, grad_wk, grad_wv, grad_wo, grad_gain)
```

```python
import functools
import jax
import jax.numpy as jnp
from jax import lax
from jax.experimental import pallas as pl
from jax.experimental.pallas import tpu as pltpu
from jax.sharding import PartitionSpec as P

NORM_EPS = 1e-5
F32 = jnp.float32
BF16 = jnp.bfloat16
LANES = 128
BLK = 512
HALF = BLK // 2
SEQ = 8 * BLK
QROWS = 2 * BLK
UPP = 8
LAG = 3
VMEM_LIMIT = 60 * 2**20
NT = (((1,), (1,)), ((), ()))
TN = (((0,), (0,)), ((), ()))

STAGES = {
    'C': ('z1', 'z2', 'z3', 'y', 'x', 'd'),
    'D': ('z1', 'z2', 'z3', 'x', 'y', 'd'),
    'E': ('x', 'y', 'z1', 'z2', 'z3', 'd'),
    'F': ('y', 'x', 'z1', 'z2', 'z3', 'd'),
}
SLOT = {'z1': 0, 'z2': 2, 'z3': 4, 'x': 6, 'y': 7, 'd': 8}
N_STAGE = 6
N_SLOT = 9


def rope_apply(vectors, cos_t, sin_t):
    half_dim = vectors.shape[-1] // 2
    lo_half = vectors[..., :half_dim]
    hi_half = vectors[..., half_dim:]
    return jnp.concatenate([lo_half * cos_t - hi_half * sin_t, hi_half * cos_t + lo_half * sin_t], axis=-1)


def rope_undo(vectors, cos_t, sin_t):
    half_dim = vectors.shape[-1] // 2
    lo_half = vectors[..., :half_dim]
    hi_half = vectors[..., half_dim:]
    return jnp.concatenate([lo_half * cos_t + hi_half * sin_t, hi_half * cos_t - lo_half * sin_t], axis=-1)


class Gather:
    def __init__(self, send_sem, recv_sem):
        self.z = lax.axis_index('hp')
        cp = lax.axis_index('cp')
        self.c, self.x, self.y = lax.rem(cp, 2), lax.rem(lax.div(cp, 2), 2), lax.div(cp, 4)
        self.send_sem, self.recv_sem = send_sem, recv_sem

    def device(self, c=None, x=None, y=None, z=None):
        c = self.c if c is None else c
        x = self.x if x is None else x
        y = self.y if y is None else y
        z = self.z if z is None else z
        return (z, y * 4 + x * 2 + c)

    def copies(self, sem_row, kind, view, stage):
        c, x, y, z = self.c, self.x, self.y, self.z
        order = STAGES[kind]
        done = {st[0] for st in order[:order.index(stage)]}
        every = slice(None)
        gx, gy, gz = (every if d in done else v for d, v in (('x', x), ('y', y), ('z', z)))
        slot = SLOT[stage]

        def copy(place, device, slot):
            return lambda: pltpu.make_async_remote_copy(
                place, place, self.send_sem.at[sem_row, slot], self.recv_sem.at[sem_row, slot],
                device_id=device, device_id_type=pl.DeviceIdType.MESH)

        if stage == 'x':
            dev = self.device(x=1 - x)
            return [(None, copy(view(c, x, gy, gz), dev, slot), None, copy(view(c, 1 - x, gy, gz), dev, slot))]
        if stage == 'y':
            dev = self.device(y=1 - y)
            return [(None, copy(view(c, gx, y, gz), dev, slot), None, copy(view(c, gx, 1 - y, gz), dev, slot))]
        if stage == 'd':
            dev = self.device(c=1 - c)
            return [(None, copy(view(c, every, every, every), dev, slot),
                     None, copy(view(1 - c, every, every, every), dev, slot))]
        hop = int(stage[1])
        up, down = self.device(z=jnp.minimum(z + 1, 3)), self.device(z=jnp.maximum(z - 1, 0))
        return [
            ((z >= hop - 1) & (z < 3), copy(view(c, gx, gy, jnp.maximum(z - hop + 1, 0)), up, slot),
             z >= hop, copy(view(c, gx, gy, jnp.maximum(z - hop, 0)), up, slot)),
            ((z + hop <= 4) & (z > 0), copy(view(c, gx, gy, jnp.minimum(z + hop - 1, 3)), down, slot + 1),
             z + hop <= 3, copy(view(c, gx, gy, jnp.minimum(z + hop, 3)), down, slot + 1)),
        ]

    def run(self, sem_row, kind, view, stage, what):
        for can_send, send, can_recv, recv in self.copies(sem_row, kind, view, stage):
            cond = can_recv if what == 'recv' else can_send

            def act(send=send, recv=recv):
                if what == 'start':
                    send().start()
                elif what == 'sent':
                    send().wait_send()
                else:
                    recv().wait_recv()

            if cond is None:
                act()
            else:
                pl.when(cond)(act)

    def advance(self, sem_row, kind, view, s):
        if s > 0:
            self.run(sem_row, kind, view, STAGES[kind][s - 1], 'recv')
        if s < N_STAGE:
            self.run(sem_row, kind, view, STAGES[kind][s], 'start')

    def kinds(self, u):
        w = lax.rem(u, 8)
        m = lax.rem(w, 3)
        return (('C', m == 0), ('D', m == 1), ('E', w == 2), ('F', w == 5))

    def tick(self, t, n_units, view):
        for s in range(N_STAGE + 1):
            u = t - s * LAG
            uc = jnp.clip(u, 0, n_units - 1)
            for kind, is_kind in self.kinds(uc):
                @pl.when((u >= 0) & (u < n_units) & is_kind)
                def _(kind=kind, s=s, uc=uc):
                    self.advance(uc, kind, view(uc), s)

    def drain(self, n_units, view):
        def body(u, carry):
            for kind, is_kind in self.kinds(u):
                @pl.when(is_kind)
                def _(kind=kind):
                    for stage in STAGES[kind]:
                        self.run(u, kind, view(u), stage, 'sent')
            return carry
        lax.fori_loop(0, n_units, body, 0)


def n_ticks(n_units):
    return n_units + N_STAGE * LAG


def turn(v):
    return pltpu.roll(v, LANES // 2, 1)


def cos_sin(cs):
    low = lax.broadcasted_iota(jnp.int32, cs.shape, 1) < LANES // 2
    other = turn(cs)
    return jnp.where(low, cs, other), jnp.where(low, -other, cs)


def gather_in_kernel(h_ref, dy_ref, cs_ref, wq_ref, wk_ref, wv_ref, wo_ref,
                     hd_ref, csg_ref, q_ref, k_ref, v_ref, do_ref,
                     rows_buf, cs_buf, wq_buf, wkv_buf, wo_buf, send_sem, recv_sem, csend, crecv, lsem, wsem, rsem, tsem):
    net = Gather(send_sem, recv_sem)
    small = Gather(csend, crecv)
    own = (net.y, net.x, net.c, net.z)
    head, quarter = net.c * 4 + net.z, net.y * 2 + net.x
    mine = [pltpu.make_async_copy(src, dst, lsem.at[i]) for i, (src, dst) in enumerate((
        (h_ref, hd_ref.at[(0, *own)]), (cs_ref, csg_ref.at[own]), (dy_ref, hd_ref.at[(1, *own)])))]
    for m in mine:
        m.start()
    q_cols = pl.ds(pl.multiple_of(head * 3 * LANES, LANES), 3 * LANES)
    kv_cols = pl.ds(pl.multiple_of(head * LANES, LANES), LANES)
    weights = [pltpu.make_async_copy(src, dst, wsem.at[i]) for i, (src, dst) in enumerate((
        (wq_ref.at[:, q_cols], wq_buf), (wk_ref.at[:, kv_cols], wkv_buf.at[:, :LANES]),
        (wv_ref.at[:, kv_cols], wkv_buf.at[:, LANES:]), (wo_ref.at[q_cols, :], wo_buf)))]
    for w in weights:
        w.start()
    for m in mine:
        m.wait()

    def view(u):
        rows = pl.ds(pl.multiple_of(lax.rem(u, 8) * 16, 16), 16)
        which = lax.div(u, 8)
        return lambda c, x, y, z: hd_ref.at[which, y, x, c, z, rows, :]

    def cs_view(c, x, y, z):
        return csg_ref.at[y, x, c, z]

    def blocks(which, pair):
        slot = lax.rem(pair, 2)
        y, x, c = lax.div(pair, 4), lax.rem(lax.div(pair, 2), 2), slot
        out = []
        for z in range(4):
            rows = pl.ds(z * LANES, LANES)
            out.append(pltpu.make_async_copy(hd_ref.at[which, y, x, c, z], rows_buf.at[slot, rows], rsem.at[slot, z]))
            if which == 0:
                out.append(pltpu.make_async_copy(csg_ref.at[y, x, c, z], cs_buf.at[slot, rows], tsem.at[slot, z]))
        return out

    def low(pair):
        return pl.ds(pl.multiple_of(pair * HALF, HALF), HALF)

    def to_queries(dst, value, side):
        for j in range(3):
            cols = slice(j * LANES, (j + 1) * LANES)
            dst[j, low(side), :] = value[:HALF, cols].astype(BF16)
            dst[j, low(3 - side), :] = value[HALF:, cols].astype(BF16)

    def project(pair):
        slot = lax.rem(pair, 2)
        for c in blocks(0, pair):
            c.wait()

        @pl.when(pair < 7)
        def _():
            for c in blocks(0, pair + 1):
                c.start()
        cos, sin = cos_sin(cs_buf[slot])
        kv = jnp.dot(rows_buf[slot], wkv_buf[...], preferred_element_type=F32)
        key = kv[:, :LANES]
        key = (key * cos + turn(key) * sin).astype(BF16)
        value = kv[:, LANES:].astype(BF16)
        for dst, src in ((k_ref, key), (v_ref, value)):
            dst[low(pair), :] = src[:HALF]
            dst[low(15 - pair), :] = src[HALF:]

        @pl.when(lax.div(pair, 2) == quarter)
        def _():
            q = jnp.dot(rows_buf[slot], wq_buf[...], preferred_element_type=F32)
            parts = [q[:, j * LANES:(j + 1) * LANES] for j in range(3)]
            to_queries(q_ref, jnp.concatenate([p * cos + turn(p) * sin for p in parts], axis=1), slot)

    ready = 8 + N_STAGE * LAG

    def body(t, carry):
        net.tick(t, 16, view)
        for s in range(N_STAGE + 1):
            @pl.when(t == 2 + s * LAG)
            def _(s=s):
                small.advance(0, 'D', cs_view, s)

        @pl.when(t == ready)
        def _():
            for c in blocks(0, jnp.int32(0)):
                c.start()
            for w in weights:
                w.wait()

        @pl.when((t > ready) & (t <= ready + 8))
        def _():
            project(t - ready - 1)
        return carry

    lax.fori_loop(0, ready + 9, body, 0)
    for side in range(2):
        for c in blocks(1, quarter * 2 + side):
            c.start()
    for side in range(2):
        for c in blocks(1, quarter * 2 + side):
            c.wait()
        to_queries(do_ref, lax.dot_general(rows_buf[side], wo_buf[...], NT, preferred_element_type=F32), side)
    net.drain(16, view)
    for stage in STAGES['D']:
        small.run(0, 'D', cs_view, stage, 'sent')


def any_spec():
    return pl.BlockSpec(memory_space=pl.ANY)


def vmem_spec():
    return pl.BlockSpec(memory_space=pltpu.VMEM)


def sems(*shape):
    return pltpu.SemaphoreType.DMA(shape)


def like(shape, dtype):
    return jax.ShapeDtypeStruct(shape, dtype)


def gather_in(h, dy, cs, w_q, w_k, w_v, w_o):
    model = h.shape[1]
    queries, keys = like((3, QROWS, LANES), BF16), like((SEQ, LANES), BF16)
    return pl.pallas_call(
        gather_in_kernel,
        out_shape=[like((2, 2, 2, 2, 4) + h.shape, BF16), like((2, 2, 2, 4) + cs.shape, F32), queries, keys, keys, queries],
        in_specs=[vmem_spec()] * 3 + [any_spec()] * 4,
        out_specs=[any_spec()] * 2 + [vmem_spec()] * 4,
        scratch_shapes=[pltpu.VMEM((2, BLK, model), BF16), pltpu.VMEM((2, BLK, LANES), F32),
                        pltpu.VMEM((model, 3 * LANES), BF16), pltpu.VMEM((model, 2 * LANES), BF16),
                        pltpu.VMEM((3 * LANES, model), BF16),
                        sems(16, N_SLOT), sems(16, N_SLOT), sems(1, N_SLOT), sems(1, N_SLOT),
                        sems(3), sems(4), sems(2, 4), sems(2, 4)],
        compiler_params=pltpu.CompilerParams(has_side_effects=True, vmem_limit_bytes=VMEM_LIMIT),
    )(h, dy, cs, w_q, w_k, w_v, w_o)


N_PIECE = 8
O_PIECE = 5
N_TILE = 6
PER_PIECE = 2 * N_TILE
IN_GATHER = 7
N_GATHER = IN_GATHER * PER_PIECE


def tile_product(operand, piece, of_output):
    left, right = (piece, operand) if of_output else (operand, piece)
    return lax.dot_general(left, right, TN, preferred_element_type=F32)


def operand_copy(hd_ref, abuf, asem, which, t, slot):
    return pltpu.make_async_copy(
        hd_ref.at[which, :, pl.ds(pl.multiple_of(t * BLK, BLK), BLK)], abuf.at[slot], asem.at[slot])


def piece_copies(g_ref, gbuf, gsem, p, core, slot):
    return [pltpu.make_async_copy(g_ref.at[p, core, z, r // 2, r % 2],
                                  gbuf.at[slot, pl.ds(r * QROWS, QROWS), pl.ds(z * LANES, LANES)], gsem.at[slot, z * 4 + r])
            for z in range(4) for r in range(4)]


def lane_groups(op, s):
    out = s[:, :LANES]
    for i in range(1, s.shape[1] // LANES):
        out = op(out, s[:, i * LANES:(i + 1) * LANES])
    return out


class Attention:
    def __init__(self, q, do, k, v, cs, out, dk_acc, dv_acc, s, state, quarter):
        self.q, self.do, self.k, self.v, self.cs, self.out = q, do, k, v, cs, out
        self.dk, self.dv, self.s, self.state = dk_acc, dv_acc, s, state
        self.quarter = quarter
        self.scale = LANES ** -0.5
        self.factor = self.scale * 1.4426950408889634

    def step(self, t):
        head, half = lax.div(t, 8), lax.rem(lax.div(t, 4), 2)
        n_key = jnp.where(half == 0, self.quarter + 1, SEQ // BLK - self.quarter)
        rows = pl.ds(pl.multiple_of(half * BLK, BLK), BLK)
        for i, act in enumerate((self.scores, self.exps, self.values, self.grads)):
            @pl.when(lax.rem(t, 4) == i)
            def _(act=act):
                act(head, half, n_key, rows)

    def keys(self, kb):
        return pl.ds(pl.multiple_of(kb * BLK, BLK), BLK)

    def zeros(self):
        return jnp.zeros((BLK, LANES), F32)

    def keep(self, i, column):
        self.state[i] = jnp.broadcast_to(column, (BLK, LANES))

    def kept(self, i):
        return self.state[i, :, :1]

    def scores(self, head, half, n_key, rows):
        q = self.q[head, rows, :]

        def block(kb, m, diagonal=False):
            s = lax.dot_general(q, self.k[self.keys(kb), :], NT, preferred_element_type=F32)
            if diagonal:
                visible = lax.broadcasted_iota(jnp.int32, s.shape, 0) >= lax.broadcasted_iota(jnp.int32, s.shape, 1)
                s = jnp.where(visible, s, -1e30)
            self.s[kb] = s
            return jnp.maximum(m, lane_groups(jnp.maximum, s))

        m = lax.fori_loop(0, n_key - 1, block, self.zeros() - 1e30)
        m = block(n_key - 1, m, diagonal=True)
        self.keep(0, jnp.max(m, axis=1, keepdims=True) * self.factor)

    def exps(self, head, half, n_key, rows):
        m = self.kept(0)

        def block(kb, total):
            e = jnp.exp2(self.s[kb] * self.factor - m)
            self.s[kb] = e
            return total + lane_groups(jnp.add, e)

        total = lax.fori_loop(0, n_key, block, self.zeros())
        self.keep(0, 1.0 / jnp.sum(total, axis=1, keepdims=True))

    def sides(self, half):
        for side in range(2):
            place = (half * (1 - side) + (1 - half) * side) * HALF
            yield pl.ds(pl.multiple_of(place, HALF), HALF), pl.ds(pl.multiple_of(side * BLK + half * HALF, HALF), HALF)

    def values(self, head, half, n_key, rows):
        do, inv = self.do[head, rows, :], self.kept(0)

        def block(kb, o):
            p = self.s[kb] * inv
            self.s[kb] = p
            p = p.astype(BF16)
            self.dv[self.keys(kb), :] += lax.dot_general(p, do, TN, preferred_element_type=F32)
            return o + jnp.dot(p, self.v[self.keys(kb), :], preferred_element_type=F32)

        o = lax.fori_loop(0, n_key, block, self.zeros()).astype(BF16).astype(F32)
        self.keep(0, jnp.sum(do.astype(F32) * o, axis=1, keepdims=True))
        self.state[1] = o
        for place, stored in self.sides(half):
            self.out[1, head, stored, :] = self.state[1, place, :].astype(BF16)

    def grads(self, head, half, n_key, rows):
        q, do, delta = self.q[head, rows, :], self.do[head, rows, :], self.kept(0)

        def block(kb, dq):
            dp = lax.dot_general(do, self.v[self.keys(kb), :], NT, preferred_element_type=F32)
            ds = (self.s[kb] * (dp - delta)).astype(BF16)
            self.dk[self.keys(kb), :] += lax.dot_general(ds, q, TN, preferred_element_type=F32)
            return dq + jnp.dot(ds, self.k[self.keys(kb), :], preferred_element_type=F32)

        dq = lax.fori_loop(0, n_key, block, self.zeros()) * self.scale
        self.state[1] = dq.astype(BF16).astype(F32)
        for place, stored in self.sides(half):
            cos, sin = cos_sin(self.cs[stored, :])
            part = self.state[1, place, :]
            self.out[0, head, stored, :] = (part * cos - turn(part) * sin).astype(BF16)

    def key_grads(self, out):
        for pair in range(8):
            for i, (acc, factor) in enumerate(((self.dk, self.scale), (self.dv, 1.0))):
                for part, block in enumerate((pair, 15 - pair)):
                    out[pair // 2, i, pl.ds(pair % 2 * BLK + part * HALF, HALF), :] = (
                        acc[pl.ds(block * HALF, HALF), :] * factor).astype(BF16)


N_STEP = 24
START = 8
N_UNIT = N_PIECE * UPP
GAIN_PARTS = 12
N_DEV = 32


def main_kernel(q_ref, do_ref, k_ref, v_ref, cs_ref, x_ref, dy_ref, gain_ref, hd_ref, wq_ref, wk_ref, wv_ref,
                g_ref, t_ref, o_ref, dx_ref, dgain_ref,
                piece_buf, dk_acc, dv_acc, s_buf, state, dkv_buf, peer_buf, gbuf, abuf, obuf, own_buf, w_buf, dn_buf, part_buf, parts,
                send_sem, recv_sem, lsem, gsem, asem, osem, tsend, trecv, psend, precv, rsem, wsem, gain_send, gain_recv):
    net = Gather(send_sem, recv_sem)
    quarter = net.y * 2 + net.x
    model = x_ref.shape[1]
    attn = Attention(q_ref, do_ref, k_ref, v_ref, cs_ref, piece_buf, dk_acc, dv_acc, s_buf, state, quarter)
    dk_acc[...] = jnp.zeros_like(dk_acc)
    dv_acc[...] = jnp.zeros_like(dv_acc)

    def local(p, src):
        return pltpu.make_async_copy(src, g_ref.at[p, net.c, net.z, net.y, net.x], lsem.at[p])

    def head_pieces(head):
        return [local(head + p, piece_buf.at[i, head]) for i, p in ((0, 0), (1, O_PIECE))]

    peers = []
    for i, (dx, dy) in enumerate(((1, 0), (0, 1), (1, 1))):
        x, y = (1 - net.x if dx else net.x), (1 - net.y if dy else net.y)
        peers.append(functools.partial(
            pltpu.make_async_remote_copy, dkv_buf.at[y * 2 + x], peer_buf.at[i], psend.at[i], precv.at[i],
            device_id=net.device(x=x, y=y), device_id_type=pl.DeviceIdType.MESH))

    def add_peers():
        for peer in peers:
            peer().wait_recv()
        total = dkv_buf[quarter].astype(F32)
        for i in range(3):
            total = total + peer_buf[i].astype(F32)
        total = total.astype(BF16)
        cos, sin = cos_sin(cs_ref[...])
        dk = total[0].astype(F32)
        piece_buf[0, 0] = (dk * cos - turn(dk) * sin).astype(BF16)
        piece_buf[0, 1] = total[1]
        kv = [local(3 + i, piece_buf.at[0, i]) for i in range(2)]
        for copy in kv:
            copy.start()
        for copy in kv:
            copy.wait()

    def view(u):
        unit_rows = QROWS // UPP
        rows = pl.ds(pl.multiple_of(lax.rem(u, UPP) * unit_rows, unit_rows), unit_rows)
        p = lax.div(u, UPP)
        return lambda c, x, y, z: g_ref.at[p, c, z, y, x, rows, :]

    def place(n):
        return lax.div(n, N_TILE) * PER_PIECE + lax.rem(n, N_TILE) * 2 + net.c

    def keep_tile(n, slot):
        return pltpu.make_async_copy(obuf.at[slot], t_ref.at[place(n)], osem.at[slot])

    def give_tile(n, slot):
        return pltpu.make_async_remote_copy(
            obuf.at[slot], t_ref.at[place(n)], tsend.at[slot], trecv.at[n],
            device_id=net.device(c=1 - net.c), device_id_type=pl.DeviceIdType.MESH)

    def operand(n):
        return operand_copy(hd_ref, abuf, asem, jnp.where(n < O_PIECE * N_TILE, 0, 1), lax.rem(n, N_TILE), lax.rem(n, 2))

    def piece(p):
        return piece_copies(g_ref, gbuf, gsem, p, net.c, lax.rem(p, 2))

    n_own = IN_GATHER * N_TILE

    def tile(n, carry):
        slot = lax.rem(n, 3)
        p = lax.div(n, N_TILE)

        @pl.when(lax.rem(n, N_TILE) == 0)
        def _():
            for copy in piece(p):
                copy.wait()
        operand(n).wait()

        @pl.when(n + 1 < n_own)
        def _():
            operand(n + 1).start()

        @pl.when(n >= 3)
        def _():
            keep_tile(n, slot).wait()
            give_tile(n, slot).wait_send()
        for of_output in (False, True):
            @pl.when((p >= O_PIECE) == of_output)
            def _(of_output=of_output):
                obuf[slot] = tile_product(abuf[lax.rem(n, 2)], gbuf[lax.rem(p, 2)], of_output)
        keep_tile(n, slot).start()
        give_tile(n, slot).start()
        return carry

    def own_copies(p):
        rows = pl.ds(pl.multiple_of(net.c * BLK + net.z * LANES, LANES), LANES)
        for g in range(8):
            if p < 3:
                dst, col = own_buf, 3 * g + p
            elif p < O_PIECE:
                dst, col = own_buf, 8 * p + g
            else:
                dst, col = o_ref, 3 * g + p - O_PIECE
            yield pltpu.make_async_copy(
                g_ref.at[p, g // 4, g % 4, net.y, net.x, rows, :], dst.at[:, pl.ds(col * LANES, LANES)], rsem.at[p, g])

    def own(pieces, wait):
        for p in pieces:
            for copy in own_copies(p):
                if wait:
                    copy.wait()
                else:
                    copy.start()

    def weight_rows(i):
        slot = lax.rem(i, 2)
        rows = pl.ds(pl.multiple_of(i * HALF, HALF), HALF)
        kv = wk_ref.shape[1]
        return [pltpu.make_async_copy(src.at[rows, :], w_buf.at[slot, :, cols], wsem.at[slot, j]) for j, (src, cols) in enumerate((
            (wq_ref, slice(0, 3 * kv)), (wk_ref, slice(3 * kv, 4 * kv)), (wv_ref, slice(4 * kv, 5 * kv))))]

    def inv_rms():
        x = x_ref[...].astype(F32)
        return lax.rsqrt(jnp.mean(x * x, axis=-1, keepdims=True) + NORM_EPS)

    def norm_grad(i):
        slot = lax.rem(i, 2)
        for copy in weight_rows(i):
            copy.wait()

        @pl.when(i + 1 < GAIN_PARTS)
        def _():
            for copy in weight_rows(i + 1):
                copy.start()
        cols = pl.ds(pl.multiple_of(i * HALF, HALF), HALF)
        dn = lax.dot_general(own_buf[...], w_buf[slot], NT, preferred_element_type=F32)
        dn_buf[:, cols] = dn
        x_hat = x_ref[:, cols].astype(F32) * inv_rms()
        part = jnp.sum(dn * x_hat, axis=0, keepdims=True)
        for j in range(2):
            part_buf[pl.ds(i * 2 + j, 1), :] = part[:, j * LANES:(j + 1) * LANES]

    me = lax.axis_index('cp') * 4 + net.z

    def gain_copy(step, slot):
        other = lax.rem(me + step, N_DEV)
        return pltpu.make_async_remote_copy(
            part_buf, parts.at[slot], gain_send.at[step], gain_recv.at[slot],
            device_id=(lax.rem(other, 4), lax.div(other, 4)), device_id_type=pl.DeviceIdType.MESH)

    def others(act):
        def run(step, carry):
            act(step)
            return carry
        lax.fori_loop(1, N_DEV, run, 0)

    def input_grad():
        x_hat = x_ref[...].astype(F32) * inv_rms()
        d_hat = dn_buf[...] * gain_ref[...].astype(F32)
        dx_ref[...] = (dy_ref[...].astype(F32) + inv_rms() * (
            d_hat - x_hat * jnp.mean(d_hat * x_hat, axis=-1, keepdims=True))).astype(BF16)

    operand(jnp.int32(0)).start()
    kv_tick = START + 3 * UPP
    own_tick = START + O_PIECE * UPP + N_STAGE * LAG

    def body(t, carry):
        n, loaded = carry

        @pl.when((t > 0) & (t <= N_STEP) & (lax.rem(t, 8) == 0))
        def _():
            for copy in head_pieces(lax.div(t, 8) - 1):
                copy.wait()

        @pl.when(t == N_STEP)
        def _():
            attn.key_grads(dkv_buf)
            for peer in peers:
                peer().start()

        @pl.when(t == kv_tick)
        def _():
            add_peers()
        net.tick(t - START, N_UNIT, view)

        @pl.when(t < N_STEP)
        def _():
            attn.step(t)

            @pl.when(lax.rem(t, 8) == 7)
            def _():
                for copy in head_pieces(lax.div(t, 8)):
                    copy.start()

        complete = jnp.minimum(lax.div(jnp.maximum(t - START - (N_STAGE - 1) * LAG + 1, 0), UPP), IN_GATHER)
        load = (loaded < complete) & (loaded <= lax.div(n, N_TILE) + 1)

        @pl.when(load)
        def _():
            for copy in piece(loaded):
                copy.start()

        @pl.when(t == own_tick)
        def _():
            own(range(O_PIECE), False)
            for copy in weight_rows(jnp.int32(0)):
                copy.start()

        @pl.when(t == own_tick + 1)
        def _():
            own(range(O_PIECE), True)

        @pl.when((t > own_tick) & (t <= own_tick + GAIN_PARTS))
        def _():
            norm_grad(t - own_tick - 1)

        @pl.when(t == own_tick + GAIN_PARTS + 1)
        def _():
            mine = pltpu.make_async_copy(part_buf, parts.at[me], gain_send.at[0])
            mine.start()
            mine.wait()
            others(lambda step: gain_copy(step, me).start())
            input_grad()

        n_end = jnp.minimum(jnp.minimum(n + 1, loaded * N_TILE), n_own)
        lax.fori_loop(n, n_end, tile, 0)
        return n_end, loaded + load.astype(jnp.int32)

    n, _ = lax.fori_loop(0, START + n_ticks(N_UNIT) + 1, body, (jnp.int32(0), jnp.int32(0)))
    own(range(O_PIECE, N_PIECE), False)
    lax.fori_loop(n, n_own, tile, 0)
    others(lambda step: gain_copy(step, lax.rem(me + step, N_DEV)).wait_recv())
    dgain_ref[...] = jnp.sum(parts[...], axis=0)
    for slot in range(3):
        keep_tile(0, slot).wait()
        give_tile(0, slot).wait_send()

    def received(n, carry):
        give_tile(n, 0).wait_recv()
        return carry

    lax.fori_loop(0, n_own, received, 0)
    own(range(O_PIECE, N_PIECE), True)
    for peer in peers:
        peer().wait_send()
    others(lambda step: gain_copy(step, me).wait_send())
    net.drain(N_UNIT, view)


def main(q, do, k, v, cs, x, dy, gain, hd, w_q, w_k, w_v):
    model = x.shape[1]
    qkv = w_q.shape[1] + w_k.shape[1] + w_v.shape[1]
    return pl.pallas_call(
        main_kernel,
        out_shape=[like((N_PIECE, 2, 4, 2, 2, QROWS, LANES), BF16), like((N_GATHER, BLK, BLK), F32),
                   like((LANES, model), BF16), like(x.shape, BF16), like((2 * GAIN_PARTS, LANES), F32)],
        in_specs=[vmem_spec()] * 8 + [any_spec()] * 4,
        out_specs=[any_spec()] * 2 + [vmem_spec()] * 3,
        scratch_shapes=[
            pltpu.VMEM((2, 3, QROWS, LANES), BF16), pltpu.VMEM((SEQ, LANES), F32), pltpu.VMEM((SEQ, LANES), F32),
            pltpu.VMEM((SEQ // BLK, BLK, BLK), F32), pltpu.VMEM((2, BLK, LANES), F32),
            pltpu.VMEM((4, 2, QROWS, LANES), BF16), pltpu.VMEM((3, 2, QROWS, LANES), BF16),
            pltpu.VMEM((2, SEQ, BLK), BF16), pltpu.VMEM((2, SEQ, BLK), BF16), pltpu.VMEM((3, BLK, BLK), F32),
            pltpu.VMEM((LANES, qkv), BF16), pltpu.VMEM((2, HALF, qkv), BF16), pltpu.VMEM(x.shape, F32),
            pltpu.VMEM((2 * GAIN_PARTS, LANES), F32), pltpu.VMEM((N_DEV, 2 * GAIN_PARTS, LANES), F32),
            sems(N_UNIT, N_SLOT), sems(N_UNIT, N_SLOT), sems(N_PIECE), sems(2, 16), sems(2), sems(3), sems(3),
            sems(IN_GATHER * N_TILE), sems(3), sems(3), sems(N_PIECE, 8), sems(2, 3), sems(N_DEV), sems(N_DEV)],
        compiler_params=pltpu.CompilerParams(has_side_effects=True, vmem_limit_bytes=VMEM_LIMIT),
    )(q, do, k, v, cs, x, dy, gain, hd, w_q, w_k, w_v)


GROUP = IN_GATHER


def finish_kernel(hd_ref, g_ref, t_ref, wq_ref, wk_ref, wv_ref, wo_ref,
                  gbuf, abuf, obuf, cbuf, gsem, asem, osem, isem, csem):
    n_step, group = PER_PIECE, GROUP

    def operand(t):
        return operand_copy(hd_ref, abuf, asem, 1, t, lax.rem(t, 2))

    def cut(t):
        return pl.ds(pl.multiple_of(t * BLK, BLK), BLK)

    def lanes(i):
        return pl.ds(pl.multiple_of(i * LANES, LANES), LANES)

    def to_output(p, t, sub, src, sem):
        return [pltpu.make_async_copy(
            src.at[pl.ds(i * LANES, LANES), :], wo_ref.at[lanes(3 * (sub * 4 + i) + p - O_PIECE), cut(t)], sem.at[i])
            for i in range(4)]

    def to_input(dst, place, t, sub, src, sem):
        return [pltpu.make_async_copy(
            src.at[:, pl.ds(i * LANES, LANES)], dst.at[cut(t), lanes(place(sub * 4 + i))], sem.at[i]) for i in range(4)]

    def ins(n):
        return [pltpu.make_async_copy(t_ref.at[n * group + i], cbuf.at[lax.rem(n, 3), i], isem.at[lax.rem(n, 3), i])
                for i in range(group)]

    def start_outs(n):
        for i in range(group):
            m = n * group + i
            p, t, sub = lax.div(m, PER_PIECE), lax.rem(lax.div(m, 2), N_TILE), lax.rem(m, 2)
            src, sem = cbuf.at[lax.rem(n, 3), i], csem.at[lax.rem(n, 3), i]
            for cond, copies in (
                (p < 3, lambda: to_input(wq_ref, lambda g: 3 * g + p, t, sub, src, sem)),
                (p == 3, lambda: to_input(wk_ref, lambda g: g, t, sub, src, sem)),
                (p == 4, lambda: to_input(wv_ref, lambda g: g, t, sub, src, sem)),
                (p >= O_PIECE, lambda: to_output(p, t, sub, src, sem)),
            ):
                @pl.when(cond)
                def _(copies=copies):
                    for c in copies():
                        c.start()

    def wait_outs(n):
        for i in range(group):
            for c in to_output(O_PIECE, 0, 0, cbuf.at[0, i], csem.at[lax.rem(n, 3), i]):
                c.wait()

    for sub in range(2):
        for c in piece_copies(g_ref, gbuf, gsem, IN_GATHER, sub, sub):
            c.start()
    operand(jnp.int32(0)).start()

    def step(n, carry):
        t, p, sub = lax.div(n, 2), IN_GATHER, lax.rem(n, 2)
        slot = lax.rem(n, 3)

        @pl.when(n >= 3)
        def _():
            wait_outs(n - 3)
        for c in ins(n):
            c.start()

        @pl.when(n >= 1)
        def _():
            for c in ins(n - 1):
                c.wait()
            start_outs(n - 1)

        @pl.when(sub == 0)
        def _():
            operand(t).wait()

            @pl.when(t + 1 < N_TILE)
            def _():
                operand(t + 1).start()

        @pl.when(n < 2)
        def _():
            for c in piece_copies(g_ref, gbuf, gsem, p, sub, sub):
                c.wait()

        @pl.when(n >= 3)
        def _():
            for c in to_output(O_PIECE, 0, 0, obuf.at[0], osem.at[slot]):
                c.wait()
        obuf[slot] = tile_product(abuf[lax.rem(t, 2)], gbuf[sub], True)
        for c in to_output(p, t, sub, obuf.at[slot], osem.at[slot]):
            c.start()
        return carry

    lax.fori_loop(0, n_step, step, 0)
    for c in ins(n_step - 1):
        c.wait()
    start_outs(jnp.int32(n_step - 1))
    for n in range(n_step - 3, n_step):
        wait_outs(n)
        for c in to_output(O_PIECE, 0, 0, obuf.at[0], osem.at[n % 3]):
            c.wait()


def finish(hd, g, tiles):
    model, kv = hd.shape[2], 8 * LANES
    return pl.pallas_call(
        finish_kernel,
        out_shape=[like((model, n), F32) for n in (3 * kv, kv, kv)] + [like((3 * kv, model), F32)],
        in_specs=[any_spec()] * 3,
        out_specs=[any_spec()] * 4,
        scratch_shapes=[pltpu.VMEM((2, SEQ, BLK), BF16), pltpu.VMEM((2, SEQ, BLK), BF16), pltpu.VMEM((3, BLK, BLK), F32),
                        pltpu.VMEM((3, GROUP, BLK, BLK), F32),
                        sems(2, 16), sems(2), sems(3, 4), sems(3, GROUP), sems(3, GROUP, 4)],
        cost_estimate=pl.CostEstimate(flops=2 * SEQ * kv * model, bytes_accessed=250 * 2**20, transcendentals=0),
        compiler_params=pltpu.CompilerParams(vmem_limit_bytes=VMEM_LIMIT),
    )(hd, g, tiles)


def solution(mesh):
    assert mesh.shape['hp'] == 4 and mesh.shape['cp'] == 8

    def device_step(hidden, grad_out, positions, norm_gain, w_q, w_k, w_v, w_o, inv_freq):
        model = hidden.shape[1]
        quarter = lax.div(lax.axis_index('cp'), 2)
        gain = norm_gain.astype(F32)
        x_f32 = hidden.astype(F32)
        inv_rms = lax.rsqrt(jnp.mean(x_f32 * x_f32, axis=-1, keepdims=True) + NORM_EPS)
        x_hat = x_f32 * inv_rms
        normed = (x_hat * gain).astype(BF16)
        angles = positions.astype(F32)[:, None] * inv_freq[None, :]
        cs = jnp.concatenate([jnp.cos(angles), jnp.sin(angles)], axis=1)

        hd, csg, q, k, v, d_out = gather_in(normed, grad_out, cs, w_q, w_k, w_v, w_o)
        hd = hd.reshape(2, SEQ, model)
        cs_rows = lax.dynamic_slice(csg.reshape(SEQ, LANES), (quarter * QROWS, 0), (QROWS, LANES))
        gathered, tiles, o_own, grad_hidden, gains = main(
            q, d_out, k, v, cs_rows, hidden, grad_out, norm_gain.reshape(1, model), hd, w_q, w_k, w_v)
        grad_wq, grad_wk, grad_wv, grad_wo = finish(hd, gathered, tiles)
        output = (x_f32 + jnp.dot(o_own, w_o, preferred_element_type=F32)).astype(BF16)
        grad_gain = gains.reshape(-1)
        return output, grad_hidden, grad_wq, grad_wk, grad_wv, grad_wo, grad_gain

    rows, whole = P(('cp', 'hp'), None), P()
    return jax.shard_map(
        device_step, mesh=mesh,
        in_specs=(rows, rows, P(('cp', 'hp')), whole, whole, whole, whole, whole, whole),
        out_specs=(rows, rows, whole, whole, whole, whole, whole), check_vma=False)
```

```python
import functools
import jax
import jax.numpy as jnp
from jax import lax
from jax.experimental import pallas as pl
from jax.experimental.pallas import tpu as pltpu
from jax.sharding import PartitionSpec as P

NORM_EPS = 1e-5
ALL = Ellipsis
EVERY = slice(None)
PAIR, TRIO, QUAD = 2, 3, 4
GRID = (PAIR, PAIR, PAIR, QUAD)
BY_COLUMN = {'axis': 0, 'keepdims': True}
BY_ROW = {'axis': 1, 'keepdims': True}
F32 = jnp.float32
BF16 = jnp.bfloat16
LANES = 128
BLK = 512
HALF = BLK // 2
SEQ = 8 * BLK
QROWS = PAIR * BLK
UPP = 8
LAG = 2
RING = 20
VMEM_LIMIT = 64 * 2**20 - 2**16
NT = (((1,), (1,)), ((), ()))
TN = (((0,), (0,)), ((), ()))

STAGES = {
    'C': ('z1', 'z2', 'z3', 'y', 'x', 'd'),
    'D': ('z1', 'z2', 'z3', 'x', 'y', 'd'),
    'E': ('x', 'y', 'z1', 'z2', 'z3', 'd'),
    'F': ('y', 'x', 'z1', 'z2', 'z3', 'd'),
}
SLOT = {'z1': 0, 'z2': 2, 'z3': 4, 'x': 6, 'y': 7, 'd': 8}
N_STAGE = 6
N_SLOT = 9


def odd(i):
    return lax.rem(i, PAIR)


def half_of(i):
    return lax.div(i, PAIR)


def nxt(i):
    return i + 1


def zero():
    return jnp.int32(0)


def loop(n, body, init):
    return lax.fori_loop(0, n, body, init)


class Gather:
    def __init__(self, send_sem, recv_sem, period, base=0):
        self.period, self.base = period, base
        self.z = lax.axis_index('hp')
        cp = lax.axis_index('cp')
        self.c, self.x, self.y = odd(cp), odd(half_of(cp)), lax.div(cp, 4)
        self.send_sem, self.recv_sem = send_sem, recv_sem

    def device(self, **moved):
        at = {name: moved.get(name, getattr(self, name)) for name in 'cxyz'}
        return at['z'], (at['y'] * PAIR + at['x']) * PAIR + at['c']

    def copies(self, sem_row, kind, view, stage):
        c, x, y, z = self.c, self.x, self.y, self.z
        order = STAGES[kind]
        done = {st[0] for st in order[:order.index(stage)]}
        every = EVERY
        gx, gy, gz = (every if d in done else v for d, v in (('x', x), ('y', y), ('z', z)))
        slot = SLOT[stage]

        def copy(place, device, slot):
            return lambda: pltpu.make_async_remote_copy(
                place, place, self.send_sem.at[sem_row, slot], self.recv_sem.at[sem_row, slot],
                device_id=device, device_id_type=pl.DeviceIdType.MESH)

        if stage == 'x':
            dev = self.device(x=1 - x)
            return [(None, copy(view(c, x, gy, gz), dev, slot), None, copy(view(c, 1 - x, gy, gz), dev, slot))]
        if stage == 'y':
            dev = self.device(y=1 - y)
            return [(None, copy(view(c, gx, y, gz), dev, slot), None, copy(view(c, gx, 1 - y, gz), dev, slot))]
        if stage == 'd':
            dev = self.device(c=1 - c)
            return [(None, copy(view(c, every, every, every), dev, slot),
                     None, copy(view(1 - c, every, every, every), dev, slot))]
        hop = int(stage[1])
        up, down = self.device(z=jnp.minimum(z + 1, 3)), self.device(z=jnp.maximum(z - 1, 0))
        return [
            ((z >= hop - 1) & (z < 3), copy(view(c, gx, gy, jnp.maximum(z - hop + 1, 0)), up, slot),
             z >= hop, copy(view(c, gx, gy, jnp.maximum(z - hop, 0)), up, slot)),
            ((z + hop <= 4) & (z > 0), copy(view(c, gx, gy, jnp.minimum(z + hop - 1, 3)), down, slot + 1),
             z + hop <= 3, copy(view(c, gx, gy, jnp.minimum(z + hop, 3)), down, slot + 1)),
        ]

    def run(self, sem_row, kind, view, stage, what):
        for can_send, send, can_recv, recv in self.copies(sem_row, kind, view, stage):
            cond = can_recv if what == 'recv' else can_send

            def act(send=send, recv=recv):
                if what == 'start':
                    send().start()
                elif what == 'sent':
                    send().wait_send()
                else:
                    recv().wait_recv()

            if cond is None:
                act()
            else:
                pl.when(cond)(act)

    def advance(self, sem_row, kind, view, s):
        if 0 < s <= N_STAGE:
            self.run(sem_row, kind, view, STAGES[kind][s - 1], 'recv')
        if s < N_STAGE:
            self.run(sem_row, kind, view, STAGES[kind][s], 'start')
        if s > N_STAGE:
            for stage in STAGES[kind]:
                self.run(sem_row, kind, view, stage, 'sent')

    def kinds(self, u):
        w, even = lax.rem(u, self.period), odd(u) == 0
        e, f = w == 0, w == self.period - 5
        return (('C', ~(e | f) & even), ('D', ~(e | f) & ~even), ('E', e), ('F', f))

    def tick(self, t, n_units, view):
        for s in range(N_STAGE + 2):
            u = t - s * LAG

            @pl.when((u >= 0) & (u < n_units))
            def _(u=u, s=s):
                for kind, is_kind in self.kinds(u):
                    @pl.when(is_kind)
                    def _(kind=kind):
                        self.advance(lax.rem(u + self.base, RING), kind, view(u), s)


def turn(v):
    return pltpu.roll(v, LANES // 2, 1)


def low_lanes(shape):
    return lax.broadcasted_iota(jnp.int32, shape, 1) < LANES // 2


def cos_sin(cs):
    low = low_lanes(cs.shape)
    other = turn(cs)
    return jnp.where(low, cs, other), jnp.where(low, -other, cs)


def any_spec():
    return pl.BlockSpec(memory_space=pl.ANY)


def vmem_spec():
    return pl.BlockSpec(memory_space=pltpu.VMEM)


def sems(*shape):
    return pltpu.SemaphoreType.DMA(shape) if shape else pltpu.SemaphoreType.DMA


def like(shape, dtype):
    return jax.ShapeDtypeStruct(shape, dtype)


def start_all(copies):
    for copy in copies:
        copy.start()


def wait_all(copies):
    for copy in copies:
        copy.wait()


N_PIECE = 8
O_PIECES = (3, 6, 7)
KEY_PIECE = 4
N_TILE = 6
PER_PIECE = PAIR * N_TILE
IN_GATHER = 7
N_GATHER = IN_GATHER * PER_PIECE


def tile_product(operand, piece, of_output):
    left, right = (piece, operand) if of_output else (operand, piece)
    return lax.dot_general(left, right, TN, preferred_element_type=F32)


def operand_copy(hd_ref, abuf, asem, which, t, slot):
    return pltpu.make_async_copy(
        hd_ref.at[which, :, pl.ds(pl.multiple_of(t * BLK, BLK), BLK)], abuf.at[slot], asem.at[slot])


def piece_copies(g_ref, gbuf, gsem, p, core, slot):
    return [pltpu.make_async_copy(g_ref.at[p, core, z, r // 2, r % 2],
                                  gbuf.at[slot, pl.ds(r * QROWS, QROWS), pl.ds(z * LANES, LANES)], gsem.at[slot])
            for z in range(QUAD) for r in range(QUAD)]


def wait_piece(gbuf, gsem, slot):
    pltpu.make_async_copy(gbuf.at[slot], gbuf.at[slot], gsem.at[slot]).wait()


def lane_groups(op, s):
    out = s[:, :LANES]
    for i in range(1, s.shape[1] // LANES):
        out = op(out, s[:, i * LANES:(i + 1) * LANES])
    return out


class Attention:
    def __init__(self, q, do, k, v, cs, out, dk_acc, dv_acc, s, state, quarter):
        self.q, self.do, self.k, self.v, self.cs, self.out = q, do, k, v, cs, out
        self.dk, self.dv, self.s, self.state = dk_acc, dv_acc, s, state
        self.quarter = quarter
        self.scale = LANES ** -0.5
        self.factor = self.scale * 1.4426950408889634

    def step(self, t):
        head, half = lax.div(t, 8), odd(lax.div(t, 4))
        n_key = jnp.where(half == 0, self.quarter + 1, SEQ // BLK - self.quarter)
        rows = pl.ds(pl.multiple_of(half * BLK, BLK), BLK)
        for i, act in enumerate((self.scores, self.exps, self.values, self.grads)):
            @pl.when(lax.rem(t, 4) == i)
            def _(act=act):
                act(head, half, n_key, rows)

    def keys(self, kb):
        return pl.ds(pl.multiple_of(kb * BLK, BLK), BLK)

    def zeros(self):
        return jnp.zeros((BLK, LANES), F32)

    def keep(self, i, column):
        self.state[i] = jnp.broadcast_to(column, (BLK, LANES))

    def kept(self, i):
        return self.state[i, :, :1]

    def scores(self, head, half, n_key, rows):
        q = self.q[head, rows, :]

        def block(kb, m, diagonal=False):
            s = lax.dot_general(q, self.k[self.keys(kb), :], NT, preferred_element_type=F32)
            if diagonal:
                visible = lax.broadcasted_iota(jnp.int32, s.shape, 0) >= lax.broadcasted_iota(jnp.int32, s.shape, 1)
                s = jnp.where(visible, s, -1e30)
            self.s[kb] = s
            return jnp.maximum(m, lane_groups(jnp.maximum, s))

        m = loop(n_key - 1, block, self.zeros() - 1e30)
        m = block(n_key - 1, m, diagonal=True)
        self.keep(0, jnp.max(m, **BY_ROW) * self.factor)

    def exps(self, head, half, n_key, rows):
        m = self.kept(0)

        def block(kb, total):
            e = jnp.exp2(self.s[kb] * self.factor - m)
            self.s[kb] = e
            return total + lane_groups(jnp.add, e)

        total = loop(n_key, block, self.zeros())
        self.keep(0, 1.0 / jnp.sum(total, **BY_ROW))

    def sides(self, half):
        for side in range(PAIR):
            place = (half * (1 - side) + (1 - half) * side) * HALF
            yield pl.ds(pl.multiple_of(place, HALF), HALF), pl.ds(pl.multiple_of(side * BLK + half * HALF, HALF), HALF)

    def values(self, head, half, n_key, rows):
        do, inv = self.do[head, rows, :], self.kept(0)
        turned = do.T

        def block(kb, o):
            p = (self.s[kb] * inv).astype(BF16)
            self.dv[:, self.keys(kb)] += jnp.dot(turned, p, preferred_element_type=F32)
            return o + jnp.dot(p, self.v[self.keys(kb), :], preferred_element_type=F32)

        o = loop(n_key, block, self.zeros()).astype(BF16).astype(F32)
        self.keep(1, jnp.sum(do.astype(F32) * o, **BY_ROW))
        self.state[2] = o
        for place, stored in self.sides(half):
            self.out[1, head, stored, :] = self.state[2, place, :].astype(BF16)

    def grads(self, head, half, n_key, rows):
        do, inv, delta = self.do[head, rows, :], self.kept(0), self.kept(1)
        turned = self.q[head, rows, :].T

        def block(kb, dq):
            dp = lax.dot_general(do, self.v[self.keys(kb), :], NT, preferred_element_type=F32)
            ds = (self.s[kb] * inv * (dp - delta)).astype(BF16)
            self.dk[:, self.keys(kb)] += jnp.dot(turned, ds, preferred_element_type=F32)
            return dq + jnp.dot(ds, self.k[self.keys(kb), :], preferred_element_type=F32)

        dq = loop(n_key, block, self.zeros()) * self.scale
        self.state[2] = dq.astype(BF16).astype(F32)
        for place, stored in self.sides(half):
            cos, sin = cos_sin(self.cs[stored, :])
            part = self.state[2, place, :]
            self.out[0, head, stored, :] = (part * cos - turn(part) * sin).astype(BF16)

    def key_grads(self, out):
        for pair in range(8):
            for i, (acc, factor) in enumerate(((self.dk, self.scale), (self.dv, 1.0))):
                for part, block in enumerate((pair, 15 - pair)):
                    out[pair // 2, i, pl.ds(pair % PAIR * BLK + part * HALF, HALF), :] = (
                        acc[:, pl.ds(block * HALF, HALF)].T * factor).astype(BF16)


ROWS_UNIT = 8
N_IN = LANES // ROWS_UNIT
N_STEP = 24
N_UNIT = N_PIECE * UPP
N_PART = 12
SEND_DO = N_PART + 1
DELAY = N_STAGE * LAG
CHUNK = PAIR * ROWS_UNIT
N_CHUNK = LANES // CHUNK
PROJECT = DELAY + 2
ATTEND = PROJECT + PAIR * N_CHUNK - 1
ATTENDED = ATTEND + N_STEP
START = ATTEND + 4
N_SEND = 8
KEYS_IN = START + KEY_PIECE * UPP
QUERY_IN = START + 3 * UPP + DELAY
OWN_IN = START + O_PIECES[1] * UPP + DELAY
OUT_IN = OWN_IN + N_PART // 2 + 2
N_OUT = 8
LAST = START + N_UNIT + DELAY + LAG
N_DEV = 32


def main_kernel(x_ref, dy_ref, gain_ref, mypos_ref, freq_ref, wq_ref, wk_ref, wv_ref, wo_ref,
                hd_ref, pos_ref, g_ref, t_ref, o_ref, sum_ref, dx_ref, dgain_ref,
                h_buf, q_buf, do_buf, k_buf, v_buf, rows_buf, mypos_buf, gain_buf, freq_buf, pos_buf, pos_t, cs_buf, own_cs, do_parts,
                piece_buf, dk_acc, dv_acc, s_buf, state, dkv_buf, peer_buf, gbuf, abuf, obuf, own_buf, oo_buf, w_buf, dn_buf, part_buf, parts,
                cs_send, cs_recv, send_sem, recv_sem, first_sem, proj_sem, rows_sem, do_send, do_recv,
                lsem, gsem, asem, osem, tsend, trecv, psend, precv, rsem, wsem, gain_send, gain_recv):
    net_in, net_cs, net = Gather(send_sem, recv_sem, 9), Gather(cs_send, cs_recv, 9), Gather(send_sem, recv_sem, 8, START)
    quarter = net.y * 2 + net.x
    head = net.c * 4 + net.z
    spot = (net.y, net.x, net.c, net.z)
    attn = Attention(q_buf, do_buf, k_buf, v_buf, own_cs, piece_buf, dk_acc, dv_acc, s_buf, state, quarter)

    def inv_rms():
        x = x_ref[ALL].astype(F32)
        return lax.rsqrt(jnp.mean(x * x, **BY_ROW) + NORM_EPS)

    me = lax.axis_index('cp') * 4 + net.z

    def device_at(step):
        other = lax.rem(me + step, N_DEV)
        return lax.rem(other, 4), lax.div(other, 4)

    barrier = pltpu.get_barrier_semaphore()

    def greet(step, carry):
        pl.semaphore_signal(barrier, inc=1, device_id=device_at(step), device_id_type=pl.DeviceIdType.MESH)
        return carry

    lax.fori_loop(1, N_DEV, greet, 0)

    gain_buf[ALL] = gain_ref[ALL].astype(F32).reshape(gain_buf.shape)
    freq_buf[ALL] = jnp.concatenate([freq_ref[ALL], freq_ref[ALL]], axis=0).reshape(freq_buf.shape)
    mypos_buf[ALL] = jnp.broadcast_to(mypos_ref[ALL].astype(F32).reshape(1, LANES), mypos_buf.shape)
    h_buf[ALL] = (x_ref[ALL].astype(F32) * inv_rms() * gain_buf[ALL]).astype(BF16)
    first = [pltpu.make_async_copy(src, dst, first_sem.at[i]) for i, (src, dst) in enumerate((
        (h_buf, hd_ref.at[(0, *spot)]), (dy_ref, hd_ref.at[(1, *spot)]), (mypos_buf, pos_ref.at[spot])))]
    start_all(first)
    wait_all(first)
    pl.semaphore_wait(barrier, N_DEV - 1)
    q_cols = pl.ds(pl.multiple_of(head * TRIO * LANES, LANES), TRIO * LANES)
    kv_cols = pl.ds(pl.multiple_of(head * LANES, LANES), LANES)
    w_rows = slice(0, wq_ref.shape[0])
    wq_buf, wkv_buf = gbuf.at[0, w_rows, :TRIO * LANES], gbuf.at[1, w_rows, :PAIR * LANES]
    weights = [pltpu.make_async_copy(src, dst, proj_sem.at[i]) for i, (src, dst) in enumerate((
        (wq_ref.at[:, q_cols], wq_buf), (wk_ref.at[:, kv_cols], gbuf.at[1, w_rows, :LANES]),
        (wv_ref.at[:, kv_cols], gbuf.at[1, w_rows, LANES:PAIR * LANES])))]

    def view_in(u):
        rows = pl.ds(pl.multiple_of(lax.rem(u, N_IN) * ROWS_UNIT, ROWS_UNIT), ROWS_UNIT)
        which = lax.div(u, N_IN)
        return lambda c, x, y, z: hd_ref.at[which, y, x, c, z, rows, :]

    def view_cs(c, x, y, z):
        return pos_ref.at[y, x, c, z]

    def part(i, width=HALF):
        return pl.ds(pl.multiple_of(i * width, width), width)

    def wo_rows(i):
        slot = odd(i)
        return pltpu.make_async_copy(wo_ref.at[part(i), :], w_buf.at[slot, :, :wo_ref.shape[1]], wsem.at[slot, 0])

    def head_grad(i):
        slot = odd(i)
        wo_rows(i).wait()

        @pl.when(nxt(i) < N_PART)
        def _():
            wo_rows(nxt(i)).start()
        own_buf[:, part(i)] = lax.dot_general(
            dy_ref[ALL], w_buf[slot, :, :wo_ref.shape[1]], NT, preferred_element_type=F32).astype(BF16)

    def do_copy(step, mine):
        me = net.c * 4 + net.z
        other = lax.rem(me + step, 8)
        slot = me if mine else lax.rem(me + 8 - step, 8)
        return pltpu.make_async_remote_copy(
            own_buf.at[:, part(other, TRIO * LANES)], do_parts.at[slot], do_send.at[step], do_recv.at[step],
            device_id=net.device(c=lax.div(other, 4), z=lax.rem(other, 4)), device_id_type=pl.DeviceIdType.MESH)

    own_do = pltpu.make_async_copy(own_buf.at[:, part(head, TRIO * LANES)], do_parts.at[head], do_send.at[0])

    def query_row(c, z):
        return c * HALF + z * LANES if z < 2 else BLK + (1 - c) * HALF + (z - 2) * LANES

    def take_do():
        for step in range(1, 8):
            do_copy(step, False).wait_recv()
        for c in range(PAIR):
            for z in range(QUAD):
                for j in range(TRIO):
                    do_buf[j, pl.ds(query_row(c, z), LANES), :] = do_parts[c * 4 + z, :, j * LANES:(j + 1) * LANES]

    every = EVERY

    def chunk(k, base=0):
        return pl.ds(pl.multiple_of(base + k * CHUNK, CHUNK), CHUNK)

    def chunk_rows(k):
        return pltpu.make_async_copy(hd_ref.at[0, every, every, every, every, chunk(k), every], rows_buf, rows_sem)

    def take_positions():
        copy = pltpu.make_async_copy(pos_ref, pos_buf, rows_sem)
        copy.start()
        copy.wait()
        for i in range(PAIR):
            pos_t[i] = pos_buf[i].reshape(LANES, LANES).T

    def angles(k):
        for dev in range(N_DEV):
            column = pos_t[dev // 16, chunk(k), dev % 16 * 8:dev % 16 * 8 + 1]
            cs_buf[dev * CHUNK:(dev + 1) * CHUNK, :] = jnp.broadcast_to(column, (CHUNK, LANES)) * freq_buf[ALL]
        angle = cs_buf[ALL]
        cs_buf[ALL] = jnp.where(low_lanes(angle.shape), jnp.cos(angle), jnp.sin(angle))

    def rotate(v, cs):
        cos, sin = cos_sin(cs)
        return (v * cos + turn(v) * sin).astype(BF16)

    def project(k):
        chunk_rows(k).wait()
        n_rows = N_DEV * CHUNK
        kv = jnp.dot(rows_buf[ALL].reshape(n_rows, -1), wkv_buf[ALL], preferred_element_type=F32)
        key = rotate(kv[:, :LANES], cs_buf[ALL])
        value = kv[:, LANES:].astype(BF16)
        for cp in range(8):
            for z in range(QUAD):
                block = 2 * cp + z if z < 2 else 28 - 2 * cp + z
                rows = slice((cp * 4 + z) * CHUNK, (cp * 4 + z + 1) * CHUNK)
                k_buf[chunk(k, block * LANES), :] = key[rows]
                v_buf[chunk(k, block * LANES), :] = value[rows]
        mine, cs = rows_buf[net.y, net.x].reshape(LANES, -1), cs_buf[part(quarter, LANES), :]
        q = jnp.dot(mine, wq_buf[ALL], preferred_element_type=F32)
        for j in range(TRIO):
            p = rotate(q[:, j * LANES:(j + 1) * LANES], cs)
            for c in range(PAIR):
                for z in range(QUAD):
                    rows = slice((c * 4 + z) * CHUNK, (c * 4 + z + 1) * CHUNK)
                    q_buf[j, chunk(k, query_row(c, z)), :] = p[rows]
                    if j == 0:
                        own_cs[chunk(k, c * BLK + z * LANES), :] = cs[rows]

    def local(p, i, src, rows=pl.ds(0, QROWS)):
        return pltpu.make_async_copy(src, g_ref.at[p, net.c, net.z, net.y, net.x, rows, :], lsem.at[p, i])

    def step_pieces(step):
        head, half = lax.div(step, 8), odd(lax.div(step, 4))
        out_piece = jnp.where(head == 0, O_PIECES[0], O_PIECES[0] + 2 + head)
        return [local(p, side, piece_buf.at[i, head, rows], rows) for i, p in ((0, head), (1, out_piece))
                for side, (_, rows) in enumerate(attn.sides(half))]

    def key_copies(rows):
        for i, moved in enumerate(('x', 'y', 'xy')):
            x, y = (1 - at if name in moved else at for name, at in (('x', net.x), ('y', net.y)))
            yield pltpu.make_async_remote_copy(
                dkv_buf.at[y * 2 + x, :, rows], peer_buf.at[i, :, rows], psend.at[i], precv.at[i],
                device_id=net.device(x=x, y=y), device_id_type=pl.DeviceIdType.MESH)

    def add_peers():
        for copy in key_copies(pl.ds(0, QROWS)):
            copy.wait_recv()
        total = dkv_buf[quarter].astype(F32)
        for i in range(TRIO):
            total = total + peer_buf[i].astype(F32)
        total = total.astype(BF16)
        cos, sin = cos_sin(own_cs[ALL])
        dk = total[0].astype(F32)
        piece_buf[0, 0] = (dk * cos - turn(dk) * sin).astype(BF16)
        piece_buf[0, 1] = total[1]
        kv = [local(KEY_PIECE + i, 0, piece_buf.at[0, i]) for i in range(PAIR)]
        start_all(kv)
        wait_all(kv)

    def view(u):
        p, k = lax.div(u, UPP), lax.rem(u, UPP)
        two = half_of(k)
        rows = part(odd(two) * 4 + half_of(two) * 2 + odd(k), QROWS // UPP)
        return lambda c, x, y, z: g_ref.at[p, c, z, y, x, rows, :]

    def place(n):
        return lax.div(n, N_TILE) * PER_PIECE + lax.rem(n, N_TILE) * 2 + net.c

    def keep_tile(n, slot):
        return pltpu.make_async_copy(obuf.at[slot], t_ref.at[place(n)], osem.at[slot])

    def give_tile(n, slot):
        return pltpu.make_async_remote_copy(
            obuf.at[slot], t_ref.at[place(n)], tsend.at[slot], trecv.at[n],
            device_id=net.device(c=1 - net.c), device_id_type=pl.DeviceIdType.MESH)

    def of_output(p):
        return (p == O_PIECES[0]) | (p == O_PIECES[1])

    def operand(n):
        which, slot = of_output(lax.div(n, N_TILE)).astype(jnp.int32), odd(n)
        return pltpu.make_async_copy(
            hd_ref.at[which, every, every, every, every, every, part(lax.rem(n, N_TILE), BLK)], abuf.at[slot], asem.at[slot])

    def piece(p):
        return piece_copies(g_ref, gbuf, gsem, p, net.c, odd(p))

    n_own = IN_GATHER * N_TILE

    def tile(n, carry):
        slot = lax.rem(n, TRIO)
        p = lax.div(n, N_TILE)

        @pl.when(lax.rem(n, N_TILE) == 0)
        def _():
            wait_piece(gbuf, gsem, odd(p))
        operand(n).wait()

        @pl.when(nxt(n) < n_own)
        def _():
            operand(nxt(n)).start()

        @pl.when(n >= 3)
        def _():
            keep_tile(n, slot).wait()
            give_tile(n, slot).wait_send()
        for output in (False, True):
            @pl.when(of_output(p) == output)
            def _(output=output):
                obuf[slot] = tile_product(abuf[odd(n)].reshape(SEQ, BLK), gbuf[odd(p)], output)
        keep_tile(n, slot).start()
        give_tile(n, slot).start()
        return carry

    kv = wk_ref.shape[1]
    groups = (((0, 1, 2), own_buf, slice(0, TRIO * kv)), ((KEY_PIECE, KEY_PIECE + 1), own_buf, slice(TRIO * kv, 5 * kv)),
              (O_PIECES[:2], oo_buf, slice(0, PAIR * kv)), (O_PIECES[2:], o_ref, slice(0, kv)))

    def start_own(i):
        rows = pl.ds(pl.multiple_of(net.c * BLK + net.z * LANES, LANES), LANES)
        pieces, dst, cols = groups[i]
        for k, p in enumerate(pieces):
            for g in range(8):
                col = cols.start // LANES + (TRIO * g + k if len(pieces) == 3 else 8 * k + g)
                pltpu.make_async_copy(
                    g_ref.at[p, g // 4, g % 4, net.y, net.x, rows, :], dst.at[:, pl.ds(col * LANES, LANES)], rsem.at[i]).start()

    def wait_own(i):
        _, dst, cols = groups[i]
        pltpu.make_async_copy(dst.at[:, cols], dst.at[:, cols], rsem.at[i]).wait()

    def weight_rows(turn, i):
        slot = odd(i)
        if turn == 0:
            places = ((wq_ref, part(i), 0, TRIO * kv),)
        else:
            places = [(src, part(i * 2 + j), (j * 2 + k) * kv, kv) for j in range(PAIR) for k, src in enumerate((wk_ref, wv_ref))]
        return [pltpu.make_async_copy(src.at[rows, :], w_buf.at[slot, :, pl.ds(at, width)], wsem.at[slot, j])
                for j, (src, rows, at, width) in enumerate(places)]

    def norm_grad(turn, i, n_steps):
        slot = odd(i)
        wait_all(weight_rows(turn, i))

        @pl.when(nxt(i) < n_steps)
        def _():
            start_all(weight_rows(turn, nxt(i)))
        if turn == 0:
            dn_buf[:, part(i)] = lax.dot_general(
                own_buf[:, :TRIO * kv], w_buf[slot, :, :TRIO * kv], NT, preferred_element_type=F32)
            return
        for j in range(PAIR):
            block = i * 2 + j
            dn = dn_buf[:, part(block)] + lax.dot_general(
                own_buf[:, TRIO * kv:], w_buf[slot, :, pl.ds(j * PAIR * kv, PAIR * kv)], NT, preferred_element_type=F32)
            dn_buf[:, part(block)] = dn
            x_hat = x_ref[:, part(block)].astype(F32) * inv_rms()
            total = jnp.sum(dn * x_hat, **BY_COLUMN)
            for k in range(PAIR):
                part_buf[pl.ds(block * 2 + k, 1), :] = total[:, k * LANES:(k + 1) * LANES]

    def send_gain(step, carry):
        pltpu.make_async_remote_copy(
            part_buf, parts.at[me], gain_send, gain_recv,
            device_id=device_at(step), device_id_type=pl.DeviceIdType.MESH).start()
        return carry

    def all_gains():
        rest = parts.at[pl.ds(1, N_DEV - 1)]
        return pltpu.make_async_remote_copy(
            rest, rest, gain_send, gain_recv, device_id=net.device(c=1 - net.c), device_id_type=pl.DeviceIdType.MESH)

    def input_grad():
        x_hat = x_ref[ALL].astype(F32) * inv_rms()
        d_hat = dn_buf[ALL] * gain_buf[ALL]
        dx_ref[ALL] = (dy_ref[ALL].astype(F32) + inv_rms() * (
            d_hat - x_hat * jnp.mean(d_hat * x_hat, **BY_ROW))).astype(BF16)

    n_cols = x_ref.shape[1] // BLK

    def out_rows(i):
        slot = odd(i)
        head = lax.rem(i, 4) * 6 + lax.div(i, 4)
        return [pltpu.make_async_copy(
            wo_ref.at[part(head + TRIO * j, LANES), :], w_buf.at[slot, j * LANES:(j + 1) * LANES, :wo_ref.shape[1]], wsem.at[slot, j])
            for j in range(PAIR)]

    def out_part(i):
        slot = odd(i)
        wait_all(out_rows(i))

        @pl.when(nxt(i) < N_OUT)
        def _():
            start_all(out_rows(nxt(i)))
        left = oo_buf[:, part(i)]
        for j in range(n_cols):
            cols = slice(j * BLK, (j + 1) * BLK)
            term = jnp.dot(left, w_buf[slot, :, cols], preferred_element_type=F32)
            before = jnp.where(i == 0, x_ref[:, cols].astype(F32), s_buf[j, :LANES, :])
            s_buf[j, :LANES, :] = before + term

    def body(t, carry):
        n, loaded = carry
        since = t - ATTEND

        @pl.when(t == 1)
        def _():
            wo_rows(zero()).start()
            start_all(weights)

        @pl.when(t == SEND_DO + 1)
        def _():
            own_do.start()
            for step in range(1, 8):
                do_copy(step, True).start()
            wait_all(weights)

        @pl.when((since > 0) & (t <= ATTENDED) & (lax.rem(since, 4) == 0))
        def _():
            wait_all(step_pieces(since - 1))

        @pl.when(t == ATTENDED)
        def _():
            attn.key_grads(dkv_buf)

        @pl.when((t >= ATTENDED) & (t < ATTENDED + N_SEND))
        def _():
            start_all(key_copies(part(t - ATTENDED, QROWS // N_SEND)))

        @pl.when(t == KEYS_IN)
        def _():
            add_peers()
        net_in.tick(t, PAIR * N_IN, view_in)
        net.tick(t - START, N_UNIT, view)
        for s in range(N_STAGE + 2):
            @pl.when(t == s * LAG)
            def _(s=s):
                net_cs.advance(0, 'D', view_cs, s)

        @pl.when((t > 1) & (t <= N_PART + 1))
        def _():
            head_grad(t - 2)

        ahead = t - PROJECT + 1

        @pl.when(ahead == 0)
        def _():
            take_positions()
            angles(0)

        @pl.when((ahead >= 0) & (odd(ahead) == 0) & (ahead < PAIR * N_CHUNK))
        def _():
            chunk_rows(half_of(ahead)).start()

        @pl.when((ahead > 0) & (odd(ahead) == 1) & (ahead < PAIR * N_CHUNK))
        def _():
            project(half_of(ahead))

            @pl.when(half_of(ahead) + 1 < N_CHUNK)
            def _():
                angles(half_of(ahead) + 1)

        @pl.when(t == ATTEND)
        def _():
            own_do.wait()
            take_do()
            operand(zero()).start()
            dk_acc[ALL] = jnp.zeros_like(dk_acc)
            dv_acc[ALL] = jnp.zeros_like(dv_acc)

        @pl.when((t >= ATTEND) & (t < ATTENDED))
        def _():
            attn.step(since)

            @pl.when(lax.rem(since, 4) == 3)
            def _():
                start_all(step_pieces(since))

        complete = jnp.minimum(lax.div(jnp.maximum(t - START - (N_STAGE - 1) * LAG + 1, 0), UPP), IN_GATHER)
        load = (loaded < complete) & (loaded <= lax.div(n, N_TILE) + 1)

        @pl.when(load)
        def _():
            start_all(piece(loaded))

        @pl.when(t == QUERY_IN)
        def _():
            for step in range(1, 8):
                do_copy(step, True).wait_send()

        for turn, (tick, n_steps) in enumerate(((QUERY_IN, N_PART), (OWN_IN, N_PART // 2))):
            @pl.when(t == tick)
            def _(turn=turn):
                start_own(turn)
                start_all(weight_rows(turn, zero()))

            @pl.when(t == tick + 1)
            def _(turn=turn):
                wait_own(turn)

            @pl.when((t > tick) & (t <= tick + n_steps))
            def _(turn=turn, tick=tick, n_steps=n_steps):
                norm_grad(turn, t - tick - 1, n_steps)

        @pl.when(t == OWN_IN + N_PART // 2 + 1)
        def _():
            mine = pltpu.make_async_copy(part_buf, parts.at[me], rows_sem)
            mine.start()
            mine.wait()
            lax.fori_loop(1, N_DEV, send_gain, 0)
            input_grad()
            start_own(2)
            start_all(out_rows(zero()))

        @pl.when(t == OUT_IN)
        def _():
            wait_own(2)

        @pl.when((t >= OUT_IN) & (t < OUT_IN + N_OUT))
        def _():
            out_part(t - OUT_IN)

        n_end = jnp.minimum(jnp.minimum(n + 1, loaded * N_TILE), n_own)
        lax.fori_loop(n, n_end, tile, 0)
        return n_end, loaded + load.astype(jnp.int32)

    n, _ = loop(LAST + 1, body, (zero(), zero()))
    start_own(3)
    for j in range(n_cols):
        sum_ref[:, j * BLK:(j + 1) * BLK] = s_buf[j, :LANES, :]
    lax.fori_loop(n, n_own, tile, 0)
    all_gains().wait_recv()
    dgain_ref[ALL] = jnp.sum(parts[ALL], axis=0)
    for slot in range(TRIO):
        keep_tile(0, slot).wait()
        give_tile(0, slot).wait_send()

    def received(n, carry):
        give_tile(n, 0).wait_recv()
        return carry

    loop(n_own, received, 0)
    wait_own(3)
    for copy in key_copies(pl.ds(0, QROWS)):
        copy.wait_send()
    all_gains().wait_send()


def main(x, dy, gain, pos, freq, w_q, w_k, w_v, w_o):
    model = x.shape[1]
    qkv = w_q.shape[1] + w_k.shape[1] + w_v.shape[1]
    queries, keys = pltpu.VMEM((TRIO, QROWS, LANES), BF16), pltpu.VMEM((SEQ, LANES), BF16)
    return pl.pallas_call(
        main_kernel,
        out_shape=[like((PAIR, *GRID) + x.shape, BF16), like((*GRID, 8, LANES), F32),
                   like((N_PIECE, PAIR, QUAD, PAIR, PAIR, QROWS, LANES), BF16), like((N_GATHER, BLK, BLK), F32),
                   like((LANES, model // 3), BF16), like(x.shape, F32), like(x.shape, BF16), like((PAIR * N_PART, LANES), F32)],
        in_specs=[vmem_spec()] * 5 + [any_spec()] * 4,
        out_specs=[any_spec()] * 4 + [vmem_spec()] * 4,
        scratch_shapes=[
            pltpu.VMEM(x.shape, BF16), queries, queries, keys, keys,
            pltpu.VMEM((*GRID, CHUNK, model), BF16), pltpu.VMEM((8, LANES), F32), pltpu.VMEM((1, model), F32), pltpu.VMEM((1, LANES), F32),
            pltpu.VMEM((*GRID, 8, LANES), F32), pltpu.VMEM((PAIR, LANES, LANES), F32), pltpu.VMEM((N_DEV * CHUNK, LANES), F32),
            pltpu.VMEM((QROWS, LANES), F32), pltpu.VMEM((8, LANES, TRIO * LANES), BF16),
            pltpu.VMEM((PAIR, 3, QROWS, LANES), BF16), pltpu.VMEM((LANES, SEQ), F32), pltpu.VMEM((LANES, SEQ), F32),
            pltpu.VMEM((SEQ // BLK, BLK, BLK), F32), pltpu.VMEM((TRIO, BLK, LANES), F32),
            pltpu.VMEM((QUAD, PAIR, QROWS, LANES), BF16), pltpu.VMEM((TRIO, 2, QROWS, LANES), BF16),
            pltpu.VMEM((PAIR, SEQ, BLK), BF16), pltpu.VMEM((PAIR, *GRID, LANES, BLK), BF16), pltpu.VMEM((TRIO, BLK, BLK), F32),
            pltpu.VMEM((LANES, qkv), BF16), pltpu.VMEM((LANES, PAIR * w_k.shape[1]), BF16), pltpu.VMEM((PAIR, HALF, qkv), BF16), pltpu.VMEM(x.shape, F32),
            pltpu.VMEM((PAIR * N_PART, LANES), F32), pltpu.VMEM((N_DEV, PAIR * N_PART, LANES), F32),
            sems(1, N_SLOT), sems(1, N_SLOT), sems(RING, N_SLOT), sems(RING, N_SLOT),
            sems(TRIO), sems(TRIO), sems(), sems(8), sems(8),
            sems(N_PIECE, 2), sems(PAIR), sems(PAIR), sems(TRIO), sems(TRIO),
            sems(IN_GATHER * N_TILE), sems(TRIO), sems(TRIO), sems(QUAD), sems(PAIR, 4), sems(), sems()],
        compiler_params=pltpu.CompilerParams(collective_id=0, has_side_effects=True, vmem_limit_bytes=VMEM_LIMIT),
    )(x, dy, gain, pos, freq, w_q, w_k, w_v, w_o)


N_LATE = N_PIECE - IN_GATHER
GROUP = IN_GATHER // N_LATE


def finish_kernel(sum_ref, o_ref, dx_ref, dgain_ref, w_ref, hd_ref, g_ref, t_ref,
                  y_ref, dx_out, dgain_out, wq_ref, wk_ref, wv_ref, wo_ref,
                  gbuf, abuf, obuf, cbuf, acc, wbuf, gsem, asem, osem, isem, csem, wsem):
    n_step, group = N_LATE * PER_PIECE, GROUP

    def operand(t):
        return operand_copy(hd_ref, abuf, asem, 1, t, odd(t))

    def cut(t):
        return pl.ds(pl.multiple_of(t * BLK, BLK), BLK)

    def lanes(i):
        return pl.ds(pl.multiple_of(i * LANES, LANES), LANES)

    def to_output(p, t, sub, src, sem):
        j = jnp.where(p == O_PIECES[0], 0, p - O_PIECES[0] - 2)
        return [pltpu.make_async_copy(
            src.at[pl.ds(i * LANES, LANES), :], wo_ref.at[lanes(TRIO * (sub * 4 + i) + j), cut(t)], sem.at[i])
            for i in range(QUAD)]

    def to_input(dst, place, t, sub, src, sem):
        return [pltpu.make_async_copy(
            src.at[:, pl.ds(i * LANES, LANES)], dst.at[cut(t), lanes(place(sub * 4 + i))], sem.at[i]) for i in range(QUAD)]

    def ins(n):
        return [pltpu.make_async_copy(t_ref.at[n * group + i], cbuf.at[lax.rem(n, TRIO), i], isem.at[lax.rem(n, TRIO), i])
                for i in range(group)]

    def start_outs(n):
        for i in range(group):
            m = n * group + i
            p, t, sub = lax.div(m, PER_PIECE), lax.rem(half_of(m), N_TILE), odd(m)
            src, sem = cbuf.at[lax.rem(n, TRIO), i], csem.at[lax.rem(n, TRIO), i]
            for cond, copies in (
                (p < 3, lambda: to_input(wq_ref, lambda g: TRIO * g + p, t, sub, src, sem)),
                (p == KEY_PIECE, lambda: to_input(wk_ref, lambda g: g, t, sub, src, sem)),
                (p == KEY_PIECE + 1, lambda: to_input(wv_ref, lambda g: g, t, sub, src, sem)),
                ((p == O_PIECES[0]) | (p == O_PIECES[1]), lambda: to_output(p, t, sub, src, sem)),
            ):
                @pl.when(cond)
                def _(copies=copies):
                    for c in copies():
                        c.start()

    def wait_outs(n):
        for i in range(group):
            for c in to_output(IN_GATHER, 0, 0, cbuf.at[0, i], csem.at[lax.rem(n, TRIO), i]):
                c.wait()

    def weight(i):
        slot = odd(i)
        return pltpu.make_async_copy(w_ref.at[lanes(TRIO * i + 2), :], wbuf.at[slot], wsem.at[slot])

    for late in range(N_LATE):
        for sub in range(PAIR):
            start_all(piece_copies(g_ref, gbuf, gsem, IN_GATHER + late, sub, late * 2 + sub))
    operand(zero()).start()
    weight(zero()).start()
    acc[ALL] = sum_ref[ALL]
    dx_out[ALL] = dx_ref[ALL]
    dgain_out[ALL] = dgain_ref[ALL]

    def step(n, carry):
        t, late, sub = lax.div(n, PAIR * N_LATE), lax.rem(half_of(n), N_LATE), odd(n)
        p, held = IN_GATHER + late, late * 2 + sub
        slot = lax.rem(n, TRIO)

        @pl.when(n >= 3)
        def _():
            wait_outs(n - 3)
        for c in ins(n):
            c.start()

        @pl.when(n >= 1)
        def _():
            for c in ins(n - 1):
                c.wait()
            start_outs(n - 1)

        @pl.when(held == 0)
        def _():
            operand(t).wait()

            @pl.when(nxt(t) < N_TILE)
            def _():
                operand(nxt(t)).start()

        @pl.when(n < PAIR * N_LATE)
        def _():
            wait_piece(gbuf, gsem, held)

        @pl.when(n >= 3)
        def _():
            for c in to_output(IN_GATHER, 0, 0, obuf.at[0], osem.at[slot]):
                c.wait()
        @pl.when(n < 8)
        def _():
            weight(n).wait()

            @pl.when(n < 7)
            def _():
                weight(n + 1).start()
            acc[ALL] += jnp.dot(o_ref[:, lanes(n)], wbuf[odd(n)], preferred_element_type=F32)
        obuf[slot] = tile_product(abuf[odd(t)], gbuf[held], True)
        for c in to_output(p, t, sub, obuf.at[slot], osem.at[slot]):
            c.start()
        return carry

    loop(n_step, step, 0)
    y_ref[ALL] = acc[ALL].astype(BF16)
    for c in ins(n_step - 1):
        c.wait()
    start_outs(jnp.int32(n_step - 1))
    for n in range(n_step - 3, n_step):
        wait_outs(n)
        for c in to_output(IN_GATHER, 0, 0, obuf.at[0], osem.at[n % 3]):
            c.wait()


def finish(x, o, dx, dgain, w_o, hd, g, tiles):
    model, kv = hd.shape[2], 8 * LANES
    return pl.pallas_call(
        finish_kernel,
        out_shape=[like(x.shape, BF16), like(dx.shape, BF16), like(dgain.shape, F32)]
        + [like((model, n), F32) for n in (TRIO * kv, kv, kv)] + [like((TRIO * kv, model), F32)],
        in_specs=[vmem_spec()] * 4 + [any_spec()] * 4,
        out_specs=[vmem_spec()] * 3 + [any_spec()] * 4,
        scratch_shapes=[pltpu.VMEM((PAIR * N_LATE, SEQ, BLK), BF16), pltpu.VMEM((PAIR, SEQ, BLK), BF16), pltpu.VMEM((TRIO, BLK, BLK), F32),
                        pltpu.VMEM((TRIO, GROUP, BLK, BLK), F32), pltpu.VMEM(x.shape, F32), pltpu.VMEM((PAIR, LANES, model), BF16),
                        sems(PAIR * N_LATE), sems(PAIR), sems(TRIO, 4), sems(TRIO, GROUP), sems(TRIO, GROUP, 4), sems(PAIR)],
        cost_estimate=pl.CostEstimate(flops=4 * SEQ * kv * model, bytes_accessed=250 * 2**20, transcendentals=0),
        compiler_params=pltpu.CompilerParams(vmem_limit_bytes=VMEM_LIMIT),
    )(x, o, dx, dgain, w_o, hd, g, tiles)


def solution(mesh):
    assert mesh.shape['hp'] == 4 and mesh.shape['cp'] == 8

    def device_step(hidden, grad_out, positions, norm_gain, w_q, w_k, w_v, w_o, inv_freq):
        model = hidden.shape[1]
        hd, _, gathered, tiles, o_own, total, dx, gains = main(
            hidden, grad_out, norm_gain, positions, inv_freq, w_q, w_k, w_v, w_o)
        output, grad_hidden, grad_gain, grad_wq, grad_wk, grad_wv, grad_wo = finish(
            total, o_own, dx, gains, w_o, hd.reshape(2, SEQ, model), gathered, tiles)
        grad_gain = grad_gain.reshape(-1)
        return output, grad_hidden, grad_wq, grad_wk, grad_wv, grad_wo, grad_gain

    rows, whole = P(('cp', 'hp'), None), P()
    return jax.shard_map(
        device_step, mesh=mesh,
        in_specs=(rows, rows, P(('cp', 'hp')), whole, whole, whole, whole, whole, whole),
        out_specs=(rows, rows, whole, whole, whole, whole, whole), check_vma=False)
```

```python
import functools
import jax
import jax.numpy as jnp
from jax import lax
from jax.experimental import pallas as pl
from jax.experimental.pallas import tpu as pltpu
from jax.sharding import PartitionSpec as P

NORM_EPS = 1e-5
ALL = Ellipsis
EVERY = slice(None)
PAIR, TRIO, QUAD = 2, 3, 4
GRID = (PAIR, PAIR, PAIR, QUAD)
BY_COLUMN = {'axis': 0, 'keepdims': True}
BY_ROW = {'axis': 1, 'keepdims': True}
F32 = jnp.float32
BF16 = jnp.bfloat16
LANES = 128
BLK = 512
HALF = BLK // 2
SEQ = 8 * BLK
QROWS = PAIR * BLK
UPP = 8
LAG = 2
RING = 20
VMEM_LIMIT = 64 * 2**20 - 2**16
NT = (((1,), (1,)), ((), ()))
TN = (((0,), (0,)), ((), ()))

STAGES = {
    'C': ('z1', 'z2', 'z3', 'y', 'x', 'd'),
    'D': ('z1', 'z2', 'z3', 'x', 'y', 'd'),
    'E': ('x', 'y', 'z1', 'z2', 'z3', 'd'),
    'F': ('y', 'x', 'z1', 'z2', 'z3', 'd'),
}
SLOT = {'z1': 0, 'z2': 2, 'z3': 4, 'x': 6, 'y': 7, 'd': 8}
N_STAGE = 6
N_SLOT = 9


def odd(i):
    return lax.rem(i, PAIR)


def half_of(i):
    return lax.div(i, PAIR)


def nxt(i):
    return i + 1


def zero():
    return jnp.int32(0)


def loop(n, body, init):
    return lax.fori_loop(0, n, body, init)


class Gather:
    def __init__(self, send_sem, recv_sem, mix, base=0):
        self.mix, self.base = mix, base
        self.z = lax.axis_index('hp')
        cp = lax.axis_index('cp')
        self.c, self.x, self.y = odd(cp), odd(half_of(cp)), lax.div(cp, 4)
        self.send_sem, self.recv_sem = send_sem, recv_sem

    def device(self, **moved):
        at = {name: moved.get(name, getattr(self, name)) for name in 'cxyz'}
        return at['z'], (at['y'] * PAIR + at['x']) * PAIR + at['c']

    def copies(self, sem_row, kind, view, stage):
        c, x, y, z = self.c, self.x, self.y, self.z
        order = STAGES[kind]
        done = {st[0] for st in order[:order.index(stage)]}
        every = EVERY
        gx, gy, gz = (every if d in done else v for d, v in (('x', x), ('y', y), ('z', z)))
        slot = SLOT[stage]

        def copy(place, device, slot):
            return lambda: pltpu.make_async_remote_copy(
                place, place, self.send_sem.at[sem_row, slot], self.recv_sem.at[sem_row, slot],
                device_id=device, device_id_type=pl.DeviceIdType.MESH)

        if stage == 'x':
            dev = self.device(x=1 - x)
            return [(None, copy(view(c, x, gy, gz), dev, slot), None, copy(view(c, 1 - x, gy, gz), dev, slot))]
        if stage == 'y':
            dev = self.device(y=1 - y)
            return [(None, copy(view(c, gx, y, gz), dev, slot), None, copy(view(c, gx, 1 - y, gz), dev, slot))]
        if stage == 'd':
            dev = self.device(c=1 - c)
            return [(None, copy(view(c, every, every, every), dev, slot),
                     None, copy(view(1 - c, every, every, every), dev, slot))]
        hop = int(stage[1])
        up, down = self.device(z=jnp.minimum(z + 1, 3)), self.device(z=jnp.maximum(z - 1, 0))
        return [
            ((z >= hop - 1) & (z < 3), copy(view(c, gx, gy, jnp.maximum(z - hop + 1, 0)), up, slot),
             z >= hop, copy(view(c, gx, gy, jnp.maximum(z - hop, 0)), up, slot)),
            ((z + hop <= 4) & (z > 0), copy(view(c, gx, gy, jnp.minimum(z + hop - 1, 3)), down, slot + 1),
             z + hop <= 3, copy(view(c, gx, gy, jnp.minimum(z + hop, 3)), down, slot + 1)),
        ]

    def run(self, sem_row, kind, view, stage, what):
        for can_send, send, can_recv, recv in self.copies(sem_row, kind, view, stage):
            cond = can_recv if what == 'recv' else can_send

            def act(send=send, recv=recv):
                if what == 'start':
                    send().start()
                elif what == 'sent':
                    send().wait_send()
                else:
                    recv().wait_recv()

            if cond is None:
                act()
            else:
                pl.when(cond)(act)

    def advance(self, sem_row, kind, view, s):
        if 0 < s <= N_STAGE:
            self.run(sem_row, kind, view, STAGES[kind][s - 1], 'recv')
        if s < N_STAGE:
            self.run(sem_row, kind, view, STAGES[kind][s], 'start')
        if s > N_STAGE:
            for stage in STAGES[kind]:
                self.run(sem_row, kind, view, stage, 'sent')

    def kinds(self, u):
        word, at = lax.div(u, 16), lax.rem(u, 16)
        code = jnp.int32(self.mix[0])
        for i in range(1, len(self.mix)):
            code = jnp.where(word == i, self.mix[i], code)
        code = lax.shift_right_logical(code, at * 2) & 3
        return tuple((kind, code == i) for i, kind in enumerate('CDEF'))

    def tick(self, t, n_units, view):
        for s in range(N_STAGE + 2):
            u = t - s * LAG

            @pl.when((u >= 0) & (u < n_units))
            def _(u=u, s=s):
                for kind, is_kind in self.kinds(u):
                    @pl.when(is_kind)
                    def _(kind=kind):
                        self.advance(lax.rem(u + self.base, RING), kind, view(u), s)


def turn(v):
    return pltpu.roll(v, LANES // 2, 1)


def low_lanes(shape):
    return lax.broadcasted_iota(jnp.int32, shape, 1) < LANES // 2


def cos_sin(cs):
    low = low_lanes(cs.shape)
    other = turn(cs)
    return jnp.where(low, cs, other), jnp.where(low, -other, cs)


def any_spec():
    return pl.BlockSpec(memory_space=pl.ANY)


def vmem_spec():
    return pl.BlockSpec(memory_space=pltpu.VMEM)


def sems(*shape):
    return pltpu.SemaphoreType.DMA(shape) if shape else pltpu.SemaphoreType.DMA


def like(shape, dtype):
    return jax.ShapeDtypeStruct(shape, dtype)


def start_all(copies):
    for copy in copies:
        copy.start()


def wait_all(copies):
    for copy in copies:
        copy.wait()


N_PIECE = 8
O_PIECES = (3, 6, 7)
KEY_PIECE = 4
N_TILE = 6
PER_PIECE = PAIR * N_TILE
IN_GATHER = 7
N_GATHER = IN_GATHER * PER_PIECE


def tile_product(operand, piece, of_output):
    left, right = (piece, operand) if of_output else (operand, piece)
    return lax.dot_general(left, right, TN, preferred_element_type=F32)


def operand_copy(hd_ref, abuf, asem, which, t, slot):
    return pltpu.make_async_copy(
        hd_ref.at[which, :, pl.ds(pl.multiple_of(t * BLK, BLK), BLK)], abuf.at[slot], asem.at[slot])


def piece_copies(g_ref, gbuf, gsem, p, core, slot):
    return [pltpu.make_async_copy(g_ref.at[p, core, z, r // 2, r % 2],
                                  gbuf.at[slot, pl.ds(r * QROWS, QROWS), pl.ds(z * LANES, LANES)], gsem.at[slot])
            for z in range(QUAD) for r in range(QUAD)]


def wait_piece(gbuf, gsem, slot):
    pltpu.make_async_copy(gbuf.at[slot], gbuf.at[slot], gsem.at[slot]).wait()


def lane_groups(op, s):
    out = s[:, :LANES]
    for i in range(1, s.shape[1] // LANES):
        out = op(out, s[:, i * LANES:(i + 1) * LANES])
    return out


class Attention:
    def __init__(self, q, do, k, v, cs, out, dk_acc, dv_acc, s, state, quarter):
        self.q, self.do, self.k, self.v, self.cs, self.out = q, do, k, v, cs, out
        self.dk, self.dv, self.s, self.state = dk_acc, dv_acc, s, state
        self.quarter = quarter
        self.scale = LANES ** -0.5
        self.factor = self.scale * 1.4426950408889634

    def step(self, t):
        head, half = lax.div(t, 8), odd(lax.div(t, 4))
        n_key = jnp.where(half == 0, self.quarter + 1, SEQ // BLK - self.quarter)
        rows = pl.ds(pl.multiple_of(half * BLK, BLK), BLK)
        for i, act in enumerate((self.scores, self.exps, self.values, self.grads)):
            @pl.when(lax.rem(t, 4) == i)
            def _(act=act):
                act(head, half, n_key, rows)

    def keys(self, kb):
        return pl.ds(pl.multiple_of(kb * BLK, BLK), BLK)

    def zeros(self):
        return jnp.zeros((BLK, LANES), F32)

    def keep(self, i, column):
        self.state[i] = jnp.broadcast_to(column, (BLK, LANES))

    def kept(self, i):
        return self.state[i, :, :1]

    def scores(self, head, half, n_key, rows):
        q = self.q[head, rows, :]

        def block(kb, m, diagonal=False):
            s = lax.dot_general(q, self.k[self.keys(kb), :], NT, preferred_element_type=F32)
            if diagonal:
                visible = lax.broadcasted_iota(jnp.int32, s.shape, 0) >= lax.broadcasted_iota(jnp.int32, s.shape, 1)
                s = jnp.where(visible, s, -1e30)
            self.s[kb] = s
            return jnp.maximum(m, lane_groups(jnp.maximum, s))

        m = loop(n_key - 1, block, self.zeros() - 1e30)
        m = block(n_key - 1, m, diagonal=True)
        self.keep(0, jnp.max(m, **BY_ROW) * self.factor)

    def exps(self, head, half, n_key, rows):
        m = self.kept(0)

        def block(kb, total):
            e = jnp.exp2(self.s[kb] * self.factor - m)
            self.s[kb] = e
            return total + lane_groups(jnp.add, e)

        total = loop(n_key, block, self.zeros())
        self.keep(0, 1.0 / jnp.sum(total, **BY_ROW))

    def sides(self, half):
        for side in range(PAIR):
            place = (half * (1 - side) + (1 - half) * side) * HALF
            yield pl.ds(pl.multiple_of(place, HALF), HALF), pl.ds(pl.multiple_of(side * BLK + half * HALF, HALF), HALF)

    def values(self, head, half, n_key, rows):
        do, inv = self.do[head, rows, :], self.kept(0)
        turned = do.T

        def block(kb, o):
            p = (self.s[kb] * inv).astype(BF16)
            self.dv[:, self.keys(kb)] += jnp.dot(turned, p, preferred_element_type=F32)
            return o + jnp.dot(p, self.v[self.keys(kb), :], preferred_element_type=F32)

        o = loop(n_key, block, self.zeros()).astype(BF16).astype(F32)
        self.keep(1, jnp.sum(do.astype(F32) * o, **BY_ROW))
        self.state[2] = o
        for place, stored in self.sides(half):
            self.out[1, head, stored, :] = self.state[2, place, :].astype(BF16)

    def grads(self, head, half, n_key, rows):
        do, inv, delta = self.do[head, rows, :], self.kept(0), self.kept(1)
        turned = self.q[head, rows, :].T

        def block(kb, dq):
            dp = lax.dot_general(do, self.v[self.keys(kb), :], NT, preferred_element_type=F32)
            ds = (self.s[kb] * inv * (dp - delta)).astype(BF16)
            self.dk[:, self.keys(kb)] += jnp.dot(turned, ds, preferred_element_type=F32)
            return dq + jnp.dot(ds, self.k[self.keys(kb), :], preferred_element_type=F32)

        dq = loop(n_key, block, self.zeros()) * self.scale
        self.state[2] = dq.astype(BF16).astype(F32)
        for place, stored in self.sides(half):
            cos, sin = cos_sin(self.cs[stored, :])
            part = self.state[2, place, :]
            self.out[0, head, stored, :] = (part * cos - turn(part) * sin).astype(BF16)

    def key_grads(self, out):
        for pair in range(8):
            for i, (acc, factor) in enumerate(((self.dk, self.scale), (self.dv, 1.0))):
                for part, block in enumerate((pair, 15 - pair)):
                    out[pair // 2, i, pl.ds(pair % PAIR * BLK + part * HALF, HALF), :] = (
                        acc[:, pl.ds(block * HALF, HALF)].T * factor).astype(BF16)


ROWS_UNIT = 8
N_IN = LANES // ROWS_UNIT
N_STEP = 24
N_UNIT = N_PIECE * UPP
N_PART = 12
SEND_DO = N_PART + 1
DELAY = N_STAGE * LAG
CHUNK = PAIR * ROWS_UNIT
N_CHUNK = LANES // CHUNK
PROJECT = DELAY + 2
ATTEND = PROJECT + PAIR * N_CHUNK - 1
ATTENDED = ATTEND + N_STEP
START = ATTEND + 4
N_SEND = 8
KEYS_IN = START + KEY_PIECE * UPP
QUERY_IN = START + 3 * UPP + DELAY
OWN_IN = START + O_PIECES[1] * UPP + DELAY
OUT_IN = OWN_IN + N_PART // 2 + 2
N_OUT = 8
LAST = START + N_UNIT + DELAY + LAG
N_DEV = 32


def main_kernel(x_ref, dy_ref, gain_ref, mypos_ref, freq_ref, wq_ref, wk_ref, wv_ref, wo_ref,
                hd_ref, pos_ref, g_ref, t_ref, o_ref, sum_ref, dx_ref, dgain_ref,
                h_buf, q_buf, do_buf, k_buf, v_buf, rows_buf, mypos_buf, gain_buf, freq_buf, pos_buf, pos_t, cs_buf, own_cs, do_parts,
                piece_buf, dk_acc, dv_acc, s_buf, state, dkv_buf, peer_buf, gbuf, abuf, obuf, own_buf, oo_buf, w_buf, dn_buf, part_buf, parts,
                cs_send, cs_recv, send_sem, recv_sem, first_sem, proj_sem, rows_sem, do_send, do_recv,
                lsem, gsem, asem, osem, tsend, trecv, psend, precv, rsem, wsem, gain_send, gain_recv):
    net_in, net_cs, net = Gather(send_sem, recv_sem, (293880977, 1175604295)), Gather(cs_send, cs_recv, (293880977, 1175604295)), Gather(send_sem, recv_sem, (-398134202, 303174049, 1212958790, -1471626106), START)
    quarter = net.y * 2 + net.x
    head = net.c * 4 + net.z
    spot = (net.y, net.x, net.c, net.z)
    attn = Attention(q_buf, do_buf, k_buf, v_buf, own_cs, piece_buf, dk_acc, dv_acc, s_buf, state, quarter)

    def inv_rms():
        x = x_ref[ALL].astype(F32)
        return lax.rsqrt(jnp.mean(x * x, **BY_ROW) + NORM_EPS)

    me = lax.axis_index('cp') * 4 + net.z

    def device_at(step):
        other = lax.rem(me + step, N_DEV)
        return lax.rem(other, 4), lax.div(other, 4)

    barrier = pltpu.get_barrier_semaphore()

    def greet(step, carry):
        pl.semaphore_signal(barrier, inc=1, device_id=device_at(step), device_id_type=pl.DeviceIdType.MESH)
        return carry

    lax.fori_loop(1, N_DEV, greet, 0)

    gain_buf[ALL] = gain_ref[ALL].astype(F32).reshape(gain_buf.shape)
    freq_buf[ALL] = jnp.concatenate([freq_ref[ALL], freq_ref[ALL]], axis=0).reshape(freq_buf.shape)
    mypos_buf[ALL] = jnp.broadcast_to(mypos_ref[ALL].astype(F32).reshape(1, LANES), mypos_buf.shape)
    h_buf[ALL] = (x_ref[ALL].astype(F32) * inv_rms() * gain_buf[ALL]).astype(BF16)
    first = [pltpu.make_async_copy(src, dst, first_sem.at[i]) for i, (src, dst) in enumerate((
        (h_buf, hd_ref.at[(0, *spot)]), (dy_ref, hd_ref.at[(1, *spot)]), (mypos_buf, pos_ref.at[spot])))]
    start_all(first)
    wait_all(first)
    pl.semaphore_wait(barrier, N_DEV - 1)
    q_cols = pl.ds(pl.multiple_of(head * TRIO * LANES, LANES), TRIO * LANES)
    kv_cols = pl.ds(pl.multiple_of(head * LANES, LANES), LANES)
    w_rows = slice(0, wq_ref.shape[0])
    wq_buf, wkv_buf = gbuf.at[0, w_rows, :TRIO * LANES], gbuf.at[1, w_rows, :PAIR * LANES]
    weights = [pltpu.make_async_copy(src, dst, proj_sem.at[i]) for i, (src, dst) in enumerate((
        (wq_ref.at[:, q_cols], wq_buf), (wk_ref.at[:, kv_cols], gbuf.at[1, w_rows, :LANES]),
        (wv_ref.at[:, kv_cols], gbuf.at[1, w_rows, LANES:PAIR * LANES])))]

    def view_in(u):
        rows = pl.ds(pl.multiple_of(lax.rem(u, N_IN) * ROWS_UNIT, ROWS_UNIT), ROWS_UNIT)
        which = lax.div(u, N_IN)
        return lambda c, x, y, z: hd_ref.at[which, y, x, c, z, rows, :]

    def view_cs(c, x, y, z):
        return pos_ref.at[y, x, c, z]

    def part(i, width=HALF):
        return pl.ds(pl.multiple_of(i * width, width), width)

    def wo_rows(i):
        slot = odd(i)
        return pltpu.make_async_copy(wo_ref.at[part(i), :], w_buf.at[slot, :, :wo_ref.shape[1]], wsem.at[slot, 0])

    def head_grad(i):
        slot = odd(i)
        wo_rows(i).wait()

        @pl.when(nxt(i) < N_PART)
        def _():
            wo_rows(nxt(i)).start()
        own_buf[:, part(i)] = lax.dot_general(
            dy_ref[ALL], w_buf[slot, :, :wo_ref.shape[1]], NT, preferred_element_type=F32).astype(BF16)

    def do_copy(step, mine):
        me = net.c * 4 + net.z
        other = lax.rem(me + step, 8)
        slot = me if mine else lax.rem(me + 8 - step, 8)
        return pltpu.make_async_remote_copy(
            own_buf.at[:, part(other, TRIO * LANES)], do_parts.at[slot], do_send.at[step], do_recv.at[step],
            device_id=net.device(c=lax.div(other, 4), z=lax.rem(other, 4)), device_id_type=pl.DeviceIdType.MESH)

    own_do = pltpu.make_async_copy(own_buf.at[:, part(head, TRIO * LANES)], do_parts.at[head], do_send.at[0])

    def query_row(c, z):
        return c * HALF + z * LANES if z < 2 else BLK + (1 - c) * HALF + (z - 2) * LANES

    def take_do():
        for step in range(1, 8):
            do_copy(step, False).wait_recv()
        for c in range(PAIR):
            for z in range(QUAD):
                for j in range(TRIO):
                    do_buf[j, pl.ds(query_row(c, z), LANES), :] = do_parts[c * 4 + z, :, j * LANES:(j + 1) * LANES]

    every = EVERY

    def chunk(k, base=0):
        return pl.ds(pl.multiple_of(base + k * CHUNK, CHUNK), CHUNK)

    def chunk_rows(k):
        return pltpu.make_async_copy(hd_ref.at[0, every, every, every, every, chunk(k), every], rows_buf, rows_sem)

    def take_positions():
        copy = pltpu.make_async_copy(pos_ref, pos_buf, rows_sem)
        copy.start()
        copy.wait()
        for i in range(PAIR):
            pos_t[i] = pos_buf[i].reshape(LANES, LANES).T

    def angles(k):
        for dev in range(N_DEV):
            column = pos_t[dev // 16, chunk(k), dev % 16 * 8:dev % 16 * 8 + 1]
            cs_buf[dev * CHUNK:(dev + 1) * CHUNK, :] = jnp.broadcast_to(column, (CHUNK, LANES)) * freq_buf[ALL]
        angle = cs_buf[ALL]
        cs_buf[ALL] = jnp.where(low_lanes(angle.shape), jnp.cos(angle), jnp.sin(angle))

    def rotate(v, cs):
        cos, sin = cos_sin(cs)
        return (v * cos + turn(v) * sin).astype(BF16)

    def project(k):
        chunk_rows(k).wait()
        n_rows = N_DEV * CHUNK
        kv = jnp.dot(rows_buf[ALL].reshape(n_rows, -1), wkv_buf[ALL], preferred_element_type=F32)
        key = rotate(kv[:, :LANES], cs_buf[ALL])
        value = kv[:, LANES:].astype(BF16)
        for cp in range(8):
            for z in range(QUAD):
                block = 2 * cp + z if z < 2 else 28 - 2 * cp + z
                rows = slice((cp * 4 + z) * CHUNK, (cp * 4 + z + 1) * CHUNK)
                k_buf[chunk(k, block * LANES), :] = key[rows]
                v_buf[chunk(k, block * LANES), :] = value[rows]
        mine, cs = rows_buf[net.y, net.x].reshape(LANES, -1), cs_buf[part(quarter, LANES), :]
        q = jnp.dot(mine, wq_buf[ALL], preferred_element_type=F32)
        for j in range(TRIO):
            p = rotate(q[:, j * LANES:(j + 1) * LANES], cs)
            for c in range(PAIR):
                for z in range(QUAD):
                    rows = slice((c * 4 + z) * CHUNK, (c * 4 + z + 1) * CHUNK)
                    q_buf[j, chunk(k, query_row(c, z)), :] = p[rows]
                    if j == 0:
                        own_cs[chunk(k, c * BLK + z * LANES), :] = cs[rows]

    def local(p, i, src, rows=pl.ds(0, QROWS)):
        return pltpu.make_async_copy(src, g_ref.at[p, net.c, net.z, net.y, net.x, rows, :], lsem.at[p, i])

    def step_pieces(step):
        head, half = lax.div(step, 8), odd(lax.div(step, 4))
        out_piece = jnp.where(head == 0, O_PIECES[0], O_PIECES[0] + 2 + head)
        return [local(p, side, piece_buf.at[i, head, rows], rows) for i, p in ((0, head), (1, out_piece))
                for side, (_, rows) in enumerate(attn.sides(half))]

    def key_copies(rows):
        for i, moved in enumerate(('x', 'y', 'xy')):
            x, y = (1 - at if name in moved else at for name, at in (('x', net.x), ('y', net.y)))
            yield pltpu.make_async_remote_copy(
                dkv_buf.at[y * 2 + x, :, rows], peer_buf.at[i, :, rows], psend.at[i], precv.at[i],
                device_id=net.device(x=x, y=y), device_id_type=pl.DeviceIdType.MESH)

    def add_peers():
        for copy in key_copies(pl.ds(0, QROWS)):
            copy.wait_recv()
        total = dkv_buf[quarter].astype(F32)
        for i in range(TRIO):
            total = total + peer_buf[i].astype(F32)
        total = total.astype(BF16)
        cos, sin = cos_sin(own_cs[ALL])
        dk = total[0].astype(F32)
        piece_buf[0, 0] = (dk * cos - turn(dk) * sin).astype(BF16)
        piece_buf[0, 1] = total[1]
        kv = [local(KEY_PIECE + i, 0, piece_buf.at[0, i]) for i in range(PAIR)]
        start_all(kv)
        wait_all(kv)

    def view(u):
        p, k = lax.div(u, UPP), lax.rem(u, UPP)
        two = half_of(k)
        rows = part(odd(two) * 4 + half_of(two) * 2 + odd(k), QROWS // UPP)
        return lambda c, x, y, z: g_ref.at[p, c, z, y, x, rows, :]

    def place(n):
        return lax.div(n, N_TILE) * PER_PIECE + lax.rem(n, N_TILE) * 2 + net.c

    def keep_tile(n, slot):
        return pltpu.make_async_copy(obuf.at[slot], t_ref.at[place(n)], osem.at[slot])

    def give_tile(n, slot):
        return pltpu.make_async_remote_copy(
            obuf.at[slot], t_ref.at[place(n)], tsend.at[slot], trecv.at[n],
            device_id=net.device(c=1 - net.c), device_id_type=pl.DeviceIdType.MESH)

    def of_output(p):
        return (p == O_PIECES[0]) | (p == O_PIECES[1])

    def operand(n):
        which, slot = of_output(lax.div(n, N_TILE)).astype(jnp.int32), odd(n)
        return pltpu.make_async_copy(
            hd_ref.at[which, every, every, every, every, every, part(lax.rem(n, N_TILE), BLK)], abuf.at[slot], asem.at[slot])

    def piece(p):
        return piece_copies(g_ref, gbuf, gsem, p, net.c, odd(p))

    n_own = IN_GATHER * N_TILE

    def tile(n, carry):
        slot = lax.rem(n, TRIO)
        p = lax.div(n, N_TILE)

        @pl.when(lax.rem(n, N_TILE) == 0)
        def _():
            wait_piece(gbuf, gsem, odd(p))
        operand(n).wait()

        @pl.when(nxt(n) < n_own)
        def _():
            operand(nxt(n)).start()

        @pl.when(n >= 3)
        def _():
            keep_tile(n, slot).wait()
            give_tile(n, slot).wait_send()
        for output in (False, True):
            @pl.when(of_output(p) == output)
            def _(output=output):
                obuf[slot] = tile_product(abuf[odd(n)].reshape(SEQ, BLK), gbuf[odd(p)], output)
        keep_tile(n, slot).start()
        give_tile(n, slot).start()
        return carry

    kv = wk_ref.shape[1]
    groups = (((0, 1, 2), own_buf, slice(0, TRIO * kv)), ((KEY_PIECE, KEY_PIECE + 1), own_buf, slice(TRIO * kv, 5 * kv)),
              (O_PIECES[:2], oo_buf, slice(0, PAIR * kv)), (O_PIECES[2:], o_ref, slice(0, kv)))

    def start_own(i):
        rows = pl.ds(pl.multiple_of(net.c * BLK + net.z * LANES, LANES), LANES)
        pieces, dst, cols = groups[i]
        for k, p in enumerate(pieces):
            for g in range(8):
                col = cols.start // LANES + (TRIO * g + k if len(pieces) == 3 else 8 * k + g)
                pltpu.make_async_copy(
                    g_ref.at[p, g // 4, g % 4, net.y, net.x, rows, :], dst.at[:, pl.ds(col * LANES, LANES)], rsem.at[i]).start()

    def wait_own(i):
        _, dst, cols = groups[i]
        pltpu.make_async_copy(dst.at[:, cols], dst.at[:, cols], rsem.at[i]).wait()

    def weight_rows(turn, i):
        slot = odd(i)
        if turn == 0:
            places = ((wq_ref, part(i), 0, TRIO * kv),)
        else:
            places = [(src, part(i * 2 + j), (j * 2 + k) * kv, kv) for j in range(PAIR) for k, src in enumerate((wk_ref, wv_ref))]
        return [pltpu.make_async_copy(src.at[rows, :], w_buf.at[slot, :, pl.ds(at, width)], wsem.at[slot, j])
                for j, (src, rows, at, width) in enumerate(places)]

    def norm_grad(turn, i, n_steps):
        slot = odd(i)
        wait_all(weight_rows(turn, i))

        @pl.when(nxt(i) < n_steps)
        def _():
            start_all(weight_rows(turn, nxt(i)))
        if turn == 0:
            dn_buf[:, part(i)] = lax.dot_general(
                own_buf[:, :TRIO * kv], w_buf[slot, :, :TRIO * kv], NT, preferred_element_type=F32)
            return
        for j in range(PAIR):
            block = i * 2 + j
            dn = dn_buf[:, part(block)] + lax.dot_general(
                own_buf[:, TRIO * kv:], w_buf[slot, :, pl.ds(j * PAIR * kv, PAIR * kv)], NT, preferred_element_type=F32)
            dn_buf[:, part(block)] = dn
            x_hat = x_ref[:, part(block)].astype(F32) * inv_rms()
            total = jnp.sum(dn * x_hat, **BY_COLUMN)
            for k in range(PAIR):
                part_buf[pl.ds(block * 2 + k, 1), :] = total[:, k * LANES:(k + 1) * LANES]

    def send_gain(step, carry):
        pltpu.make_async_remote_copy(
            part_buf, parts.at[me], gain_send, gain_recv,
            device_id=device_at(step), device_id_type=pl.DeviceIdType.MESH).start()
        return carry

    def all_gains():
        rest = parts.at[pl.ds(1, N_DEV - 1)]
        return pltpu.make_async_remote_copy(
            rest, rest, gain_send, gain_recv, device_id=net.device(c=1 - net.c), device_id_type=pl.DeviceIdType.MESH)

    def input_grad():
        x_hat = x_ref[ALL].astype(F32) * inv_rms()
        d_hat = dn_buf[ALL] * gain_buf[ALL]
        dx_ref[ALL] = (dy_ref[ALL].astype(F32) + inv_rms() * (
            d_hat - x_hat * jnp.mean(d_hat * x_hat, **BY_ROW))).astype(BF16)

    n_cols = x_ref.shape[1] // BLK

    def out_rows(i):
        slot = odd(i)
        head = lax.rem(i, 4) * 6 + lax.div(i, 4)
        return [pltpu.make_async_copy(
            wo_ref.at[part(head + TRIO * j, LANES), :], w_buf.at[slot, j * LANES:(j + 1) * LANES, :wo_ref.shape[1]], wsem.at[slot, j])
            for j in range(PAIR)]

    def out_part(i):
        slot = odd(i)
        wait_all(out_rows(i))

        @pl.when(nxt(i) < N_OUT)
        def _():
            start_all(out_rows(nxt(i)))
        left = oo_buf[:, part(i)]
        for j in range(n_cols):
            cols = slice(j * BLK, (j + 1) * BLK)
            term = jnp.dot(left, w_buf[slot, :, cols], preferred_element_type=F32)
            before = jnp.where(i == 0, x_ref[:, cols].astype(F32), s_buf[j, :LANES, :])
            s_buf[j, :LANES, :] = before + term

    def body(t, carry):
        n, loaded = carry
        since = t - ATTEND

        @pl.when(t == 1)
        def _():
            wo_rows(zero()).start()
            start_all(weights)

        @pl.when(t == SEND_DO + 1)
        def _():
            own_do.start()
            for step in range(1, 8):
                do_copy(step, True).start()
            wait_all(weights)

        @pl.when((since > 0) & (t <= ATTENDED) & (lax.rem(since, 4) == 0))
        def _():
            wait_all(step_pieces(since - 1))

        @pl.when(t == ATTENDED)
        def _():
            attn.key_grads(dkv_buf)

        @pl.when((t >= ATTENDED) & (t < ATTENDED + N_SEND))
        def _():
            start_all(key_copies(part(t - ATTENDED, QROWS // N_SEND)))

        @pl.when(t == KEYS_IN)
        def _():
            add_peers()
        net_in.tick(t, PAIR * N_IN, view_in)
        net.tick(t - START, N_UNIT, view)
        for s in range(N_STAGE + 2):
            @pl.when(t == s * LAG)
            def _(s=s):
                net_cs.advance(0, 'D', view_cs, s)

        @pl.when((t > 1) & (t <= N_PART + 1))
        def _():
            head_grad(t - 2)

        ahead = t - PROJECT + 1

        @pl.when(ahead == 0)
        def _():
            take_positions()
            angles(0)

        @pl.when((ahead >= 0) & (odd(ahead) == 0) & (ahead < PAIR * N_CHUNK))
        def _():
            chunk_rows(half_of(ahead)).start()

        @pl.when((ahead > 0) & (odd(ahead) == 1) & (ahead < PAIR * N_CHUNK))
        def _():
            project(half_of(ahead))

            @pl.when(half_of(ahead) + 1 < N_CHUNK)
            def _():
                angles(half_of(ahead) + 1)

        @pl.when(t == ATTEND)
        def _():
            own_do.wait()
            take_do()
            operand(zero()).start()
            dk_acc[ALL] = jnp.zeros_like(dk_acc)
            dv_acc[ALL] = jnp.zeros_like(dv_acc)

        @pl.when((t >= ATTEND) & (t < ATTENDED))
        def _():
            attn.step(since)

            @pl.when(lax.rem(since, 4) == 3)
            def _():
                start_all(step_pieces(since))

        complete = jnp.minimum(lax.div(jnp.maximum(t - START - (N_STAGE - 1) * LAG + 1, 0), UPP), IN_GATHER)
        load = (loaded < complete) & (loaded <= lax.div(n, N_TILE) + 1)

        @pl.when(load)
        def _():
            start_all(piece(loaded))

        @pl.when(t == QUERY_IN)
        def _():
            for step in range(1, 8):
                do_copy(step, True).wait_send()

        for turn, (tick, n_steps) in enumerate(((QUERY_IN, N_PART), (OWN_IN, N_PART // 2))):
            @pl.when(t == tick)
            def _(turn=turn):
                start_own(turn)
                start_all(weight_rows(turn, zero()))

            @pl.when(t == tick + 1)
            def _(turn=turn):
                wait_own(turn)

            @pl.when((t > tick) & (t <= tick + n_steps))
            def _(turn=turn, tick=tick, n_steps=n_steps):
                norm_grad(turn, t - tick - 1, n_steps)

        @pl.when(t == OWN_IN + N_PART // 2 + 1)
        def _():
            mine = pltpu.make_async_copy(part_buf, parts.at[me], rows_sem)
            mine.start()
            mine.wait()
            lax.fori_loop(1, N_DEV, send_gain, 0)
            input_grad()
            start_own(2)
            start_all(out_rows(zero()))

        @pl.when(t == OUT_IN)
        def _():
            wait_own(2)

        @pl.when((t >= OUT_IN) & (t < OUT_IN + N_OUT))
        def _():
            out_part(t - OUT_IN)

        n_end = jnp.minimum(jnp.minimum(n + 1, loaded * N_TILE), n_own)
        lax.fori_loop(n, n_end, tile, 0)
        return n_end, loaded + load.astype(jnp.int32)

    n, _ = loop(LAST + 1, body, (zero(), zero()))
    start_own(3)
    for j in range(n_cols):
        sum_ref[:, j * BLK:(j + 1) * BLK] = s_buf[j, :LANES, :]
    lax.fori_loop(n, n_own, tile, 0)
    all_gains().wait_recv()
    dgain_ref[ALL] = jnp.sum(parts[ALL], axis=0)
    for slot in range(TRIO):
        keep_tile(0, slot).wait()
        give_tile(0, slot).wait_send()

    def received(n, carry):
        give_tile(n, 0).wait_recv()
        return carry

    loop(n_own, received, 0)
    wait_own(3)
    for copy in key_copies(pl.ds(0, QROWS)):
        copy.wait_send()
    all_gains().wait_send()


def main(x, dy, gain, pos, freq, w_q, w_k, w_v, w_o):
    model = x.shape[1]
    qkv = w_q.shape[1] + w_k.shape[1] + w_v.shape[1]
    queries, keys = pltpu.VMEM((TRIO, QROWS, LANES), BF16), pltpu.VMEM((SEQ, LANES), BF16)
    return pl.pallas_call(
        main_kernel,
        out_shape=[like((PAIR, *GRID) + x.shape, BF16), like((*GRID, 8, LANES), F32),
                   like((N_PIECE, PAIR, QUAD, PAIR, PAIR, QROWS, LANES), BF16), like((N_GATHER, BLK, BLK), F32),
                   like((LANES, model // 3), BF16), like(x.shape, F32), like(x.shape, BF16), like((PAIR * N_PART, LANES), F32)],
        in_specs=[vmem_spec()] * 5 + [any_spec()] * 4,
        out_specs=[any_spec()] * 4 + [vmem_spec()] * 4,
        scratch_shapes=[
            pltpu.VMEM(x.shape, BF16), queries, queries, keys, keys,
            pltpu.VMEM((*GRID, CHUNK, model), BF16), pltpu.VMEM((8, LANES), F32), pltpu.VMEM((1, model), F32), pltpu.VMEM((1, LANES), F32),
            pltpu.VMEM((*GRID, 8, LANES), F32), pltpu.VMEM((PAIR, LANES, LANES), F32), pltpu.VMEM((N_DEV * CHUNK, LANES), F32),
            pltpu.VMEM((QROWS, LANES), F32), pltpu.VMEM((8, LANES, TRIO * LANES), BF16),
            pltpu.VMEM((PAIR, 3, QROWS, LANES), BF16), pltpu.VMEM((LANES, SEQ), F32), pltpu.VMEM((LANES, SEQ), F32),
            pltpu.VMEM((SEQ // BLK, BLK, BLK), F32), pltpu.VMEM((TRIO, BLK, LANES), F32),
            pltpu.VMEM((QUAD, PAIR, QROWS, LANES), BF16), pltpu.VMEM((TRIO, 2, QROWS, LANES), BF16),
            pltpu.VMEM((PAIR, SEQ, BLK), BF16), pltpu.VMEM((PAIR, *GRID, LANES, BLK), BF16), pltpu.VMEM((TRIO, BLK, BLK), F32),
            pltpu.VMEM((LANES, qkv), BF16), pltpu.VMEM((LANES, PAIR * w_k.shape[1]), BF16), pltpu.VMEM((PAIR, HALF, qkv), BF16), pltpu.VMEM(x.shape, F32),
            pltpu.VMEM((PAIR * N_PART, LANES), F32), pltpu.VMEM((N_DEV, PAIR * N_PART, LANES), F32),
            sems(1, N_SLOT), sems(1, N_SLOT), sems(RING, N_SLOT), sems(RING, N_SLOT),
            sems(TRIO), sems(TRIO), sems(), sems(8), sems(8),
            sems(N_PIECE, 2), sems(PAIR), sems(PAIR), sems(TRIO), sems(TRIO),
            sems(IN_GATHER * N_TILE), sems(TRIO), sems(TRIO), sems(QUAD), sems(PAIR, 4), sems(), sems()],
        compiler_params=pltpu.CompilerParams(collective_id=0, has_side_effects=True, vmem_limit_bytes=VMEM_LIMIT),
    )(x, dy, gain, pos, freq, w_q, w_k, w_v, w_o)


N_LATE = N_PIECE - IN_GATHER
GROUP = IN_GATHER // N_LATE


def finish_kernel(sum_ref, o_ref, dx_ref, dgain_ref, w_ref, hd_ref, g_ref, t_ref,
                  y_ref, dx_out, dgain_out, wq_ref, wk_ref, wv_ref, wo_ref,
                  gbuf, abuf, obuf, cbuf, acc, wbuf, gsem, asem, osem, isem, csem, wsem):
    n_step, group = N_LATE * PER_PIECE, GROUP

    def operand(t):
        return operand_copy(hd_ref, abuf, asem, 1, t, odd(t))

    def cut(t):
        return pl.ds(pl.multiple_of(t * BLK, BLK), BLK)

    def lanes(i):
        return pl.ds(pl.multiple_of(i * LANES, LANES), LANES)

    def to_output(p, t, sub, src, sem):
        j = jnp.where(p == O_PIECES[0], 0, p - O_PIECES[0] - 2)
        return [pltpu.make_async_copy(
            src.at[pl.ds(i * LANES, LANES), :], wo_ref.at[lanes(TRIO * (sub * 4 + i) + j), cut(t)], sem.at[i])
            for i in range(QUAD)]

    def to_input(dst, place, t, sub, src, sem):
        return [pltpu.make_async_copy(
            src.at[:, pl.ds(i * LANES, LANES)], dst.at[cut(t), lanes(place(sub * 4 + i))], sem.at[i]) for i in range(QUAD)]

    def ins(n):
        return [pltpu.make_async_copy(t_ref.at[n * group + i], cbuf.at[lax.rem(n, TRIO), i], isem.at[lax.rem(n, TRIO), i])
                for i in range(group)]

    def start_outs(n):
        for i in range(group):
            m = n * group + i
            p, t, sub = lax.div(m, PER_PIECE), lax.rem(half_of(m), N_TILE), odd(m)
            src, sem = cbuf.at[lax.rem(n, TRIO), i], csem.at[lax.rem(n, TRIO), i]
            for cond, copies in (
                (p < 3, lambda: to_input(wq_ref, lambda g: TRIO * g + p, t, sub, src, sem)),
                (p == KEY_PIECE, lambda: to_input(wk_ref, lambda g: g, t, sub, src, sem)),
                (p == KEY_PIECE + 1, lambda: to_input(wv_ref, lambda g: g, t, sub, src, sem)),
                ((p == O_PIECES[0]) | (p == O_PIECES[1]), lambda: to_output(p, t, sub, src, sem)),
            ):
                @pl.when(cond)
                def _(copies=copies):
                    for c in copies():
                        c.start()

    def wait_outs(n):
        for i in range(group):
            for c in to_output(IN_GATHER, 0, 0, cbuf.at[0, i], csem.at[lax.rem(n, TRIO), i]):
                c.wait()

    def weight(i):
        slot = odd(i)
        return pltpu.make_async_copy(w_ref.at[lanes(TRIO * i + 2), :], wbuf.at[slot], wsem.at[slot])

    for late in range(N_LATE):
        for sub in range(PAIR):
            start_all(piece_copies(g_ref, gbuf, gsem, IN_GATHER + late, sub, late * 2 + sub))
    operand(zero()).start()
    weight(zero()).start()
    acc[ALL] = sum_ref[ALL]
    dx_out[ALL] = dx_ref[ALL]
    dgain_out[ALL] = dgain_ref[ALL]

    def step(n, carry):
        t, late, sub = lax.div(n, PAIR * N_LATE), lax.rem(half_of(n), N_LATE), odd(n)
        p, held = IN_GATHER + late, late * 2 + sub
        slot = lax.rem(n, TRIO)

        @pl.when(n >= 3)
        def _():
            wait_outs(n - 3)
        for c in ins(n):
            c.start()

        @pl.when(n >= 1)
        def _():
            for c in ins(n - 1):
                c.wait()
            start_outs(n - 1)

        @pl.when(held == 0)
        def _():
            operand(t).wait()

            @pl.when(nxt(t) < N_TILE)
            def _():
                operand(nxt(t)).start()

        @pl.when(n < PAIR * N_LATE)
        def _():
            wait_piece(gbuf, gsem, held)

        @pl.when(n >= 3)
        def _():
            for c in to_output(IN_GATHER, 0, 0, obuf.at[0], osem.at[slot]):
                c.wait()
        @pl.when(n < 8)
        def _():
            weight(n).wait()

            @pl.when(n < 7)
            def _():
                weight(n + 1).start()
            acc[ALL] += jnp.dot(o_ref[:, lanes(n)], wbuf[odd(n)], preferred_element_type=F32)
        obuf[slot] = tile_product(abuf[odd(t)], gbuf[held], True)
        for c in to_output(p, t, sub, obuf.at[slot], osem.at[slot]):
            c.start()
        return carry

    loop(n_step, step, 0)
    y_ref[ALL] = acc[ALL].astype(BF16)
    for c in ins(n_step - 1):
        c.wait()
    start_outs(jnp.int32(n_step - 1))
    for n in range(n_step - 3, n_step):
        wait_outs(n)
        for c in to_output(IN_GATHER, 0, 0, obuf.at[0], osem.at[n % 3]):
            c.wait()


def finish(x, o, dx, dgain, w_o, hd, g, tiles):
    model, kv = hd.shape[2], 8 * LANES
    return pl.pallas_call(
        finish_kernel,
        out_shape=[like(x.shape, BF16), like(dx.shape, BF16), like(dgain.shape, F32)]
        + [like((model, n), F32) for n in (TRIO * kv, kv, kv)] + [like((TRIO * kv, model), F32)],
        in_specs=[vmem_spec()] * 4 + [any_spec()] * 4,
        out_specs=[vmem_spec()] * 3 + [any_spec()] * 4,
        scratch_shapes=[pltpu.VMEM((PAIR * N_LATE, SEQ, BLK), BF16), pltpu.VMEM((PAIR, SEQ, BLK), BF16), pltpu.VMEM((TRIO, BLK, BLK), F32),
                        pltpu.VMEM((TRIO, GROUP, BLK, BLK), F32), pltpu.VMEM(x.shape, F32), pltpu.VMEM((PAIR, LANES, model), BF16),
                        sems(PAIR * N_LATE), sems(PAIR), sems(TRIO, 4), sems(TRIO, GROUP), sems(TRIO, GROUP, 4), sems(PAIR)],
        cost_estimate=pl.CostEstimate(flops=4 * SEQ * kv * model, bytes_accessed=250 * 2**20, transcendentals=0),
        compiler_params=pltpu.CompilerParams(vmem_limit_bytes=VMEM_LIMIT),
    )(x, o, dx, dgain, w_o, hd, g, tiles)


def solution(mesh):
    assert mesh.shape['hp'] == 4 and mesh.shape['cp'] == 8

    def device_step(hidden, grad_out, positions, norm_gain, w_q, w_k, w_v, w_o, inv_freq):
        model = hidden.shape[1]
        hd, _, gathered, tiles, o_own, total, dx, gains = main(
            hidden, grad_out, norm_gain, positions, inv_freq, w_q, w_k, w_v, w_o)
        output, grad_hidden, grad_gain, grad_wq, grad_wk, grad_wv, grad_wo = finish(
            total, o_own, dx, gains, w_o, hd.reshape(2, SEQ, model), gathered, tiles)
        grad_gain = grad_gain.reshape(-1)
        return output, grad_hidden, grad_wq, grad_wk, grad_wv, grad_wo, grad_gain

    rows, whole = P(('cp', 'hp'), None), P()
    return jax.shard_map(
        device_step, mesh=mesh,
        in_specs=(rows, rows, P(('cp', 'hp')), whole, whole, whole, whole, whole, whole),
        out_specs=(rows, rows, whole, whole, whole, whole, whole), check_vma=False)
```

```python
import functools
import jax
import jax.numpy as jnp
from jax import lax
from jax.experimental import pallas as pl
from jax.experimental.pallas import tpu as pltpu
from jax.sharding import PartitionSpec as P

NORM_EPS = 1e-5
ALL = Ellipsis
EVERY = slice(None)
PAIR, TRIO, QUAD = 2, 3, 4
GRID = (PAIR, PAIR, PAIR, QUAD)
BY_COLUMN = {'axis': 0, 'keepdims': True}
BY_ROW = {'axis': 1, 'keepdims': True}
F32 = jnp.float32
BF16 = jnp.bfloat16
LANES = 128
BLK = 512
HALF = BLK // 2
SEQ = 8 * BLK
QROWS = PAIR * BLK
UPP = 8
LAG = 2
RING = 20
VMEM_LIMIT = 64 * 2**20 - 2**16
NT = (((1,), (1,)), ((), ()))
TN = (((0,), (0,)), ((), ()))

STAGES = {
    'C': ('z1', 'z2', 'z3', 'y', 'x', 'd'),
    'D': ('z1', 'z2', 'z3', 'x', 'y', 'd'),
    'E': ('x', 'y', 'z1', 'z2', 'z3', 'd'),
    'F': ('y', 'x', 'z1', 'z2', 'z3', 'd'),
}
N_STAGE = 6


def odd(i):
    return lax.rem(i, PAIR)


def half_of(i):
    return lax.div(i, PAIR)


def nxt(i):
    return i + 1


def zero():
    return jnp.int32(0)


def loop(n, body, init):
    return lax.fori_loop(0, n, body, init)


class Gather:
    def __init__(self, send_sem, recv_sem, mix, base=0):
        self.mix, self.base = mix, base
        self.z = lax.axis_index('hp')
        cp = lax.axis_index('cp')
        self.c, self.x, self.y = odd(cp), odd(half_of(cp)), lax.div(cp, 4)
        self.send_sem, self.recv_sem = send_sem, recv_sem

    def device(self, **moved):
        at = {name: moved.get(name, getattr(self, name)) for name in 'cxyz'}
        return at['z'], (at['y'] * PAIR + at['x']) * PAIR + at['c']

    def copies(self, sem_row, kind, view, stage):
        c, x, y, z = self.c, self.x, self.y, self.z
        order = STAGES[kind]
        done = {st[0] for st in order[:order.index(stage)]}
        every = EVERY
        gx, gy, gz = (every if d in done else v for d, v in (('x', x), ('y', y), ('z', z)))
        slot = order.index(stage)

        def copy(place, device):
            return lambda: pltpu.make_async_remote_copy(
                place, place, self.send_sem.at[sem_row, slot], self.recv_sem.at[sem_row, slot],
                device_id=device, device_id_type=pl.DeviceIdType.MESH)

        if stage in 'xyd':
            mine, other, dev = {
                'x': lambda: ((c, x, gy, gz), (c, 1 - x, gy, gz), self.device(x=1 - x)),
                'y': lambda: ((c, gx, y, gz), (c, gx, 1 - y, gz), self.device(y=1 - y)),
                'd': lambda: ((c, EVERY, EVERY, EVERY), (1 - c, EVERY, EVERY, EVERY), self.device(c=1 - c)),
            }[stage]()
            out, back = [(True, copy(view(*mine), dev))], [(True, copy(view(*other), dev))]
            return {'start': out, 'sent': out, 'recv': back}
        hop = int(stage[1])
        ups, downs = (z >= hop - 1) & (z < 3), (z + hop <= 4) & (z > 0)
        above, below = self.device(z=jnp.minimum(z + 1, 3)), self.device(z=jnp.maximum(z - 1, 0))

        def counted(one, other):
            return [(one != other, copy(view(c, gx, gy, 0), above)), (one & other, copy(view(c, gx, gy, pl.ds(0, PAIR)), above))]

        return {
            'start': [(ups, copy(view(c, gx, gy, jnp.maximum(z - hop + 1, 0)), above)),
                      (downs, copy(view(c, gx, gy, jnp.minimum(z + hop - 1, 3)), below))],
            'sent': counted(ups, downs),
            'recv': counted(z >= hop, z + hop <= 3),
        }

    def run(self, sem_row, kind, view, stage, what):
        for cond, copy in self.copies(sem_row, kind, view, stage)[what]:
            def act(copy=copy):
                if what == 'start':
                    copy().start()
                elif what == 'sent':
                    copy().wait_send()
                else:
                    copy().wait_recv()

            if cond is True:
                act()
            else:
                pl.when(cond)(act)

    def advance(self, sem_row, kind, view, s):
        if 0 < s <= N_STAGE:
            self.run(sem_row, kind, view, STAGES[kind][s - 1], 'recv')
        if s < N_STAGE:
            self.run(sem_row, kind, view, STAGES[kind][s], 'start')
        if s > N_STAGE:
            for stage in STAGES[kind]:
                self.run(sem_row, kind, view, stage, 'sent')

    def kinds(self, u):
        word, at = lax.div(u, 16), lax.rem(u, 16)
        code = jnp.int32(self.mix[0])
        for i in range(1, len(self.mix)):
            code = jnp.where(word == i, self.mix[i], code)
        code = lax.shift_right_logical(code, at * 2) & 3
        return tuple((kind, code == i) for i, kind in enumerate('CDEF'))

    def tick(self, t, n_units, view):
        for s in range(N_STAGE + 2):
            u = t - s * LAG

            @pl.when((u >= 0) & (u < n_units))
            def _(u=u, s=s):
                for kind, is_kind in self.kinds(u):
                    @pl.when(is_kind)
                    def _(kind=kind):
                        self.advance(lax.rem(u + self.base, RING), kind, view(u), s)


def turn(v):
    return pltpu.roll(v, LANES // 2, 1)


def low_lanes(shape):
    return lax.broadcasted_iota(jnp.int32, shape, 1) < LANES // 2


def cos_sin(cs):
    low = low_lanes(cs.shape)
    other = turn(cs)
    return jnp.where(low, cs, other), jnp.where(low, -other, cs)


def any_spec():
    return pl.BlockSpec(memory_space=pl.ANY)


def vmem_spec():
    return pl.BlockSpec(memory_space=pltpu.VMEM)


def sems(*shape):
    return pltpu.SemaphoreType.DMA(shape) if shape else pltpu.SemaphoreType.DMA


def like(shape, dtype):
    return jax.ShapeDtypeStruct(shape, dtype)


def start_all(copies):
    for copy in copies:
        copy.start()


def wait_all(copies):
    for copy in copies:
        copy.wait()


N_PIECE = 8
O_PIECES = (3, 6, 7)
KEY_PIECE = 4
N_TILE = 6
PER_PIECE = PAIR * N_TILE
IN_GATHER = 7
N_GATHER = IN_GATHER * PER_PIECE


def tile_product(operand, piece, of_output):
    left, right = (piece, operand) if of_output else (operand, piece)
    return lax.dot_general(left, right, TN, preferred_element_type=F32)


def operand_copy(hd_ref, abuf, asem, which, t, slot):
    return pltpu.make_async_copy(
        hd_ref.at[which, :, pl.ds(pl.multiple_of(t * BLK, BLK), BLK)], abuf.at[slot], asem.at[slot])


def piece_copies(g_ref, gbuf, gsem, p, core, slot):
    return [pltpu.make_async_copy(g_ref.at[p, core, z, r // 2, r % 2],
                                  gbuf.at[slot, pl.ds(r * QROWS, QROWS), pl.ds(z * LANES, LANES)], gsem.at[slot])
            for z in range(QUAD) for r in range(QUAD)]


def wait_piece(gbuf, gsem, slot):
    pltpu.make_async_copy(gbuf.at[slot], gbuf.at[slot], gsem.at[slot]).wait()


def lane_groups(op, s):
    out = s[:, :LANES]
    for i in range(1, s.shape[1] // LANES):
        out = op(out, s[:, i * LANES:(i + 1) * LANES])
    return out


class Attention:
    def __init__(self, q, do, k, v, cs, out, dk_acc, dv_acc, s, state, quarter):
        self.q, self.do, self.k, self.v, self.cs, self.out = q, do, k, v, cs, out
        self.dk, self.dv, self.s, self.state = dk_acc, dv_acc, s, state
        self.quarter = quarter
        self.scale = LANES ** -0.5
        self.factor = self.scale * 1.4426950408889634

    def step(self, t):
        head, half = lax.div(t, 8), odd(lax.div(t, 4))
        n_key = jnp.where(half == 0, self.quarter + 1, SEQ // BLK - self.quarter)
        rows = pl.ds(pl.multiple_of(half * BLK, BLK), BLK)
        for i, act in enumerate((self.scores, self.exps, self.values, self.grads)):
            @pl.when(lax.rem(t, 4) == i)
            def _(act=act):
                act(head, half, n_key, rows)

    def keys(self, kb):
        return pl.ds(pl.multiple_of(kb * BLK, BLK), BLK)

    def zeros(self):
        return jnp.zeros((BLK, LANES), F32)

    def keep(self, i, column):
        self.state[i] = jnp.broadcast_to(column, (BLK, LANES))

    def kept(self, i):
        return self.state[i, :, :1]

    def scores(self, head, half, n_key, rows):
        q = self.q[head, rows, :]

        def block(kb, m, diagonal=False):
            s = lax.dot_general(q, self.k[self.keys(kb), :], NT, preferred_element_type=F32)
            if diagonal:
                visible = lax.broadcasted_iota(jnp.int32, s.shape, 0) >= lax.broadcasted_iota(jnp.int32, s.shape, 1)
                s = jnp.where(visible, s, -1e30)
            self.s[kb] = s
            return jnp.maximum(m, lane_groups(jnp.maximum, s))

        m = loop(n_key - 1, block, self.zeros() - 1e30)
        m = block(n_key - 1, m, diagonal=True)
        self.keep(0, jnp.max(m, **BY_ROW) * self.factor)

    def exps(self, head, half, n_key, rows):
        m = self.kept(0)

        def block(kb, total):
            e = jnp.exp2(self.s[kb] * self.factor - m)
            self.s[kb] = e
            return total + lane_groups(jnp.add, e)

        total = loop(n_key, block, self.zeros())
        self.keep(0, 1.0 / jnp.sum(total, **BY_ROW))

    def sides(self, half):
        for side in range(PAIR):
            place = (half * (1 - side) + (1 - half) * side) * HALF
            yield pl.ds(pl.multiple_of(place, HALF), HALF), pl.ds(pl.multiple_of(side * BLK + half * HALF, HALF), HALF)

    def values(self, head, half, n_key, rows):
        do, inv = self.do[head, rows, :], self.kept(0)
        turned = do.T

        def block(kb, o):
            p = (self.s[kb] * inv).astype(BF16)
            self.dv[:, self.keys(kb)] += jnp.dot(turned, p, preferred_element_type=F32)
            return o + jnp.dot(p, self.v[self.keys(kb), :], preferred_element_type=F32)

        o = loop(n_key, block, self.zeros()).astype(BF16).astype(F32)
        self.keep(1, jnp.sum(do.astype(F32) * o, **BY_ROW))
        self.state[2] = o
        for place, stored in self.sides(half):
            self.out[1, head, stored, :] = self.state[2, place, :].astype(BF16)

    def grads(self, head, half, n_key, rows):
        do, inv, delta = self.do[head, rows, :], self.kept(0), self.kept(1)
        turned = self.q[head, rows, :].T

        def block(kb, dq):
            dp = lax.dot_general(do, self.v[self.keys(kb), :], NT, preferred_element_type=F32)
            ds = (self.s[kb] * inv * (dp - delta)).astype(BF16)
            self.dk[:, self.keys(kb)] += jnp.dot(turned, ds, preferred_element_type=F32)
            return dq + jnp.dot(ds, self.k[self.keys(kb), :], preferred_element_type=F32)

        dq = loop(n_key, block, self.zeros()) * self.scale
        self.state[2] = dq.astype(BF16).astype(F32)
        for place, stored in self.sides(half):
            cos, sin = cos_sin(self.cs[stored, :])
            part = self.state[2, place, :]
            self.out[0, head, stored, :] = (part * cos - turn(part) * sin).astype(BF16)

    def key_grads(self, out):
        for pair in range(8):
            for i, (acc, factor) in enumerate(((self.dk, self.scale), (self.dv, 1.0))):
                for part, block in enumerate((pair, 15 - pair)):
                    out[pair // 2, i, pl.ds(pair % PAIR * BLK + part * HALF, HALF), :] = (
                        acc[:, pl.ds(block * HALF, HALF)].T * factor).astype(BF16)


ROWS_UNIT = 8
N_IN = LANES // ROWS_UNIT
N_STEP = 24
N_UNIT = N_PIECE * UPP
N_PART = 12
SEND_DO = N_PART + 1
DELAY = N_STAGE * LAG
CHUNK = PAIR * ROWS_UNIT
N_CHUNK = LANES // CHUNK
PROJECT = DELAY + 2
ATTEND = PROJECT + PAIR * N_CHUNK - 1
ATTENDED = ATTEND + N_STEP
START = ATTEND + 4
N_SEND = 8
KEYS_IN = START + KEY_PIECE * UPP
QUERY_IN = START + 3 * UPP + DELAY
OWN_IN = START + O_PIECES[1] * UPP + DELAY
OUT_IN = OWN_IN + N_PART // 2 + 2
N_OUT = 8
LAST = START + N_UNIT + DELAY + LAG
N_DEV = 32


def main_kernel(x_ref, dy_ref, gain_ref, mypos_ref, freq_ref, wq_ref, wk_ref, wv_ref, wo_ref,
                hd_ref, pos_ref, g_ref, t_ref, o_ref, sum_ref, dx_ref, dgain_ref,
                h_buf, q_buf, do_buf, k_buf, v_buf, rows_buf, mypos_buf, gain_buf, freq_buf, pos_buf, pos_t, cs_buf, own_cs, do_parts,
                piece_buf, dk_acc, dv_acc, s_buf, state, dkv_buf, peer_buf, gbuf, abuf, obuf, own_buf, oo_buf, w_buf, dn_buf, part_buf, z_parts, sum_buf, parts,
                cs_send, cs_recv, send_sem, recv_sem, first_sem, proj_sem, rows_sem, do_send, do_recv,
                lsem, gsem, asem, osem, tsend, trecv, psend, precv, rsem, wsem, gain_send, gain_recv):
    net_in, net_cs, net = Gather(send_sem, recv_sem, (293880977, 1175604295)), Gather(cs_send, cs_recv, (293880977, 1175604295)), Gather(send_sem, recv_sem, (-398134202, 303174049, 1212958790, -1471626106), START)
    quarter = net.y * 2 + net.x
    head = net.c * 4 + net.z
    spot = (net.y, net.x, net.c, net.z)
    attn = Attention(q_buf, do_buf, k_buf, v_buf, own_cs, piece_buf, dk_acc, dv_acc, s_buf, state, quarter)

    def inv_rms():
        x = x_ref[ALL].astype(F32)
        return lax.rsqrt(jnp.mean(x * x, **BY_ROW) + NORM_EPS)

    barrier = pltpu.get_barrier_semaphore()

    def greet(**moved):
        pl.semaphore_signal(barrier, inc=1, device_id=net.device(**moved), device_id_type=pl.DeviceIdType.MESH)

    greet(x=1 - net.x)
    greet(y=1 - net.y)
    greet(c=1 - net.c)
    inner = (net.z > 0).astype(jnp.int32) + (net.z < 3).astype(jnp.int32)

    @pl.when(net.z > 0)
    def _():
        greet(z=net.z - 1)

    @pl.when(net.z < 3)
    def _():
        greet(z=net.z + 1)

    gain_buf[ALL] = gain_ref[ALL].astype(F32).reshape(gain_buf.shape)
    freq_buf[ALL] = jnp.concatenate([freq_ref[ALL], freq_ref[ALL]], axis=0).reshape(freq_buf.shape)
    mypos_buf[ALL] = jnp.broadcast_to(mypos_ref[ALL].astype(F32).reshape(1, LANES), mypos_buf.shape)
    h_buf[ALL] = (x_ref[ALL].astype(F32) * inv_rms() * gain_buf[ALL]).astype(BF16)
    first = [pltpu.make_async_copy(src, dst, first_sem.at[i]) for i, (src, dst) in enumerate((
        (h_buf, hd_ref.at[(0, *spot)]), (dy_ref, hd_ref.at[(1, *spot)]), (mypos_buf, pos_ref.at[spot])))]
    start_all(first)
    wait_all(first)
    pl.semaphore_wait(barrier, TRIO + inner)
    q_cols = pl.ds(pl.multiple_of(head * TRIO * LANES, LANES), TRIO * LANES)
    kv_cols = pl.ds(pl.multiple_of(head * LANES, LANES), LANES)
    w_rows = slice(0, wq_ref.shape[0])
    wq_buf, wkv_buf = gbuf.at[0, w_rows, :TRIO * LANES], gbuf.at[1, w_rows, :PAIR * LANES]
    weights = [pltpu.make_async_copy(src, dst, proj_sem.at[i]) for i, (src, dst) in enumerate((
        (wq_ref.at[:, q_cols], wq_buf), (wk_ref.at[:, kv_cols], gbuf.at[1, w_rows, :LANES]),
        (wv_ref.at[:, kv_cols], gbuf.at[1, w_rows, LANES:PAIR * LANES])))]

    def view_in(u):
        rows = pl.ds(pl.multiple_of(lax.rem(u, N_IN) * ROWS_UNIT, ROWS_UNIT), ROWS_UNIT)
        which = lax.div(u, N_IN)
        return lambda c, x, y, z: hd_ref.at[which, y, x, c, z, rows, :]

    def view_cs(c, x, y, z):
        return pos_ref.at[y, x, c, z]

    def part(i, width=HALF):
        return pl.ds(pl.multiple_of(i * width, width), width)

    def wo_rows(i):
        slot = odd(i)
        return pltpu.make_async_copy(wo_ref.at[part(i), :], w_buf.at[slot, :, :wo_ref.shape[1]], wsem.at[slot, 0])

    def head_grad(i):
        slot = odd(i)
        wo_rows(i).wait()

        @pl.when(nxt(i) < N_PART)
        def _():
            wo_rows(nxt(i)).start()
        own_buf[:, part(i)] = lax.dot_general(
            dy_ref[ALL], w_buf[slot, :, :wo_ref.shape[1]], NT, preferred_element_type=F32).astype(BF16)

    def do_copy(step, mine):
        me = net.c * 4 + net.z
        other = lax.rem(me + step, 8)
        slot = me if mine else lax.rem(me + 8 - step, 8)
        return pltpu.make_async_remote_copy(
            own_buf.at[:, part(other, TRIO * LANES)], do_parts.at[slot], do_send.at[step], do_recv.at[step],
            device_id=net.device(c=lax.div(other, 4), z=lax.rem(other, 4)), device_id_type=pl.DeviceIdType.MESH)

    own_do = pltpu.make_async_copy(own_buf.at[:, part(head, TRIO * LANES)], do_parts.at[head], do_send.at[0])

    def query_row(c, z):
        return c * HALF + z * LANES if z < 2 else BLK + (1 - c) * HALF + (z - 2) * LANES

    def take_do():
        for step in range(1, 8):
            do_copy(step, False).wait_recv()
        for c in range(PAIR):
            for z in range(QUAD):
                for j in range(TRIO):
                    do_buf[j, pl.ds(query_row(c, z), LANES), :] = do_parts[c * 4 + z, :, j * LANES:(j + 1) * LANES]

    every = EVERY

    def chunk(k, base=0):
        return pl.ds(pl.multiple_of(base + k * CHUNK, CHUNK), CHUNK)

    def chunk_rows(k):
        return pltpu.make_async_copy(hd_ref.at[0, every, every, every, every, chunk(k), every], rows_buf, rows_sem)

    def take_positions():
        copy = pltpu.make_async_copy(pos_ref, pos_buf, rows_sem)
        copy.start()
        copy.wait()
        for i in range(PAIR):
            pos_t[i] = pos_buf[i].reshape(LANES, LANES).T

    def angles(k):
        for dev in range(N_DEV):
            column = pos_t[dev // 16, chunk(k), dev % 16 * 8:dev % 16 * 8 + 1]
            cs_buf[dev * CHUNK:(dev + 1) * CHUNK, :] = jnp.broadcast_to(column, (CHUNK, LANES)) * freq_buf[ALL]
        angle = cs_buf[ALL]
        cs_buf[ALL] = jnp.where(low_lanes(angle.shape), jnp.cos(angle), jnp.sin(angle))

    def rotate(v, cs):
        cos, sin = cos_sin(cs)
        return (v * cos + turn(v) * sin).astype(BF16)

    def project(k):
        chunk_rows(k).wait()
        n_rows = N_DEV * CHUNK
        kv = jnp.dot(rows_buf[ALL].reshape(n_rows, -1), wkv_buf[ALL], preferred_element_type=F32)
        key = rotate(kv[:, :LANES], cs_buf[ALL])
        value = kv[:, LANES:].astype(BF16)
        for cp in range(8):
            for z in range(QUAD):
                block = 2 * cp + z if z < 2 else 28 - 2 * cp + z
                rows = slice((cp * 4 + z) * CHUNK, (cp * 4 + z + 1) * CHUNK)
                k_buf[chunk(k, block * LANES), :] = key[rows]
                v_buf[chunk(k, block * LANES), :] = value[rows]
        mine, cs = rows_buf[net.y, net.x].reshape(LANES, -1), cs_buf[part(quarter, LANES), :]
        q = jnp.dot(mine, wq_buf[ALL], preferred_element_type=F32)
        for j in range(TRIO):
            p = rotate(q[:, j * LANES:(j + 1) * LANES], cs)
            for c in range(PAIR):
                for z in range(QUAD):
                    rows = slice((c * 4 + z) * CHUNK, (c * 4 + z + 1) * CHUNK)
                    q_buf[j, chunk(k, query_row(c, z)), :] = p[rows]
                    if j == 0:
                        own_cs[chunk(k, c * BLK + z * LANES), :] = cs[rows]

    def local(p, i, src, rows=pl.ds(0, QROWS)):
        return pltpu.make_async_copy(src, g_ref.at[p, net.c, net.z, net.y, net.x, rows, :], lsem.at[p, i])

    def step_pieces(step):
        head, half = lax.div(step, 8), odd(lax.div(step, 4))
        out_piece = jnp.where(head == 0, O_PIECES[0], O_PIECES[0] + 2 + head)
        return [local(p, side, piece_buf.at[i, head, rows], rows) for i, p in ((0, head), (1, out_piece))
                for side, (_, rows) in enumerate(attn.sides(half))]

    def key_copies(rows):
        for i, moved in enumerate(('x', 'y', 'xy')):
            x, y = (1 - at if name in moved else at for name, at in (('x', net.x), ('y', net.y)))
            yield pltpu.make_async_remote_copy(
                dkv_buf.at[y * 2 + x, :, rows], peer_buf.at[i, :, rows], psend.at[i], precv.at[i],
                device_id=net.device(x=x, y=y), device_id_type=pl.DeviceIdType.MESH)

    def add_peers():
        for copy in key_copies(pl.ds(0, QROWS)):
            copy.wait_recv()
        total = dkv_buf[quarter].astype(F32)
        for i in range(TRIO):
            total = total + peer_buf[i].astype(F32)
        total = total.astype(BF16)
        cos, sin = cos_sin(own_cs[ALL])
        dk = total[0].astype(F32)
        piece_buf[0, 0] = (dk * cos - turn(dk) * sin).astype(BF16)
        piece_buf[0, 1] = total[1]
        kv = [local(KEY_PIECE + i, 0, piece_buf.at[0, i]) for i in range(PAIR)]
        start_all(kv)
        wait_all(kv)

    def view(u):
        p, k = lax.div(u, UPP), lax.rem(u, UPP)
        two = half_of(k)
        rows = part(odd(two) * 4 + half_of(two) * 2 + odd(k), QROWS // UPP)
        return lambda c, x, y, z: g_ref.at[p, c, z, y, x, rows, :]

    def place(n):
        return lax.div(n, N_TILE) * PER_PIECE + lax.rem(n, N_TILE) * 2 + net.c

    def keep_tile(n, slot):
        return pltpu.make_async_copy(obuf.at[slot], t_ref.at[place(n)], osem.at[slot])

    def give_tile(n, slot):
        return pltpu.make_async_remote_copy(
            obuf.at[slot], t_ref.at[place(n)], tsend.at[slot], trecv.at[n],
            device_id=net.device(c=1 - net.c), device_id_type=pl.DeviceIdType.MESH)

    def of_output(p):
        return (p == O_PIECES[0]) | (p == O_PIECES[1])

    def operand(n):
        which, slot = of_output(lax.div(n, N_TILE)).astype(jnp.int32), odd(n)
        return pltpu.make_async_copy(
            hd_ref.at[which, every, every, every, every, every, part(lax.rem(n, N_TILE), BLK)], abuf.at[slot], asem.at[slot])

    def piece(p):
        return piece_copies(g_ref, gbuf, gsem, p, net.c, odd(p))

    n_own = IN_GATHER * N_TILE

    def tile(n, carry):
        slot = lax.rem(n, TRIO)
        p = lax.div(n, N_TILE)

        @pl.when(lax.rem(n, N_TILE) == 0)
        def _():
            wait_piece(gbuf, gsem, odd(p))
        operand(n).wait()

        @pl.when(nxt(n) < n_own)
        def _():
            operand(nxt(n)).start()

        @pl.when(n >= 3)
        def _():
            keep_tile(n, slot).wait()
            give_tile(n, slot).wait_send()
        for output in (False, True):
            @pl.when(of_output(p) == output)
            def _(output=output):
                obuf[slot] = tile_product(abuf[odd(n)].reshape(SEQ, BLK), gbuf[odd(p)], output)
        keep_tile(n, slot).start()
        give_tile(n, slot).start()
        return carry

    kv = wk_ref.shape[1]
    groups = (((0, 1, 2), own_buf, slice(0, TRIO * kv)), ((KEY_PIECE, KEY_PIECE + 1), own_buf, slice(TRIO * kv, 5 * kv)),
              (O_PIECES[:2], oo_buf, slice(0, PAIR * kv)), (O_PIECES[2:], o_ref, slice(0, kv)))

    def start_own(i):
        rows = pl.ds(pl.multiple_of(net.c * BLK + net.z * LANES, LANES), LANES)
        pieces, dst, cols = groups[i]
        for k, p in enumerate(pieces):
            for g in range(8):
                col = cols.start // LANES + (TRIO * g + k if len(pieces) == 3 else 8 * k + g)
                pltpu.make_async_copy(
                    g_ref.at[p, g // 4, g % 4, net.y, net.x, rows, :], dst.at[:, pl.ds(col * LANES, LANES)], rsem.at[i]).start()

    def wait_own(i):
        _, dst, cols = groups[i]
        pltpu.make_async_copy(dst.at[:, cols], dst.at[:, cols], rsem.at[i]).wait()

    def weight_rows(turn, i):
        slot = odd(i)
        if turn == 0:
            places = ((wq_ref, part(i), 0, TRIO * kv),)
        else:
            places = [(src, part(i * 2 + j), (j * 2 + k) * kv, kv) for j in range(PAIR) for k, src in enumerate((wk_ref, wv_ref))]
        return [pltpu.make_async_copy(src.at[rows, :], w_buf.at[slot, :, pl.ds(at, width)], wsem.at[slot, j])
                for j, (src, rows, at, width) in enumerate(places)]

    def norm_grad(turn, i, n_steps):
        slot = odd(i)
        wait_all(weight_rows(turn, i))

        @pl.when(nxt(i) < n_steps)
        def _():
            start_all(weight_rows(turn, nxt(i)))
        if turn == 0:
            dn_buf[:, part(i)] = lax.dot_general(
                own_buf[:, :TRIO * kv], w_buf[slot, :, :TRIO * kv], NT, preferred_element_type=F32)
            return
        for j in range(PAIR):
            block = i * 2 + j
            dn = dn_buf[:, part(block)] + lax.dot_general(
                own_buf[:, TRIO * kv:], w_buf[slot, :, pl.ds(j * PAIR * kv, PAIR * kv)], NT, preferred_element_type=F32)
            dn_buf[:, part(block)] = dn
            x_hat = x_ref[:, part(block)].astype(F32) * inv_rms()
            total = jnp.sum(dn * x_hat, **BY_COLUMN)
            for k in range(PAIR):
                part_buf[pl.ds(block * 2 + k, 1), :] = total[:, k * LANES:(k + 1) * LANES]

    column = (net.y * PAIR + net.x) * PAIR + net.c

    def share(src, dst, slot, n, sem, device):
        def send(step, carry):
            pltpu.make_async_remote_copy(
                src, dst.at[slot], gain_send.at[sem], gain_recv.at[sem],
                device_id=device(lax.rem(slot + step, n)), device_id_type=pl.DeviceIdType.MESH).start()
            return carry

        mine = pltpu.make_async_copy(src, dst.at[slot], rows_sem)
        mine.start()
        mine.wait()
        lax.fori_loop(1, n, send, 0)

    def shared(dst, n, sem):
        rest = dst.at[pl.ds(1, n - 1)]
        return pltpu.make_async_remote_copy(
            rest, rest, gain_send.at[sem], gain_recv.at[sem],
            device_id=net.device(c=1 - net.c), device_id_type=pl.DeviceIdType.MESH)

    def gain_column():
        share(part_buf, z_parts, net.z, QUAD, 0, lambda z: net.device(z=z))

    def gain_rest():
        shared(z_parts, QUAD, 0).wait_recv()
        sum_buf[ALL] = jnp.sum(z_parts[ALL], axis=0)
        share(sum_buf, parts, column, 8, 1, lambda k: (net.z, k))

    def input_grad():
        x_hat = x_ref[ALL].astype(F32) * inv_rms()
        d_hat = dn_buf[ALL] * gain_buf[ALL]
        dx_ref[ALL] = (dy_ref[ALL].astype(F32) + inv_rms() * (
            d_hat - x_hat * jnp.mean(d_hat * x_hat, **BY_ROW))).astype(BF16)

    n_cols = x_ref.shape[1] // BLK

    def out_rows(i):
        slot = odd(i)
        head = lax.rem(i, 4) * 6 + lax.div(i, 4)
        return [pltpu.make_async_copy(
            wo_ref.at[part(head + TRIO * j, LANES), :], w_buf.at[slot, j * LANES:(j + 1) * LANES, :wo_ref.shape[1]], wsem.at[slot, j])
            for j in range(PAIR)]

    def out_part(i):
        slot = odd(i)
        wait_all(out_rows(i))

        @pl.when(nxt(i) < N_OUT)
        def _():
            start_all(out_rows(nxt(i)))
        left = oo_buf[:, part(i)]
        for j in range(n_cols):
            cols = slice(j * BLK, (j + 1) * BLK)
            term = jnp.dot(left, w_buf[slot, :, cols], preferred_element_type=F32)
            before = jnp.where(i == 0, x_ref[:, cols].astype(F32), s_buf[j, :LANES, :])
            s_buf[j, :LANES, :] = before + term

    def body(t, carry):
        n, loaded = carry
        since = t - ATTEND

        @pl.when(t == 1)
        def _():
            wo_rows(zero()).start()
            start_all(weights)

        @pl.when(t == SEND_DO + 1)
        def _():
            own_do.start()
            for step in range(1, 8):
                do_copy(step, True).start()
            wait_all(weights)

        @pl.when((since > 0) & (t <= ATTENDED) & (lax.rem(since, 4) == 0))
        def _():
            wait_all(step_pieces(since - 1))

        @pl.when(t == ATTENDED)
        def _():
            attn.key_grads(dkv_buf)

        @pl.when((t >= ATTENDED) & (t < ATTENDED + N_SEND))
        def _():
            start_all(key_copies(part(t - ATTENDED, QROWS // N_SEND)))

        @pl.when(t == KEYS_IN)
        def _():
            add_peers()
        net_in.tick(t, PAIR * N_IN, view_in)
        net.tick(t - START, N_UNIT, view)
        for s in range(N_STAGE + 2):
            @pl.when(t == s * LAG)
            def _(s=s):
                net_cs.advance(0, 'D', view_cs, s)

        @pl.when((t > 1) & (t <= N_PART + 1))
        def _():
            head_grad(t - 2)

        ahead = t - PROJECT + 1

        @pl.when(ahead == 0)
        def _():
            take_positions()
            angles(0)

        @pl.when((ahead >= 0) & (odd(ahead) == 0) & (ahead < PAIR * N_CHUNK))
        def _():
            chunk_rows(half_of(ahead)).start()

        @pl.when((ahead > 0) & (odd(ahead) == 1) & (ahead < PAIR * N_CHUNK))
        def _():
            project(half_of(ahead))

            @pl.when(half_of(ahead) + 1 < N_CHUNK)
            def _():
                angles(half_of(ahead) + 1)

        @pl.when(t == ATTEND)
        def _():
            own_do.wait()
            take_do()
            operand(zero()).start()
            dk_acc[ALL] = jnp.zeros_like(dk_acc)
            dv_acc[ALL] = jnp.zeros_like(dv_acc)

        @pl.when((t >= ATTEND) & (t < ATTENDED))
        def _():
            attn.step(since)

            @pl.when(lax.rem(since, 4) == 3)
            def _():
                start_all(step_pieces(since))

        complete = jnp.minimum(lax.div(jnp.maximum(t - START - (N_STAGE - 1) * LAG + 1, 0), UPP), IN_GATHER)
        load = (loaded < complete) & (loaded <= lax.div(n, N_TILE) + 1)

        @pl.when(load)
        def _():
            start_all(piece(loaded))

        @pl.when(t == QUERY_IN)
        def _():
            for step in range(1, 8):
                do_copy(step, True).wait_send()

        for turn, (tick, n_steps) in enumerate(((QUERY_IN, N_PART), (OWN_IN, N_PART // 2))):
            @pl.when(t == tick)
            def _(turn=turn):
                start_own(turn)
                start_all(weight_rows(turn, zero()))

            @pl.when(t == tick + 1)
            def _(turn=turn):
                wait_own(turn)

            @pl.when((t > tick) & (t <= tick + n_steps))
            def _(turn=turn, tick=tick, n_steps=n_steps):
                norm_grad(turn, t - tick - 1, n_steps)

        @pl.when(t == OWN_IN + N_PART // 2 + 1)
        def _():
            gain_column()
            input_grad()
            start_own(2)
            start_all(out_rows(zero()))

        @pl.when(t == OUT_IN)
        def _():
            wait_own(2)
            gain_rest()

        @pl.when((t >= OUT_IN) & (t < OUT_IN + N_OUT))
        def _():
            out_part(t - OUT_IN)

        n_end = jnp.minimum(jnp.minimum(n + 1, loaded * N_TILE), n_own)
        lax.fori_loop(n, n_end, tile, 0)
        return n_end, loaded + load.astype(jnp.int32)

    n, _ = loop(LAST + 1, body, (zero(), zero()))
    start_own(3)
    for j in range(n_cols):
        sum_ref[:, j * BLK:(j + 1) * BLK] = s_buf[j, :LANES, :]
    lax.fori_loop(n, n_own, tile, 0)
    shared(parts, 8, 1).wait_recv()
    dgain_ref[ALL] = jnp.sum(parts[ALL], axis=0)
    for slot in range(TRIO):
        keep_tile(0, slot).wait()
        give_tile(0, slot).wait_send()

    def received(n, carry):
        give_tile(n, 0).wait_recv()
        return carry

    loop(n_own, received, 0)
    wait_own(3)
    for copy in key_copies(pl.ds(0, QROWS)):
        copy.wait_send()
    shared(z_parts, QUAD, 0).wait_send()
    shared(parts, 8, 1).wait_send()


def main(x, dy, gain, pos, freq, w_q, w_k, w_v, w_o):
    model = x.shape[1]
    qkv = w_q.shape[1] + w_k.shape[1] + w_v.shape[1]
    gains = pltpu.VMEM((PAIR * N_PART, LANES), F32)
    queries, keys = pltpu.VMEM((TRIO, QROWS, LANES), BF16), pltpu.VMEM((SEQ, LANES), BF16)
    return pl.pallas_call(
        main_kernel,
        out_shape=[like((PAIR, *GRID) + x.shape, BF16), like((*GRID, 8, LANES), F32),
                   like((N_PIECE, PAIR, QUAD, PAIR, PAIR, QROWS, LANES), BF16), like((N_GATHER, BLK, BLK), F32),
                   like((LANES, model // 3), BF16), like(x.shape, F32), like(x.shape, BF16), like((PAIR * N_PART, LANES), F32)],
        in_specs=[vmem_spec()] * 5 + [any_spec()] * 4,
        out_specs=[any_spec()] * 4 + [vmem_spec()] * 4,
        scratch_shapes=[
            pltpu.VMEM(x.shape, BF16), queries, queries, keys, keys,
            pltpu.VMEM((*GRID, CHUNK, model), BF16), pltpu.VMEM((8, LANES), F32), pltpu.VMEM((1, model), F32), pltpu.VMEM((1, LANES), F32),
            pltpu.VMEM((*GRID, 8, LANES), F32), pltpu.VMEM((PAIR, LANES, LANES), F32), pltpu.VMEM((N_DEV * CHUNK, LANES), F32),
            pltpu.VMEM((QROWS, LANES), F32), pltpu.VMEM((8, LANES, TRIO * LANES), BF16),
            pltpu.VMEM((PAIR, 3, QROWS, LANES), BF16), pltpu.VMEM((LANES, SEQ), F32), pltpu.VMEM((LANES, SEQ), F32),
            pltpu.VMEM((SEQ // BLK, BLK, BLK), F32), pltpu.VMEM((TRIO, BLK, LANES), F32),
            pltpu.VMEM((QUAD, PAIR, QROWS, LANES), BF16), pltpu.VMEM((TRIO, 2, QROWS, LANES), BF16),
            pltpu.VMEM((PAIR, SEQ, BLK), BF16), pltpu.VMEM((PAIR, *GRID, LANES, BLK), BF16), pltpu.VMEM((TRIO, BLK, BLK), F32),
            pltpu.VMEM((LANES, qkv), BF16), pltpu.VMEM((LANES, PAIR * w_k.shape[1]), BF16), pltpu.VMEM((PAIR, HALF, qkv), BF16), pltpu.VMEM(x.shape, F32),
            gains, pltpu.VMEM((QUAD, PAIR * N_PART, LANES), F32), gains, pltpu.VMEM((8, PAIR * N_PART, LANES), F32),
            sems(1, N_STAGE), sems(1, N_STAGE), sems(RING, N_STAGE), sems(RING, N_STAGE),
            sems(TRIO), sems(TRIO), sems(), sems(8), sems(8),
            sems(N_PIECE, 2), sems(PAIR), sems(PAIR), sems(TRIO), sems(TRIO),
            sems(IN_GATHER * N_TILE), sems(TRIO), sems(TRIO), sems(QUAD), sems(PAIR, 4), sems(PAIR), sems(PAIR)],
        compiler_params=pltpu.CompilerParams(collective_id=0, has_side_effects=True, vmem_limit_bytes=VMEM_LIMIT),
    )(x, dy, gain, pos, freq, w_q, w_k, w_v, w_o)


N_LATE = N_PIECE - IN_GATHER
GROUP = IN_GATHER // N_LATE


def finish_kernel(sum_ref, o_ref, dx_ref, dgain_ref, w_ref, hd_ref, g_ref, t_ref,
                  y_ref, dx_out, dgain_out, wq_ref, wk_ref, wv_ref, wo_ref,
                  gbuf, abuf, obuf, cbuf, acc, wbuf, gsem, asem, osem, isem, csem, wsem):
    n_step, group = N_LATE * PER_PIECE, GROUP

    def operand(t):
        return operand_copy(hd_ref, abuf, asem, 1, t, odd(t))

    def cut(t):
        return pl.ds(pl.multiple_of(t * BLK, BLK), BLK)

    def lanes(i):
        return pl.ds(pl.multiple_of(i * LANES, LANES), LANES)

    def to_output(p, t, sub, src, sem):
        j = jnp.where(p == O_PIECES[0], 0, p - O_PIECES[0] - 2)
        return [pltpu.make_async_copy(
            src.at[pl.ds(i * LANES, LANES), :], wo_ref.at[lanes(TRIO * (sub * 4 + i) + j), cut(t)], sem.at[i])
            for i in range(QUAD)]

    def to_input(dst, place, t, sub, src, sem):
        return [pltpu.make_async_copy(
            src.at[:, pl.ds(i * LANES, LANES)], dst.at[cut(t), lanes(place(sub * 4 + i))], sem.at[i]) for i in range(QUAD)]

    def ins(n):
        return [pltpu.make_async_copy(t_ref.at[n * group + i], cbuf.at[lax.rem(n, TRIO), i], isem.at[lax.rem(n, TRIO), i])
                for i in range(group)]

    def start_outs(n):
        for i in range(group):
            m = n * group + i
            p, t, sub = lax.div(m, PER_PIECE), lax.rem(half_of(m), N_TILE), odd(m)
            src, sem = cbuf.at[lax.rem(n, TRIO), i], csem.at[lax.rem(n, TRIO), i]
            for cond, copies in (
                (p < 3, lambda: to_input(wq_ref, lambda g: TRIO * g + p, t, sub, src, sem)),
                (p == KEY_PIECE, lambda: to_input(wk_ref, lambda g: g, t, sub, src, sem)),
                (p == KEY_PIECE + 1, lambda: to_input(wv_ref, lambda g: g, t, sub, src, sem)),
                ((p == O_PIECES[0]) | (p == O_PIECES[1]), lambda: to_output(p, t, sub, src, sem)),
            ):
                @pl.when(cond)
                def _(copies=copies):
                    for c in copies():
                        c.start()

    def wait_outs(n):
        for i in range(group):
            for c in to_output(IN_GATHER, 0, 0, cbuf.at[0, i], csem.at[lax.rem(n, TRIO), i]):
                c.wait()

    def weight(i):
        slot = odd(i)
        return pltpu.make_async_copy(w_ref.at[lanes(TRIO * i + 2), :], wbuf.at[slot], wsem.at[slot])

    for late in range(N_LATE):
        for sub in range(PAIR):
            start_all(piece_copies(g_ref, gbuf, gsem, IN_GATHER + late, sub, late * 2 + sub))
    operand(zero()).start()
    weight(zero()).start()
    acc[ALL] = sum_ref[ALL]
    dx_out[ALL] = dx_ref[ALL]
    dgain_out[ALL] = dgain_ref[ALL]

    def step(n, carry):
        t, late, sub = lax.div(n, PAIR * N_LATE), lax.rem(half_of(n), N_LATE), odd(n)
        p, held = IN_GATHER + late, late * 2 + sub
        slot = lax.rem(n, TRIO)

        @pl.when(n >= 3)
        def _():
            wait_outs(n - 3)
        for c in ins(n):
            c.start()

        @pl.when(n >= 1)
        def _():
            for c in ins(n - 1):
                c.wait()
            start_outs(n - 1)

        @pl.when(held == 0)
        def _():
            operand(t).wait()

            @pl.when(nxt(t) < N_TILE)
            def _():
                operand(nxt(t)).start()

        @pl.when(n < PAIR * N_LATE)
        def _():
            wait_piece(gbuf, gsem, held)

        @pl.when(n >= 3)
        def _():
            for c in to_output(IN_GATHER, 0, 0, obuf.at[0], osem.at[slot]):
                c.wait()
        @pl.when(n < 8)
        def _():
            weight(n).wait()

            @pl.when(n < 7)
            def _():
                weight(n + 1).start()
            acc[ALL] += jnp.dot(o_ref[:, lanes(n)], wbuf[odd(n)], preferred_element_type=F32)
        obuf[slot] = tile_product(abuf[odd(t)], gbuf[held], True)
        for c in to_output(p, t, sub, obuf.at[slot], osem.at[slot]):
            c.start()
        return carry

    loop(n_step, step, 0)
    y_ref[ALL] = acc[ALL].astype(BF16)
    for c in ins(n_step - 1):
        c.wait()
    start_outs(jnp.int32(n_step - 1))
    for n in range(n_step - 3, n_step):
        wait_outs(n)
        for c in to_output(IN_GATHER, 0, 0, obuf.at[0], osem.at[n % 3]):
            c.wait()


def finish(x, o, dx, dgain, w_o, hd, g, tiles):
    model, kv = hd.shape[2], 8 * LANES
    return pl.pallas_call(
        finish_kernel,
        out_shape=[like(x.shape, BF16), like(dx.shape, BF16), like(dgain.shape, F32)]
        + [like((model, n), F32) for n in (TRIO * kv, kv, kv)] + [like((TRIO * kv, model), F32)],
        in_specs=[vmem_spec()] * 4 + [any_spec()] * 4,
        out_specs=[vmem_spec()] * 3 + [any_spec()] * 4,
        scratch_shapes=[pltpu.VMEM((PAIR * N_LATE, SEQ, BLK), BF16), pltpu.VMEM((PAIR, SEQ, BLK), BF16), pltpu.VMEM((TRIO, BLK, BLK), F32),
                        pltpu.VMEM((TRIO, GROUP, BLK, BLK), F32), pltpu.VMEM(x.shape, F32), pltpu.VMEM((PAIR, LANES, model), BF16),
                        sems(PAIR * N_LATE), sems(PAIR), sems(TRIO, 4), sems(TRIO, GROUP), sems(TRIO, GROUP, 4), sems(PAIR)],
        cost_estimate=pl.CostEstimate(flops=4 * SEQ * kv * model, bytes_accessed=250 * 2**20, transcendentals=0),
        compiler_params=pltpu.CompilerParams(vmem_limit_bytes=VMEM_LIMIT),
    )(x, o, dx, dgain, w_o, hd, g, tiles)


def solution(mesh):
    assert mesh.shape['hp'] == 4 and mesh.shape['cp'] == 8

    def device_step(hidden, grad_out, positions, norm_gain, w_q, w_k, w_v, w_o, inv_freq):
        model = hidden.shape[1]
        hd, _, gathered, tiles, o_own, total, dx, gains = main(
            hidden, grad_out, norm_gain, positions, inv_freq, w_q, w_k, w_v, w_o)
        output, grad_hidden, grad_gain, grad_wq, grad_wk, grad_wv, grad_wo = finish(
            total, o_own, dx, gains, w_o, hd.reshape(2, SEQ, model), gathered, tiles)
        grad_gain = grad_gain.reshape(-1)
        return output, grad_hidden, grad_wq, grad_wk, grad_wv, grad_wo, grad_gain

    rows, whole = P(('cp', 'hp'), None), P()
    return jax.shard_map(
        device_step, mesh=mesh,
        in_specs=(rows, rows, P(('cp', 'hp')), whole, whole, whole, whole, whole, whole),
        out_specs=(rows, rows, whole, whole, whole, whole, whole), check_vma=False)
```

```python
import functools
import jax
import jax.numpy as jnp
from jax import lax
from jax.experimental import pallas as pl
from jax.experimental.pallas import tpu as pltpu
from jax.sharding import PartitionSpec as P

NORM_EPS = 1e-5
ALL = Ellipsis
EVERY = slice(None)
PAIR, TRIO, QUAD = 2, 3, 4
GRID = (PAIR, PAIR, PAIR, QUAD)
BY_COLUMN = {'axis': 0, 'keepdims': True}
BY_ROW = {'axis': 1, 'keepdims': True}
F32 = jnp.float32
BF16 = jnp.bfloat16
LANES = 128
BLK = 512
HALF = BLK // 2
SEQ = 8 * BLK
QROWS = PAIR * BLK
UPP = 8
LAG = 2
RING = 20
VMEM_LIMIT = 64 * 2**20 - 2**16
NT = (((1,), (1,)), ((), ()))
TN = (((0,), (0,)), ((), ()))

STAGES = {
    'C': ('z1', 'z2', 'z3', 'y', 'x', 'd'),
    'D': ('z1', 'z2', 'z3', 'x', 'y', 'd'),
    'E': ('x', 'y', 'z1', 'z2', 'z3', 'd'),
    'F': ('y', 'x', 'z1', 'z2', 'z3', 'd'),
}
N_STAGE = 6


def odd(i):
    return lax.rem(i, PAIR)


def half_of(i):
    return lax.div(i, PAIR)


def nxt(i):
    return i + 1


def zero():
    return jnp.int32(0)


def loop(n, body, init):
    return lax.fori_loop(0, n, body, init)


class Gather:
    def __init__(self, send_sem, recv_sem, mix, base=0):
        self.mix, self.base = mix, base
        self.z = lax.axis_index('hp')
        cp = lax.axis_index('cp')
        self.c, self.x, self.y = odd(cp), odd(half_of(cp)), lax.div(cp, 4)
        self.send_sem, self.recv_sem = send_sem, recv_sem

    def device(self, **moved):
        at = {name: moved.get(name, getattr(self, name)) for name in 'cxyz'}
        return at['z'], (at['y'] * PAIR + at['x']) * PAIR + at['c']

    def copies(self, sem_row, kind, view, stage):
        c, x, y, z = self.c, self.x, self.y, self.z
        order = STAGES[kind]
        done = {st[0] for st in order[:order.index(stage)]}
        every = EVERY
        gx, gy, gz = (every if d in done else v for d, v in (('x', x), ('y', y), ('z', z)))
        slot = order.index(stage)

        def copy(place, device):
            return lambda: pltpu.make_async_remote_copy(
                place, place, self.send_sem.at[sem_row, slot], self.recv_sem.at[sem_row, slot],
                device_id=device, device_id_type=pl.DeviceIdType.MESH)

        if stage in 'xyd':
            mine, other, dev = {
                'x': lambda: ((c, x, gy, gz), (c, 1 - x, gy, gz), self.device(x=1 - x)),
                'y': lambda: ((c, gx, y, gz), (c, gx, 1 - y, gz), self.device(y=1 - y)),
                'd': lambda: ((c, EVERY, EVERY, EVERY), (1 - c, EVERY, EVERY, EVERY), self.device(c=1 - c)),
            }[stage]()
            out, back = [(True, copy(view(*mine), dev))], [(True, copy(view(*other), dev))]
            return {'start': out, 'sent': out, 'recv': back}
        hop = int(stage[1])
        ups, downs = (z >= hop - 1) & (z < 3), (z + hop <= 4) & (z > 0)
        above, below = self.device(z=jnp.minimum(z + 1, 3)), self.device(z=jnp.maximum(z - 1, 0))

        def counted(one, other):
            return [(one != other, copy(view(c, gx, gy, 0), above)), (one & other, copy(view(c, gx, gy, pl.ds(0, PAIR)), above))]

        return {
            'start': [(ups, copy(view(c, gx, gy, jnp.maximum(z - hop + 1, 0)), above)),
                      (downs, copy(view(c, gx, gy, jnp.minimum(z + hop - 1, 3)), below))],
            'sent': counted(ups, downs),
            'recv': counted(z >= hop, z + hop <= 3),
        }

    def run(self, sem_row, kind, view, stage, what):
        for cond, copy in self.copies(sem_row, kind, view, stage)[what]:
            def act(copy=copy):
                if what == 'start':
                    copy().start()
                elif what == 'sent':
                    copy().wait_send()
                else:
                    copy().wait_recv()

            if cond is True:
                act()
            else:
                pl.when(cond)(act)

    def advance(self, sem_row, kind, view, s):
        if 0 < s <= N_STAGE:
            self.run(sem_row, kind, view, STAGES[kind][s - 1], 'recv')
        if s < N_STAGE:
            self.run(sem_row, kind, view, STAGES[kind][s], 'start')
        if s > N_STAGE:
            for stage in STAGES[kind]:
                self.run(sem_row, kind, view, stage, 'sent')

    def kinds(self, u):
        word, at = lax.div(u, 16), lax.rem(u, 16)
        code = jnp.int32(self.mix[0])
        for i in range(1, len(self.mix)):
            code = jnp.where(word == i, self.mix[i], code)
        code = lax.shift_right_logical(code, at * 2) & 3
        return tuple((kind, code == i) for i, kind in enumerate('CDEF'))

    def tick(self, t, n_units, view):
        for s in range(N_STAGE + 2):
            u = t - s * LAG

            @pl.when((u >= 0) & (u < n_units))
            def _(u=u, s=s):
                for kind, is_kind in self.kinds(u):
                    @pl.when(is_kind)
                    def _(kind=kind):
                        self.advance(lax.rem(u + self.base, RING), kind, view(u), s)


def turn(v):
    return pltpu.roll(v, LANES // 2, 1)


def low_lanes(shape):
    return lax.broadcasted_iota(jnp.int32, shape, 1) < LANES // 2


def cos_sin(cs):
    low = low_lanes(cs.shape)
    other = turn(cs)
    return jnp.where(low, cs, other), jnp.where(low, -other, cs)


def any_spec():
    return pl.BlockSpec(memory_space=pl.ANY)


def vmem_spec():
    return pl.BlockSpec(memory_space=pltpu.VMEM)


def sems(*shape):
    return pltpu.SemaphoreType.DMA(shape) if shape else pltpu.SemaphoreType.DMA


def like(shape, dtype):
    return jax.ShapeDtypeStruct(shape, dtype)


def start_all(copies):
    for copy in copies:
        copy.start()


def wait_all(copies):
    for copy in copies:
        copy.wait()


N_PIECE = 8
O_PIECES = (3, 6, 7)
KEY_PIECE = 4
N_TILE = 6
PER_PIECE = PAIR * N_TILE
IN_GATHER = 7
N_GATHER = IN_GATHER * PER_PIECE


def tile_product(operand, piece, of_output):
    left, right = (piece, operand) if of_output else (operand, piece)
    return lax.dot_general(left, right, TN, preferred_element_type=F32)


def operand_copy(hd_ref, abuf, asem, which, t, slot):
    return pltpu.make_async_copy(
        hd_ref.at[which, :, pl.ds(pl.multiple_of(t * BLK, BLK), BLK)], abuf.at[slot], asem.at[slot])


def piece_copies(g_ref, gbuf, gsem, p, core, slot):
    return [pltpu.make_async_copy(g_ref.at[p, core, z, r // 2, r % 2],
                                  gbuf.at[slot, pl.ds(r * QROWS, QROWS), pl.ds(z * LANES, LANES)], gsem.at[slot])
            for z in range(QUAD) for r in range(QUAD)]


def wait_piece(gbuf, gsem, slot):
    pltpu.make_async_copy(gbuf.at[slot], gbuf.at[slot], gsem.at[slot]).wait()


def lane_groups(op, s):
    out = s[:, :LANES]
    for i in range(1, s.shape[1] // LANES):
        out = op(out, s[:, i * LANES:(i + 1) * LANES])
    return out


class Attention:
    def __init__(self, q, do, k, v, cs, out, dk_acc, dv_acc, s, state, quarter):
        self.q, self.do, self.k, self.v, self.cs, self.out = q, do, k, v, cs, out
        self.dk, self.dv, self.s, self.state = dk_acc, dv_acc, s, state
        self.quarter = quarter
        self.scale = LANES ** -0.5
        self.factor = self.scale * 1.4426950408889634

    def step(self, t):
        head, half = lax.div(t, 8), odd(lax.div(t, 4))
        n_key = jnp.where(half == 0, self.quarter + 1, SEQ // BLK - self.quarter)
        rows = pl.ds(pl.multiple_of(half * BLK, BLK), BLK)
        for i, act in enumerate((self.scores, self.exps, self.values, self.grads)):
            @pl.when(lax.rem(t, 4) == i)
            def _(act=act):
                act(head, half, n_key, rows)

    def keys(self, kb):
        return pl.ds(pl.multiple_of(kb * BLK, BLK), BLK)

    def zeros(self):
        return jnp.zeros((BLK, LANES), F32)

    def keep(self, i, column):
        self.state[i] = jnp.broadcast_to(column, (BLK, LANES))

    def kept(self, i):
        return self.state[i, :, :1]

    def scores(self, head, half, n_key, rows):
        q = self.q[head, rows, :]

        def block(kb, m, diagonal=False):
            s = lax.dot_general(q, self.k[self.keys(kb), :], NT, preferred_element_type=F32)
            if diagonal:
                visible = lax.broadcasted_iota(jnp.int32, s.shape, 0) >= lax.broadcasted_iota(jnp.int32, s.shape, 1)
                s = jnp.where(visible, s, -1e30)
            self.s[kb] = s
            return jnp.maximum(m, lane_groups(jnp.maximum, s))

        m = loop(n_key - 1, block, self.zeros() - 1e30)
        m = block(n_key - 1, m, diagonal=True)
        self.keep(0, jnp.max(m, **BY_ROW) * self.factor)

    def exps(self, head, half, n_key, rows):
        m = self.kept(0)

        def block(kb, total):
            e = jnp.exp2(self.s[kb] * self.factor - m)
            self.s[kb] = e
            return total + lane_groups(jnp.add, e)

        total = loop(n_key, block, self.zeros())
        self.keep(0, 1.0 / jnp.sum(total, **BY_ROW))

    def sides(self, half):
        for side in range(PAIR):
            place = (half * (1 - side) + (1 - half) * side) * HALF
            yield pl.ds(pl.multiple_of(place, HALF), HALF), pl.ds(pl.multiple_of(side * BLK + half * HALF, HALF), HALF)

    def values(self, head, half, n_key, rows):
        do, inv = self.do[head, rows, :], self.kept(0)
        turned = do.T

        def block(kb, o):
            p = (self.s[kb] * inv).astype(BF16)
            self.dv[:, self.keys(kb)] += jnp.dot(turned, p, preferred_element_type=F32)
            return o + jnp.dot(p, self.v[self.keys(kb), :], preferred_element_type=F32)

        o = loop(n_key, block, self.zeros()).astype(BF16).astype(F32)
        self.keep(1, jnp.sum(do.astype(F32) * o, **BY_ROW))
        self.state[2] = o
        for place, stored in self.sides(half):
            self.out[1, head, stored, :] = self.state[2, place, :].astype(BF16)

    def grads(self, head, half, n_key, rows):
        do, inv, delta = self.do[head, rows, :], self.kept(0), self.kept(1)
        turned = self.q[head, rows, :].T

        def block(kb, dq):
            dp = lax.dot_general(do, self.v[self.keys(kb), :], NT, preferred_element_type=F32)
            ds = (self.s[kb] * inv * (dp - delta)).astype(BF16)
            self.dk[:, self.keys(kb)] += jnp.dot(turned, ds, preferred_element_type=F32)
            return dq + jnp.dot(ds, self.k[self.keys(kb), :], preferred_element_type=F32)

        dq = loop(n_key, block, self.zeros()) * self.scale
        self.state[2] = dq.astype(BF16).astype(F32)
        for place, stored in self.sides(half):
            cos, sin = cos_sin(self.cs[stored, :])
            part = self.state[2, place, :]
            self.out[0, head, stored, :] = (part * cos - turn(part) * sin).astype(BF16)

    def key_grads(self, out):
        for pair in range(8):
            for i, (acc, factor) in enumerate(((self.dk, self.scale), (self.dv, 1.0))):
                for part, block in enumerate((pair, 15 - pair)):
                    out[pair // 2, i, pl.ds(pair % PAIR * BLK + part * HALF, HALF), :] = (
                        acc[:, pl.ds(block * HALF, HALF)].T * factor).astype(BF16)


ROWS_UNIT = 8
N_IN = LANES // ROWS_UNIT
N_STEP = 24
N_UNIT = N_PIECE * UPP
N_PART = 12
SEND_DO = N_PART + 1
DELAY = N_STAGE * LAG
CHUNK = PAIR * ROWS_UNIT
N_CHUNK = LANES // CHUNK
PROJECT = DELAY + 2
ATTEND = PROJECT + PAIR * N_CHUNK - 1
ATTENDED = ATTEND + N_STEP
START = ATTEND + 4
N_SEND = 8
KEYS_IN = START + KEY_PIECE * UPP
QUERY_IN = START + 3 * UPP + DELAY
OWN_IN = START + O_PIECES[1] * UPP + DELAY
QUERIES_DONE = QUERY_IN + N_PART
FIRST_O = START + (O_PIECES[0] + 1) * UPP + DELAY
OUT_IN = OWN_IN + N_PART // 2 + 2
LAST = START + N_UNIT + DELAY + LAG
N_DEV = 32


def main_kernel(x_ref, dy_ref, gain_ref, mypos_ref, freq_ref, wq_ref, wk_ref, wv_ref, wo_ref,
                hd_ref, pos_ref, g_ref, t_ref, o_ref, sum_ref, dx_ref, dgain_ref,
                h_buf, q_buf, do_buf, k_buf, v_buf, rows_buf, mypos_buf, gain_buf, freq_buf, pos_buf, pos_t, cs_buf, own_cs, do_parts,
                piece_buf, dk_acc, dv_acc, s_buf, state, dkv_buf, peer_buf, gbuf, abuf, obuf, own_buf, oo_buf, w_buf, dn_buf, part_buf, z_parts, sum_buf, parts,
                cs_send, cs_recv, send_sem, recv_sem, first_sem, proj_sem, rows_sem, do_send, do_recv,
                lsem, gsem, asem, osem, tsend, trecv, psend, precv, rsem, wsem, gain_send, gain_recv):
    net_in, net_cs, net = Gather(send_sem, recv_sem, (306463953, 1175604295)), Gather(cs_send, cs_recv, (306463953, 1175604295)), Gather(send_sem, recv_sem, (-398134202, 1293043604, -2075179916, 958350436), START)
    quarter = net.y * 2 + net.x
    head = net.c * 4 + net.z
    spot = (net.y, net.x, net.c, net.z)
    attn = Attention(q_buf, do_buf, k_buf, v_buf, own_cs, piece_buf, dk_acc, dv_acc, s_buf, state, quarter)

    def inv_rms():
        x = x_ref[ALL].astype(F32)
        return lax.rsqrt(jnp.mean(x * x, **BY_ROW) + NORM_EPS)

    barrier = pltpu.get_barrier_semaphore()

    def greet(**moved):
        pl.semaphore_signal(barrier, inc=1, device_id=net.device(**moved), device_id_type=pl.DeviceIdType.MESH)

    greet(x=1 - net.x)
    greet(y=1 - net.y)
    greet(c=1 - net.c)
    inner = (net.z > 0).astype(jnp.int32) + (net.z < 3).astype(jnp.int32)

    @pl.when(net.z > 0)
    def _():
        greet(z=net.z - 1)

    @pl.when(net.z < 3)
    def _():
        greet(z=net.z + 1)

    gain_buf[ALL] = gain_ref[ALL].astype(F32).reshape(gain_buf.shape)
    freq_buf[ALL] = jnp.concatenate([freq_ref[ALL], freq_ref[ALL]], axis=0).reshape(freq_buf.shape)
    mypos_buf[ALL] = jnp.broadcast_to(mypos_ref[ALL].astype(F32).reshape(1, LANES), mypos_buf.shape)
    h_buf[ALL] = (x_ref[ALL].astype(F32) * inv_rms() * gain_buf[ALL]).astype(BF16)
    first = [pltpu.make_async_copy(src, dst, first_sem.at[i]) for i, (src, dst) in enumerate((
        (h_buf, hd_ref.at[(0, *spot)]), (dy_ref, hd_ref.at[(1, *spot)]), (mypos_buf, pos_ref.at[spot])))]
    start_all(first)
    wait_all(first)
    pl.semaphore_wait(barrier, TRIO + inner)
    q_cols = pl.ds(pl.multiple_of(head * TRIO * LANES, LANES), TRIO * LANES)
    kv_cols = pl.ds(pl.multiple_of(head * LANES, LANES), LANES)
    w_rows = slice(0, wq_ref.shape[0])
    wq_buf, wkv_buf = gbuf.at[0, w_rows, :TRIO * LANES], gbuf.at[1, w_rows, :PAIR * LANES]
    weights = [pltpu.make_async_copy(src, dst, proj_sem.at[i]) for i, (src, dst) in enumerate((
        (wq_ref.at[:, q_cols], wq_buf), (wk_ref.at[:, kv_cols], gbuf.at[1, w_rows, :LANES]),
        (wv_ref.at[:, kv_cols], gbuf.at[1, w_rows, LANES:PAIR * LANES])))]

    def view_in(u):
        rows = pl.ds(pl.multiple_of(lax.rem(u, N_IN) * ROWS_UNIT, ROWS_UNIT), ROWS_UNIT)
        which = lax.div(u, N_IN)
        return lambda c, x, y, z: hd_ref.at[which, y, x, c, z, rows, :]

    def view_cs(c, x, y, z):
        return pos_ref.at[y, x, c, z]

    def part(i, width=HALF):
        return pl.ds(pl.multiple_of(i * width, width), width)

    def wo_rows(i):
        slot = odd(i)
        return pltpu.make_async_copy(wo_ref.at[part(i), :], w_buf.at[slot, :, :wo_ref.shape[1]], wsem.at[slot, 0])

    def head_grad(i):
        slot = odd(i)
        wo_rows(i).wait()

        @pl.when(nxt(i) < N_PART)
        def _():
            wo_rows(nxt(i)).start()
        own_buf[:, part(i)] = lax.dot_general(
            dy_ref[ALL], w_buf[slot, :, :wo_ref.shape[1]], NT, preferred_element_type=F32).astype(BF16)

    def do_copy(step, mine):
        me = net.c * 4 + net.z
        other = lax.rem(me + step, 8)
        slot = me if mine else lax.rem(me + 8 - step, 8)
        return pltpu.make_async_remote_copy(
            own_buf.at[:, part(other, TRIO * LANES)], do_parts.at[slot], do_send.at[step], do_recv.at[step],
            device_id=net.device(c=lax.div(other, 4), z=lax.rem(other, 4)), device_id_type=pl.DeviceIdType.MESH)

    own_do = pltpu.make_async_copy(own_buf.at[:, part(head, TRIO * LANES)], do_parts.at[head], do_send.at[0])

    def query_row(c, z):
        return c * HALF + z * LANES if z < 2 else BLK + (1 - c) * HALF + (z - 2) * LANES

    def take_do():
        for step in range(1, 8):
            do_copy(step, False).wait_recv()
        for c in range(PAIR):
            for z in range(QUAD):
                for j in range(TRIO):
                    do_buf[j, pl.ds(query_row(c, z), LANES), :] = do_parts[c * 4 + z, :, j * LANES:(j + 1) * LANES]

    every = EVERY

    def chunk(k, base=0):
        return pl.ds(pl.multiple_of(base + k * CHUNK, CHUNK), CHUNK)

    def chunk_rows(k):
        return pltpu.make_async_copy(hd_ref.at[0, every, every, every, every, chunk(k), every], rows_buf, rows_sem)

    def take_positions():
        copy = pltpu.make_async_copy(pos_ref, pos_buf, rows_sem)
        copy.start()
        copy.wait()
        for i in range(PAIR):
            pos_t[i] = pos_buf[i].reshape(LANES, LANES).T

    def angles(k):
        for dev in range(N_DEV):
            column = pos_t[dev // 16, chunk(k), dev % 16 * 8:dev % 16 * 8 + 1]
            cs_buf[dev * CHUNK:(dev + 1) * CHUNK, :] = jnp.broadcast_to(column, (CHUNK, LANES)) * freq_buf[ALL]
        angle = cs_buf[ALL]
        cs_buf[ALL] = jnp.where(low_lanes(angle.shape), jnp.cos(angle), jnp.sin(angle))

    def rotate(v, cs):
        cos, sin = cos_sin(cs)
        return (v * cos + turn(v) * sin).astype(BF16)

    def project(k):
        chunk_rows(k).wait()
        n_rows = N_DEV * CHUNK
        kv = jnp.dot(rows_buf[ALL].reshape(n_rows, -1), wkv_buf[ALL], preferred_element_type=F32)
        key = rotate(kv[:, :LANES], cs_buf[ALL])
        value = kv[:, LANES:].astype(BF16)
        for cp in range(8):
            for z in range(QUAD):
                block = 2 * cp + z if z < 2 else 28 - 2 * cp + z
                rows = slice((cp * 4 + z) * CHUNK, (cp * 4 + z + 1) * CHUNK)
                k_buf[chunk(k, block * LANES), :] = key[rows]
                v_buf[chunk(k, block * LANES), :] = value[rows]
        mine, cs = rows_buf[net.y, net.x].reshape(LANES, -1), cs_buf[part(quarter, LANES), :]
        q = jnp.dot(mine, wq_buf[ALL], preferred_element_type=F32)
        for j in range(TRIO):
            p = rotate(q[:, j * LANES:(j + 1) * LANES], cs)
            for c in range(PAIR):
                for z in range(QUAD):
                    rows = slice((c * 4 + z) * CHUNK, (c * 4 + z + 1) * CHUNK)
                    q_buf[j, chunk(k, query_row(c, z)), :] = p[rows]
                    if j == 0:
                        own_cs[chunk(k, c * BLK + z * LANES), :] = cs[rows]

    def local(p, i, src, rows=pl.ds(0, QROWS)):
        return pltpu.make_async_copy(src, g_ref.at[p, net.c, net.z, net.y, net.x, rows, :], lsem.at[p, i])

    def step_pieces(step):
        head, half = lax.div(step, 8), odd(lax.div(step, 4))
        out_piece = jnp.where(head == 0, O_PIECES[0], O_PIECES[0] + 2 + head)
        return [local(p, side, piece_buf.at[i, head, rows], rows) for i, p in ((0, head), (1, out_piece))
                for side, (_, rows) in enumerate(attn.sides(half))]

    def key_copies(rows):
        for i, moved in enumerate(('x', 'y', 'xy')):
            x, y = (1 - at if name in moved else at for name, at in (('x', net.x), ('y', net.y)))
            yield pltpu.make_async_remote_copy(
                dkv_buf.at[y * 2 + x, :, rows], peer_buf.at[i, :, rows], psend.at[i], precv.at[i],
                device_id=net.device(x=x, y=y), device_id_type=pl.DeviceIdType.MESH)

    def add_peers():
        for copy in key_copies(pl.ds(0, QROWS)):
            copy.wait_recv()
        total = dkv_buf[quarter].astype(F32)
        for i in range(TRIO):
            total = total + peer_buf[i].astype(F32)
        total = total.astype(BF16)
        cos, sin = cos_sin(own_cs[ALL])
        dk = total[0].astype(F32)
        piece_buf[0, 0] = (dk * cos - turn(dk) * sin).astype(BF16)
        piece_buf[0, 1] = total[1]
        kv = [local(KEY_PIECE + i, 0, piece_buf.at[0, i]) for i in range(PAIR)]
        start_all(kv)
        wait_all(kv)

    def view(u):
        p, k = lax.div(u, UPP), lax.rem(u, UPP)
        two = half_of(k)
        rows = part(odd(two) * 4 + half_of(two) * 2 + odd(k), QROWS // UPP)
        return lambda c, x, y, z: g_ref.at[p, c, z, y, x, rows, :]

    def place(n):
        return lax.div(n, N_TILE) * PER_PIECE + lax.rem(n, N_TILE) * 2 + net.c

    def keep_tile(n, slot):
        return pltpu.make_async_copy(obuf.at[slot], t_ref.at[place(n)], osem.at[slot])

    def give_tile(n, slot):
        return pltpu.make_async_remote_copy(
            obuf.at[slot], t_ref.at[place(n)], tsend.at[slot], trecv.at[n],
            device_id=net.device(c=1 - net.c), device_id_type=pl.DeviceIdType.MESH)

    def of_output(p):
        return (p == O_PIECES[0]) | (p == O_PIECES[1])

    def operand(n):
        which, slot = of_output(lax.div(n, N_TILE)).astype(jnp.int32), odd(n)
        return pltpu.make_async_copy(
            hd_ref.at[which, every, every, every, every, every, part(lax.rem(n, N_TILE), BLK)], abuf.at[slot], asem.at[slot])

    def piece(p):
        return piece_copies(g_ref, gbuf, gsem, p, net.c, odd(p))

    n_own = IN_GATHER * N_TILE

    def tile(n, carry):
        slot = lax.rem(n, TRIO)
        p = lax.div(n, N_TILE)

        @pl.when(lax.rem(n, N_TILE) == 0)
        def _():
            wait_piece(gbuf, gsem, odd(p))
        operand(n).wait()

        @pl.when(nxt(n) < n_own)
        def _():
            operand(nxt(n)).start()

        @pl.when(n >= 3)
        def _():
            keep_tile(n, slot).wait()
            give_tile(n, slot).wait_send()
        for output in (False, True):
            @pl.when(of_output(p) == output)
            def _(output=output):
                obuf[slot] = tile_product(abuf[odd(n)].reshape(SEQ, BLK), gbuf[odd(p)], output)
        keep_tile(n, slot).start()
        give_tile(n, slot).start()
        return carry

    kv = wk_ref.shape[1]
    groups = (((0, 1, 2), own_buf, slice(0, TRIO * kv)), ((KEY_PIECE, KEY_PIECE + 1), own_buf, slice(TRIO * kv, 5 * kv)),
              (O_PIECES[:1], oo_buf, slice(0, kv)), (O_PIECES[1:2], oo_buf, slice(kv, PAIR * kv)), (O_PIECES[2:], o_ref, slice(0, kv)))

    def start_own(i):
        rows = pl.ds(pl.multiple_of(net.c * BLK + net.z * LANES, LANES), LANES)
        pieces, dst, cols = groups[i]
        for k, p in enumerate(pieces):
            for g in range(8):
                col = cols.start // LANES + (TRIO * g + k if len(pieces) == 3 else 8 * k + g)
                pltpu.make_async_copy(
                    g_ref.at[p, g // 4, g % 4, net.y, net.x, rows, :], dst.at[:, pl.ds(col * LANES, LANES)], rsem.at[i]).start()

    def wait_own(i):
        _, dst, cols = groups[i]
        pltpu.make_async_copy(dst.at[:, cols], dst.at[:, cols], rsem.at[i]).wait()

    def weight_rows(turn, i):
        slot = odd(i)
        if turn == 0:
            places = ((wq_ref, part(i), 0, TRIO * kv),)
        else:
            places = [(src, part(i * 2 + j), (j * 2 + k) * kv, kv) for j in range(PAIR) for k, src in enumerate((wk_ref, wv_ref))]
        return [pltpu.make_async_copy(src.at[rows, :], w_buf.at[slot, :, pl.ds(at, width)], wsem.at[slot, j])
                for j, (src, rows, at, width) in enumerate(places)]

    def norm_grad(turn, i, n_steps):
        slot = odd(i)
        wait_all(weight_rows(turn, i))

        @pl.when(nxt(i) < n_steps)
        def _():
            start_all(weight_rows(turn, nxt(i)))
        if turn == 0:
            dn_buf[:, part(i)] = lax.dot_general(
                own_buf[:, :TRIO * kv], w_buf[slot, :, :TRIO * kv], NT, preferred_element_type=F32)
            return
        for j in range(PAIR):
            block = i * 2 + j
            dn = dn_buf[:, part(block)] + lax.dot_general(
                own_buf[:, TRIO * kv:], w_buf[slot, :, pl.ds(j * PAIR * kv, PAIR * kv)], NT, preferred_element_type=F32)
            dn_buf[:, part(block)] = dn
            x_hat = x_ref[:, part(block)].astype(F32) * inv_rms()
            total = jnp.sum(dn * x_hat, **BY_COLUMN)
            for k in range(PAIR):
                part_buf[pl.ds(block * 2 + k, 1), :] = total[:, k * LANES:(k + 1) * LANES]

    column = (net.y * PAIR + net.x) * PAIR + net.c

    def share(src, dst, slot, n, sem, device):
        def send(step, carry):
            pltpu.make_async_remote_copy(
                src, dst.at[slot], gain_send.at[sem], gain_recv.at[sem],
                device_id=device(lax.rem(slot + step, n)), device_id_type=pl.DeviceIdType.MESH).start()
            return carry

        mine = pltpu.make_async_copy(src, dst.at[slot], rows_sem)
        mine.start()
        mine.wait()
        lax.fori_loop(1, n, send, 0)

    def shared(dst, n, sem):
        rest = dst.at[pl.ds(1, n - 1)]
        return pltpu.make_async_remote_copy(
            rest, rest, gain_send.at[sem], gain_recv.at[sem],
            device_id=net.device(c=1 - net.c), device_id_type=pl.DeviceIdType.MESH)

    def gain_column():
        share(part_buf, z_parts, net.z, QUAD, 0, lambda z: net.device(z=z))

    def gain_rest():
        shared(z_parts, QUAD, 0).wait_recv()
        sum_buf[ALL] = jnp.sum(z_parts[ALL], axis=0)
        share(sum_buf, parts, column, 8, 1, lambda k: (net.z, k))

    def input_grad():
        x_hat = x_ref[ALL].astype(F32) * inv_rms()
        d_hat = dn_buf[ALL] * gain_buf[ALL]
        dx_ref[ALL] = (dy_ref[ALL].astype(F32) + inv_rms() * (
            d_hat - x_hat * jnp.mean(d_hat * x_hat, **BY_ROW))).astype(BF16)

    n_cols = x_ref.shape[1] // BLK

    def out_rows(i):
        slot = odd(i)
        head = lax.rem(i, 4) * 6 + lax.div(i, 4)
        return [pltpu.make_async_copy(
            wo_ref.at[part(head + TRIO * j, LANES), :], w_buf.at[slot, j * LANES:(j + 1) * LANES, :wo_ref.shape[1]], wsem.at[slot, j])
            for j in range(PAIR)]

    def out_part(i):
        slot = odd(i)
        wait_all(out_rows(i))

        @pl.when(lax.rem(i, QUAD) < 3)
        def _():
            start_all(out_rows(nxt(i)))
        left = oo_buf[:, part(i)]
        for j in range(n_cols):
            cols = slice(j * BLK, (j + 1) * BLK)
            term = jnp.dot(left, w_buf[slot, :, cols], preferred_element_type=F32)
            before = jnp.where(i == 0, x_ref[:, cols].astype(F32), s_buf[j, :LANES, :])
            s_buf[j, :LANES, :] = before + term

    def body(t, carry):
        n, loaded = carry
        since = t - ATTEND

        @pl.when(t == 1)
        def _():
            wo_rows(zero()).start()
            start_all(weights)

        @pl.when(t == SEND_DO + 1)
        def _():
            own_do.start()
            for step in range(1, 8):
                do_copy(step, True).start()
            wait_all(weights)

        @pl.when((since > 0) & (t <= ATTENDED) & (lax.rem(since, 4) == 0))
        def _():
            wait_all(step_pieces(since - 1))

        @pl.when(t == ATTENDED)
        def _():
            attn.key_grads(dkv_buf)

        @pl.when((t >= ATTENDED) & (t < ATTENDED + N_SEND))
        def _():
            start_all(key_copies(part(t - ATTENDED, QROWS // N_SEND)))

        @pl.when(t == KEYS_IN)
        def _():
            add_peers()
        net_in.tick(t, PAIR * N_IN, view_in)
        net.tick(t - START, N_UNIT, view)
        for s in range(N_STAGE + 2):
            @pl.when(t == s * LAG)
            def _(s=s):
                net_cs.advance(0, 'D', view_cs, s)

        @pl.when((t > 1) & (t <= N_PART + 1))
        def _():
            head_grad(t - 2)

        ahead = t - PROJECT + 1

        @pl.when(ahead == 0)
        def _():
            take_positions()
            angles(0)

        @pl.when((ahead >= 0) & (odd(ahead) == 0) & (ahead < PAIR * N_CHUNK))
        def _():
            chunk_rows(half_of(ahead)).start()

        @pl.when((ahead > 0) & (odd(ahead) == 1) & (ahead < PAIR * N_CHUNK))
        def _():
            project(half_of(ahead))

            @pl.when(half_of(ahead) + 1 < N_CHUNK)
            def _():
                angles(half_of(ahead) + 1)

        @pl.when(t == ATTEND)
        def _():
            own_do.wait()
            take_do()
            operand(zero()).start()
            dk_acc[ALL] = jnp.zeros_like(dk_acc)
            dv_acc[ALL] = jnp.zeros_like(dv_acc)

        @pl.when((t >= ATTEND) & (t < ATTENDED))
        def _():
            attn.step(since)

            @pl.when(lax.rem(since, 4) == 3)
            def _():
                start_all(step_pieces(since))

        complete = jnp.minimum(lax.div(jnp.maximum(t - START - (N_STAGE - 1) * LAG + 1, 0), UPP), IN_GATHER)
        load = (loaded < complete) & (loaded <= lax.div(n, N_TILE) + 1)

        @pl.when(load)
        def _():
            start_all(piece(loaded))

        @pl.when(t == QUERY_IN)
        def _():
            for step in range(1, 8):
                do_copy(step, True).wait_send()

        for turn, (tick, n_steps) in enumerate(((QUERY_IN, N_PART), (OWN_IN, N_PART // 2))):
            @pl.when(t == tick)
            def _(turn=turn):
                start_own(turn)
                start_all(weight_rows(turn, zero()))

            @pl.when(t == tick + 1)
            def _(turn=turn):
                wait_own(turn)

            @pl.when((t > tick) & (t <= tick + n_steps))
            def _(turn=turn, tick=tick, n_steps=n_steps):
                norm_grad(turn, t - tick - 1, n_steps)

        @pl.when(t == OWN_IN + N_PART // 2 + 1)
        def _():
            gain_column()
            input_grad()
            start_own(3)
            start_all(out_rows(jnp.int32(QUAD)))

        @pl.when(t == FIRST_O)
        def _():
            start_own(2)

        @pl.when(t == QUERIES_DONE)
        def _():
            wait_own(2)
            start_all(out_rows(zero()))

        @pl.when(t == OUT_IN)
        def _():
            wait_own(3)
            gain_rest()

        early = (t > QUERIES_DONE) & (t <= QUERIES_DONE + QUAD)

        @pl.when(early | ((t >= OUT_IN) & (t < OUT_IN + QUAD)))
        def _():
            out_part(jnp.where(early, t - QUERIES_DONE - 1, t - OUT_IN + QUAD))

        n_end = jnp.minimum(jnp.minimum(n + 1, loaded * N_TILE), n_own)
        lax.fori_loop(n, n_end, tile, 0)
        return n_end, loaded + load.astype(jnp.int32)

    n, _ = loop(LAST + 1, body, (zero(), zero()))
    start_own(4)
    for j in range(n_cols):
        sum_ref[:, j * BLK:(j + 1) * BLK] = s_buf[j, :LANES, :]
    lax.fori_loop(n, n_own, tile, 0)
    shared(parts, 8, 1).wait_recv()
    dgain_ref[ALL] = jnp.sum(parts[ALL], axis=0)
    for slot in range(TRIO):
        keep_tile(0, slot).wait()
        give_tile(0, slot).wait_send()

    def received(n, carry):
        give_tile(n, 0).wait_recv()
        return carry

    loop(n_own, received, 0)
    wait_own(4)
    for copy in key_copies(pl.ds(0, QROWS)):
        copy.wait_send()
    shared(z_parts, QUAD, 0).wait_send()
    shared(parts, 8, 1).wait_send()


def main(x, dy, gain, pos, freq, w_q, w_k, w_v, w_o):
    model = x.shape[1]
    qkv = w_q.shape[1] + w_k.shape[1] + w_v.shape[1]
    gains = pltpu.VMEM((PAIR * N_PART, LANES), F32)
    queries, keys = pltpu.VMEM((TRIO, QROWS, LANES), BF16), pltpu.VMEM((SEQ, LANES), BF16)
    return pl.pallas_call(
        main_kernel,
        out_shape=[like((PAIR, *GRID) + x.shape, BF16), like((*GRID, 8, LANES), F32),
                   like((N_PIECE, PAIR, QUAD, PAIR, PAIR, QROWS, LANES), BF16), like((N_GATHER, BLK, BLK), F32),
                   like((LANES, model // 3), BF16), like(x.shape, F32), like(x.shape, BF16), like((PAIR * N_PART, LANES), F32)],
        in_specs=[vmem_spec()] * 5 + [any_spec()] * 4,
        out_specs=[any_spec()] * 4 + [vmem_spec()] * 4,
        scratch_shapes=[
            pltpu.VMEM(x.shape, BF16), queries, queries, keys, keys,
            pltpu.VMEM((*GRID, CHUNK, model), BF16), pltpu.VMEM((8, LANES), F32), pltpu.VMEM((1, model), F32), pltpu.VMEM((1, LANES), F32),
            pltpu.VMEM((*GRID, 8, LANES), F32), pltpu.VMEM((PAIR, LANES, LANES), F32), pltpu.VMEM((N_DEV * CHUNK, LANES), F32),
            pltpu.VMEM((QROWS, LANES), F32), pltpu.VMEM((8, LANES, TRIO * LANES), BF16),
            pltpu.VMEM((PAIR, 3, QROWS, LANES), BF16), pltpu.VMEM((LANES, SEQ), F32), pltpu.VMEM((LANES, SEQ), F32),
            pltpu.VMEM((SEQ // BLK, BLK, BLK), F32), pltpu.VMEM((TRIO, BLK, LANES), F32),
            pltpu.VMEM((QUAD, PAIR, QROWS, LANES), BF16), pltpu.VMEM((TRIO, 2, QROWS, LANES), BF16),
            pltpu.VMEM((PAIR, SEQ, BLK), BF16), pltpu.VMEM((PAIR, *GRID, LANES, BLK), BF16), pltpu.VMEM((TRIO, BLK, BLK), F32),
            pltpu.VMEM((LANES, qkv), BF16), pltpu.VMEM((LANES, PAIR * w_k.shape[1]), BF16), pltpu.VMEM((PAIR, HALF, qkv), BF16), pltpu.VMEM(x.shape, F32),
            gains, pltpu.VMEM((QUAD, PAIR * N_PART, LANES), F32), gains, pltpu.VMEM((8, PAIR * N_PART, LANES), F32),
            sems(1, N_STAGE), sems(1, N_STAGE), sems(RING, N_STAGE), sems(RING, N_STAGE),
            sems(TRIO), sems(TRIO), sems(), sems(8), sems(8),
            sems(N_PIECE, 2), sems(PAIR), sems(PAIR), sems(TRIO), sems(TRIO),
            sems(IN_GATHER * N_TILE), sems(TRIO), sems(TRIO), sems(5), sems(PAIR, 4), sems(PAIR), sems(PAIR)],
        compiler_params=pltpu.CompilerParams(collective_id=0, has_side_effects=True, vmem_limit_bytes=VMEM_LIMIT),
    )(x, dy, gain, pos, freq, w_q, w_k, w_v, w_o)


N_LATE = N_PIECE - IN_GATHER
GROUP = IN_GATHER // N_LATE


def finish_kernel(sum_ref, o_ref, dx_ref, dgain_ref, w_ref, hd_ref, g_ref, t_ref,
                  y_ref, dx_out, dgain_out, wq_ref, wk_ref, wv_ref, wo_ref,
                  gbuf, abuf, obuf, cbuf, acc, wbuf, gsem, asem, osem, isem, csem, wsem):
    n_step, group = N_LATE * PER_PIECE, GROUP

    def operand(t):
        return operand_copy(hd_ref, abuf, asem, 1, t, odd(t))

    def cut(t):
        return pl.ds(pl.multiple_of(t * BLK, BLK), BLK)

    def lanes(i):
        return pl.ds(pl.multiple_of(i * LANES, LANES), LANES)

    def to_output(p, t, sub, src, sem):
        j = jnp.where(p == O_PIECES[0], 0, p - O_PIECES[0] - 2)
        return [pltpu.make_async_copy(
            src.at[pl.ds(i * LANES, LANES), :], wo_ref.at[lanes(TRIO * (sub * 4 + i) + j), cut(t)], sem.at[i])
            for i in range(QUAD)]

    def to_input(dst, place, t, sub, src, sem):
        return [pltpu.make_async_copy(
            src.at[:, pl.ds(i * LANES, LANES)], dst.at[cut(t), lanes(place(sub * 4 + i))], sem.at[i]) for i in range(QUAD)]

    def ins(n):
        return [pltpu.make_async_copy(t_ref.at[n * group + i], cbuf.at[lax.rem(n, TRIO), i], isem.at[lax.rem(n, TRIO), i])
                for i in range(group)]

    def start_outs(n):
        for i in range(group):
            m = n * group + i
            p, t, sub = lax.div(m, PER_PIECE), lax.rem(half_of(m), N_TILE), odd(m)
            src, sem = cbuf.at[lax.rem(n, TRIO), i], csem.at[lax.rem(n, TRIO), i]
            for cond, copies in (
                (p < 3, lambda: to_input(wq_ref, lambda g: TRIO * g + p, t, sub, src, sem)),
                (p == KEY_PIECE, lambda: to_input(wk_ref, lambda g: g, t, sub, src, sem)),
                (p == KEY_PIECE + 1, lambda: to_input(wv_ref, lambda g: g, t, sub, src, sem)),
                ((p == O_PIECES[0]) | (p == O_PIECES[1]), lambda: to_output(p, t, sub, src, sem)),
            ):
                @pl.when(cond)
                def _(copies=copies):
                    for c in copies():
                        c.start()

    def wait_outs(n):
        for i in range(group):
            for c in to_output(IN_GATHER, 0, 0, cbuf.at[0, i], csem.at[lax.rem(n, TRIO), i]):
                c.wait()

    def weight(i):
        slot = odd(i)
        return pltpu.make_async_copy(w_ref.at[lanes(TRIO * i + 2), :], wbuf.at[slot], wsem.at[slot])

    for late in range(N_LATE):
        for sub in range(PAIR):
            start_all(piece_copies(g_ref, gbuf, gsem, IN_GATHER + late, sub, late * 2 + sub))
    operand(zero()).start()
    weight(zero()).start()
    acc[ALL] = sum_ref[ALL]
    dx_out[ALL] = dx_ref[ALL]
    dgain_out[ALL] = dgain_ref[ALL]

    def step(n, carry):
        t, late, sub = lax.div(n, PAIR * N_LATE), lax.rem(half_of(n), N_LATE), odd(n)
        p, held = IN_GATHER + late, late * 2 + sub
        slot = lax.rem(n, TRIO)

        @pl.when(n >= 3)
        def _():
            wait_outs(n - 3)
        for c in ins(n):
            c.start()

        @pl.when(n >= 1)
        def _():
            for c in ins(n - 1):
                c.wait()
            start_outs(n - 1)

        @pl.when(held == 0)
        def _():
            operand(t).wait()

            @pl.when(nxt(t) < N_TILE)
            def _():
                operand(nxt(t)).start()

        @pl.when(n < PAIR * N_LATE)
        def _():
            wait_piece(gbuf, gsem, held)

        @pl.when(n >= 3)
        def _():
            for c in to_output(IN_GATHER, 0, 0, obuf.at[0], osem.at[slot]):
                c.wait()
        @pl.when(n < 8)
        def _():
            weight(n).wait()

            @pl.when(n < 7)
            def _():
                weight(n + 1).start()
            acc[ALL] += jnp.dot(o_ref[:, lanes(n)], wbuf[odd(n)], preferred_element_type=F32)
        obuf[slot] = tile_product(abuf[odd(t)], gbuf[held], True)
        for c in to_output(p, t, sub, obuf.at[slot], osem.at[slot]):
            c.start()
        return carry

    loop(n_step, step, 0)
    y_ref[ALL] = acc[ALL].astype(BF16)
    for c in ins(n_step - 1):
        c.wait()
    start_outs(jnp.int32(n_step - 1))
    for n in range(n_step - 3, n_step):
        wait_outs(n)
        for c in to_output(IN_GATHER, 0, 0, obuf.at[0], osem.at[n % 3]):
            c.wait()


def finish(x, o, dx, dgain, w_o, hd, g, tiles):
    model, kv = hd.shape[2], 8 * LANES
    return pl.pallas_call(
        finish_kernel,
        out_shape=[like(x.shape, BF16), like(dx.shape, BF16), like(dgain.shape, F32)]
        + [like((model, n), F32) for n in (TRIO * kv, kv, kv)] + [like((TRIO * kv, model), F32)],
        in_specs=[vmem_spec()] * 4 + [any_spec()] * 4,
        out_specs=[vmem_spec()] * 3 + [any_spec()] * 4,
        scratch_shapes=[pltpu.VMEM((PAIR * N_LATE, SEQ, BLK), BF16), pltpu.VMEM((PAIR, SEQ, BLK), BF16), pltpu.VMEM((TRIO, BLK, BLK), F32),
                        pltpu.VMEM((TRIO, GROUP, BLK, BLK), F32), pltpu.VMEM(x.shape, F32), pltpu.VMEM((PAIR, LANES, model), BF16),
                        sems(PAIR * N_LATE), sems(PAIR), sems(TRIO, 4), sems(TRIO, GROUP), sems(TRIO, GROUP, 4), sems(PAIR)],
        cost_estimate=pl.CostEstimate(flops=4 * SEQ * kv * model, bytes_accessed=250 * 2**20, transcendentals=0),
        compiler_params=pltpu.CompilerParams(vmem_limit_bytes=VMEM_LIMIT),
    )(x, o, dx, dgain, w_o, hd, g, tiles)


def solution(mesh):
    assert mesh.shape['hp'] == 4 and mesh.shape['cp'] == 8

    def device_step(hidden, grad_out, positions, norm_gain, w_q, w_k, w_v, w_o, inv_freq):
        model = hidden.shape[1]
        hd, _, gathered, tiles, o_own, total, dx, gains = main(
            hidden, grad_out, norm_gain, positions, inv_freq, w_q, w_k, w_v, w_o)
        output, grad_hidden, grad_gain, grad_wq, grad_wk, grad_wv, grad_wo = finish(
            total, o_own, dx, gains, w_o, hd.reshape(2, SEQ, model), gathered, tiles)
        grad_gain = grad_gain.reshape(-1)
        return output, grad_hidden, grad_wq, grad_wk, grad_wv, grad_wo, grad_gain

    rows, whole = P(('cp', 'hp'), None), P()
    return jax.shard_map(
        device_step, mesh=mesh,
        in_specs=(rows, rows, P(('cp', 'hp')), whole, whole, whole, whole, whole, whole),
        out_specs=(rows, rows, whole, whole, whole, whole, whole), check_vma=False)
```

```python
import functools
import jax
import jax.numpy as jnp
from jax import lax
from jax.experimental import pallas as pl
from jax.experimental.pallas import tpu as pltpu
from jax.sharding import PartitionSpec as P

NORM_EPS = 1e-5
ALL = Ellipsis
EVERY = slice(None)
PAIR, TRIO, QUAD = 2, 3, 4
GRID = (PAIR, PAIR, PAIR, QUAD)
BY_COLUMN = {'axis': 0, 'keepdims': True}
BY_ROW = {'axis': 1, 'keepdims': True}
F32 = jnp.float32
BF16 = jnp.bfloat16
LANES = 128
BLK = 512
HALF = BLK // 2
SEQ = 8 * BLK
QROWS = PAIR * BLK
UPP = 8
LAG = 2
RING = 20
VMEM_LIMIT = 64 * 2**20 - 2**16
NT = (((1,), (1,)), ((), ()))
TN = (((0,), (0,)), ((), ()))

STAGES = {
    'C': ('z1', 'z2', 'z3', 'y', 'x', 'd'),
    'D': ('z1', 'z2', 'z3', 'x', 'y', 'd'),
    'E': ('x', 'y', 'z1', 'z2', 'z3', 'd'),
    'F': ('y', 'x', 'z1', 'z2', 'z3', 'd'),
}
N_STAGE = 6


def odd(i):
    return lax.rem(i, PAIR)


def half_of(i):
    return lax.div(i, PAIR)


def nxt(i):
    return i + 1


def zero():
    return jnp.int32(0)


def loop(n, body, init):
    return lax.fori_loop(0, n, body, init)


class Gather:
    def __init__(self, send_sem, recv_sem, mix, base=0, source=lambda u: ()):
        self.mix, self.base, self.source, self.unit = mix, base, source, 0
        self.z = lax.axis_index('hp')
        cp = lax.axis_index('cp')
        self.c, self.x, self.y = odd(cp), odd(half_of(cp)), lax.div(cp, 4)
        self.send_sem, self.recv_sem = send_sem, recv_sem

    def device(self, **moved):
        at = {name: moved.get(name, getattr(self, name)) for name in 'cxyz'}
        return at['z'], (at['y'] * PAIR + at['x']) * PAIR + at['c']

    def copies(self, sem_row, kind, view, stage):
        c, x, y, z = self.c, self.x, self.y, self.z
        order = STAGES[kind]
        done = {st[0] for st in order[:order.index(stage)]}
        every = EVERY
        gx, gy, gz = (every if d in done else v for d, v in (('x', x), ('y', y), ('z', z)))
        slot = order.index(stage)

        def copy(place, device, src=()):
            return lambda: pltpu.make_async_remote_copy(
                place if isinstance(src, tuple) else src, place, self.send_sem.at[sem_row, slot], self.recv_sem.at[sem_row, slot],
                device_id=device, device_id_type=pl.DeviceIdType.MESH)

        first = self.source(self.unit) if slot == 0 else ()

        if stage in 'xyd':
            mine, other, dev = {
                'x': lambda: ((c, x, gy, gz), (c, 1 - x, gy, gz), self.device(x=1 - x)),
                'y': lambda: ((c, gx, y, gz), (c, gx, 1 - y, gz), self.device(y=1 - y)),
                'd': lambda: ((c, EVERY, EVERY, EVERY), (1 - c, EVERY, EVERY, EVERY), self.device(c=1 - c)),
            }[stage]()
            out, back = [(True, copy(view(*mine), dev))], [(True, copy(view(*other), dev))]
            start = [(use, copy(view(*mine), dev, src)) for use, src in first] or out
            return {'start': start, 'sent': out, 'recv': back}
        hop = int(stage[1])
        ups, downs = (z >= hop - 1) & (z < 3), (z + hop <= 4) & (z > 0)
        above, below = self.device(z=jnp.minimum(z + 1, 3)), self.device(z=jnp.maximum(z - 1, 0))

        def counted(one, other):
            return [(one != other, copy(view(c, gx, gy, 0), above)), (one & other, copy(view(c, gx, gy, pl.ds(0, PAIR)), above))]

        return {
            'start': [(go & use, copy(view(c, gx, gy, z), to, src)) for go, to in ((ups, above), (downs, below)) for use, src in first]
            or [(ups, copy(view(c, gx, gy, jnp.maximum(z - hop + 1, 0)), above)),
                (downs, copy(view(c, gx, gy, jnp.minimum(z + hop - 1, 3)), below))],
            'sent': counted(ups, downs),
            'recv': counted(z >= hop, z + hop <= 3),
        }

    def run(self, sem_row, kind, view, stage, what):
        for cond, copy in self.copies(sem_row, kind, view, stage)[what]:
            def act(copy=copy):
                if what == 'start':
                    copy().start()
                elif what == 'sent':
                    copy().wait_send()
                else:
                    copy().wait_recv()

            if cond is True:
                act()
            else:
                pl.when(cond)(act)

    def advance(self, sem_row, kind, view, s):
        if 0 < s <= N_STAGE:
            self.run(sem_row, kind, view, STAGES[kind][s - 1], 'recv')
        if s < N_STAGE:
            self.run(sem_row, kind, view, STAGES[kind][s], 'start')
        if s > N_STAGE:
            for stage in STAGES[kind]:
                self.run(sem_row, kind, view, stage, 'sent')

    def kinds(self, u):
        word, at = lax.div(u, 16), lax.rem(u, 16)
        code = jnp.int32(self.mix[0])
        for i in range(1, len(self.mix)):
            code = jnp.where(word == i, self.mix[i], code)
        code = lax.shift_right_logical(code, at * 2) & 3
        return tuple((kind, code == i) for i, kind in enumerate('CDEF'))

    def tick(self, t, n_units, view):
        for s in range(N_STAGE + 2):
            u = t - s * LAG

            @pl.when((u >= 0) & (u < n_units))
            def _(u=u, s=s):
                for kind, is_kind in self.kinds(u):
                    @pl.when(is_kind)
                    def _(kind=kind):
                        self.unit = u
                        self.advance(lax.rem(u + self.base, RING), kind, view(u), s)


def turn(v):
    return pltpu.roll(v, LANES // 2, 1)


def low_lanes(shape):
    return lax.broadcasted_iota(jnp.int32, shape, 1) < LANES // 2


def cos_sin(cs):
    low = low_lanes(cs.shape)
    other = turn(cs)
    return jnp.where(low, cs, other), jnp.where(low, -other, cs)


def any_spec():
    return pl.BlockSpec(memory_space=pl.ANY)


def vmem_spec():
    return pl.BlockSpec(memory_space=pltpu.VMEM)


def sems(*shape):
    return pltpu.SemaphoreType.DMA(shape) if shape else pltpu.SemaphoreType.DMA


def like(shape, dtype):
    return jax.ShapeDtypeStruct(shape, dtype)


def start_all(copies):
    for copy in copies:
        copy.start()


def wait_all(copies):
    for copy in copies:
        copy.wait()


N_PIECE = 8
O_PIECES = (3, 6, 7)
KEY_PIECE = 4
N_TILE = 6
PER_PIECE = PAIR * N_TILE
IN_GATHER = 7
N_GATHER = IN_GATHER * PER_PIECE


def tile_product(operand, piece, of_output):
    left, right = (piece, operand) if of_output else (operand, piece)
    return lax.dot_general(left, right, TN, preferred_element_type=F32)


def operand_copy(hd_ref, abuf, asem, which, t, slot):
    return pltpu.make_async_copy(
        hd_ref.at[which, :, pl.ds(pl.multiple_of(t * BLK, BLK), BLK)], abuf.at[slot], asem.at[slot])


def piece_copies(g_ref, gbuf, gsem, p, core, slot):
    return [pltpu.make_async_copy(g_ref.at[p, core, z, r // 2, r % 2],
                                  gbuf.at[slot, pl.ds(r * QROWS, QROWS), pl.ds(z * LANES, LANES)], gsem.at[slot])
            for z in range(QUAD) for r in range(QUAD)]


def wait_piece(gbuf, gsem, slot):
    pltpu.make_async_copy(gbuf.at[slot], gbuf.at[slot], gsem.at[slot]).wait()


def lane_groups(op, s):
    out = s[:, :LANES]
    for i in range(1, s.shape[1] // LANES):
        out = op(out, s[:, i * LANES:(i + 1) * LANES])
    return out


class Attention:
    def __init__(self, q, do, k, v, cs, out, dk_acc, dv_acc, s, state, quarter):
        self.q, self.do, self.k, self.v, self.cs, self.out = q, do, k, v, cs, out
        self.dk, self.dv, self.s, self.state = dk_acc, dv_acc, s, state
        self.quarter = quarter
        self.scale = LANES ** -0.5
        self.factor = self.scale * 1.4426950408889634

    def step(self, t):
        head, half = lax.div(t, 8), odd(lax.div(t, 4))
        n_key = jnp.where(half == 0, self.quarter + 1, SEQ // BLK - self.quarter)
        rows = pl.ds(pl.multiple_of(half * BLK, BLK), BLK)
        for i, act in enumerate((self.scores, self.exps, self.values, self.grads)):
            @pl.when(lax.rem(t, 4) == i)
            def _(act=act):
                act(head, half, n_key, rows)

    def keys(self, kb):
        return pl.ds(pl.multiple_of(kb * BLK, BLK), BLK)

    def zeros(self):
        return jnp.zeros((BLK, LANES), F32)

    def keep(self, i, column):
        self.state[i] = jnp.broadcast_to(column, (BLK, LANES))

    def kept(self, i):
        return self.state[i, :, :1]

    def scores(self, head, half, n_key, rows):
        q = self.q[head, rows, :]

        def block(kb, m, diagonal=False):
            s = lax.dot_general(q, self.k[self.keys(kb), :], NT, preferred_element_type=F32)
            if diagonal:
                visible = lax.broadcasted_iota(jnp.int32, s.shape, 0) >= lax.broadcasted_iota(jnp.int32, s.shape, 1)
                s = jnp.where(visible, s, -1e30)
            self.s[kb] = s
            return jnp.maximum(m, lane_groups(jnp.maximum, s))

        m = loop(n_key - 1, block, self.zeros() - 1e30)
        m = block(n_key - 1, m, diagonal=True)
        self.keep(0, jnp.max(m, **BY_ROW) * self.factor)

    def exps(self, head, half, n_key, rows):
        m = self.kept(0)

        def block(kb, total):
            e = jnp.exp2(self.s[kb] * self.factor - m)
            self.s[kb] = e
            return total + lane_groups(jnp.add, e)

        total = loop(n_key, block, self.zeros())
        self.keep(0, 1.0 / jnp.sum(total, **BY_ROW))

    def sides(self, half):
        for side in range(PAIR):
            place = (half * (1 - side) + (1 - half) * side) * HALF
            yield pl.ds(pl.multiple_of(place, HALF), HALF), pl.ds(pl.multiple_of(side * BLK + half * HALF, HALF), HALF)

    def values(self, head, half, n_key, rows):
        do, inv = self.do[head, rows, :], self.kept(0)
        turned = do.T

        def block(kb, o):
            p = (self.s[kb] * inv).astype(BF16)
            self.dv[:, self.keys(kb)] += jnp.dot(turned, p, preferred_element_type=F32)
            return o + jnp.dot(p, self.v[self.keys(kb), :], preferred_element_type=F32)

        o = loop(n_key, block, self.zeros()).astype(BF16).astype(F32)
        self.keep(1, jnp.sum(do.astype(F32) * o, **BY_ROW))
        self.state[2] = o
        for place, stored in self.sides(half):
            self.out[1, head, stored, :] = self.state[2, place, :].astype(BF16)

    def grads(self, head, half, n_key, rows):
        do, inv, delta = self.do[head, rows, :], self.kept(0), self.kept(1)
        turned = self.q[head, rows, :].T

        def block(kb, dq):
            dp = lax.dot_general(do, self.v[self.keys(kb), :], NT, preferred_element_type=F32)
            ds = (self.s[kb] * inv * (dp - delta)).astype(BF16)
            self.dk[:, self.keys(kb)] += jnp.dot(turned, ds, preferred_element_type=F32)
            return dq + jnp.dot(ds, self.k[self.keys(kb), :], preferred_element_type=F32)

        dq = loop(n_key, block, self.zeros()) * self.scale
        self.state[2] = dq.astype(BF16).astype(F32)
        for place, stored in self.sides(half):
            cos, sin = cos_sin(self.cs[stored, :])
            part = self.state[2, place, :]
            self.out[0, head, stored, :] = (part * cos - turn(part) * sin).astype(BF16)

    def key_grads(self, out):
        for pair in range(8):
            for i, (acc, factor) in enumerate(((self.dk, self.scale), (self.dv, 1.0))):
                for part, block in enumerate((pair, 15 - pair)):
                    out[pair // 2, i, pl.ds(pair % PAIR * BLK + part * HALF, HALF), :] = (
                        acc[:, pl.ds(block * HALF, HALF)].T * factor).astype(BF16)


ROWS_UNIT = 8
N_IN = LANES // ROWS_UNIT
N_STEP = 24
N_UNIT = N_PIECE * UPP
N_PART = 12
SEND_DO = N_PART + 1
DELAY = N_STAGE * LAG
CHUNK = PAIR * ROWS_UNIT
N_CHUNK = LANES // CHUNK
PROJECT = DELAY + 2
ATTEND = PROJECT + PAIR * N_CHUNK - 1
ATTENDED = ATTEND + N_STEP
START = ATTEND + 4
N_SEND = 8
KEYS_IN = START + KEY_PIECE * UPP
QUERY_IN = START + 3 * UPP + DELAY
OWN_IN = START + O_PIECES[1] * UPP + DELAY
QUERIES_DONE = QUERY_IN + N_PART
FIRST_O = START + (O_PIECES[0] + 1) * UPP + DELAY
OUT_IN = OWN_IN + N_PART // 2 + 2
LAST = START + N_UNIT + DELAY + LAG
N_DEV = 32


def main_kernel(x_ref, dy_ref, gain_ref, mypos_ref, freq_ref, wq_ref, wk_ref, wv_ref, wo_ref,
                hd_ref, pos_ref, g_ref, t_ref, o_ref, sum_ref, dx_ref, dgain_ref,
                h_buf, q_buf, do_buf, k_buf, v_buf, rows_buf, mypos_buf, gain_buf, freq_buf, pos_buf, pos_t, cs_buf, own_cs, do_parts,
                piece_buf, dk_acc, dv_acc, s_buf, state, dkv_buf, peer_buf, gbuf, abuf, obuf, own_buf, oo_buf, w_buf, dn_buf, part_buf, z_parts, sum_buf, parts,
                cs_send, cs_recv, send_sem, recv_sem, first_sem, proj_sem, rows_sem, do_send, do_recv,
                lsem, gsem, asem, osem, tsend, trecv, psend, precv, rsem, wsem, gain_send, gain_recv):
    def made(u):
        rows = pl.ds(pl.multiple_of(lax.rem(u, N_IN) * ROWS_UNIT, ROWS_UNIT), ROWS_UNIT)
        return [(u < N_IN, h_buf.at[rows, :]), (u >= N_IN, dy_ref.at[rows, :])]

    net_in, net_cs, net = Gather(send_sem, recv_sem, (306463953, 1175604295), source=made), Gather(cs_send, cs_recv, (306463953, 1175604295)), Gather(send_sem, recv_sem, (-398134202, 1293043604, -2075179916, 958350436), START)
    quarter = net.y * 2 + net.x
    head = net.c * 4 + net.z
    spot = (net.y, net.x, net.c, net.z)
    attn = Attention(q_buf, do_buf, k_buf, v_buf, own_cs, piece_buf, dk_acc, dv_acc, s_buf, state, quarter)

    def inv_rms():
        x = x_ref[ALL].astype(F32)
        return lax.rsqrt(jnp.mean(x * x, **BY_ROW) + NORM_EPS)

    barrier = pltpu.get_barrier_semaphore()

    def greet(**moved):
        pl.semaphore_signal(barrier, inc=1, device_id=net.device(**moved), device_id_type=pl.DeviceIdType.MESH)

    greet(x=1 - net.x)
    greet(y=1 - net.y)
    greet(c=1 - net.c)
    inner = (net.z > 0).astype(jnp.int32) + (net.z < 3).astype(jnp.int32)

    @pl.when(net.z > 0)
    def _():
        greet(z=net.z - 1)

    @pl.when(net.z < 3)
    def _():
        greet(z=net.z + 1)

    gain_buf[ALL] = gain_ref[ALL].astype(F32).reshape(gain_buf.shape)
    freq_buf[ALL] = jnp.concatenate([freq_ref[ALL], freq_ref[ALL]], axis=0).reshape(freq_buf.shape)
    mypos_buf[ALL] = jnp.broadcast_to(mypos_ref[ALL].astype(F32).reshape(1, LANES), mypos_buf.shape)
    h_buf[ALL] = (x_ref[ALL].astype(F32) * inv_rms() * gain_buf[ALL]).astype(BF16)
    first = [pltpu.make_async_copy(src, dst, first_sem.at[i]) for i, (src, dst) in enumerate((
        (h_buf, hd_ref.at[(0, *spot)]), (dy_ref, hd_ref.at[(1, *spot)]), (mypos_buf, pos_ref.at[spot])))]
    start_all(first)
    pl.semaphore_wait(barrier, TRIO + inner)
    q_cols = pl.ds(pl.multiple_of(head * TRIO * LANES, LANES), TRIO * LANES)
    kv_cols = pl.ds(pl.multiple_of(head * LANES, LANES), LANES)
    w_rows = slice(0, wq_ref.shape[0])
    wq_buf, wkv_buf = gbuf.at[0, w_rows, :TRIO * LANES], gbuf.at[1, w_rows, :PAIR * LANES]
    weights = [pltpu.make_async_copy(src, dst, proj_sem.at[i]) for i, (src, dst) in enumerate((
        (wq_ref.at[:, q_cols], wq_buf), (wk_ref.at[:, kv_cols], gbuf.at[1, w_rows, :LANES]),
        (wv_ref.at[:, kv_cols], gbuf.at[1, w_rows, LANES:PAIR * LANES])))]

    def view_in(u):
        rows = pl.ds(pl.multiple_of(lax.rem(u, N_IN) * ROWS_UNIT, ROWS_UNIT), ROWS_UNIT)
        which = lax.div(u, N_IN)
        return lambda c, x, y, z: hd_ref.at[which, y, x, c, z, rows, :]

    def view_cs(c, x, y, z):
        return pos_ref.at[y, x, c, z]

    def part(i, width=HALF):
        return pl.ds(pl.multiple_of(i * width, width), width)

    def wo_rows(i):
        slot = odd(i)
        return pltpu.make_async_copy(wo_ref.at[part(i), :], w_buf.at[slot, :, :wo_ref.shape[1]], wsem.at[slot, 0])

    def head_grad(i):
        slot = odd(i)
        wo_rows(i).wait()

        @pl.when(nxt(i) < N_PART)
        def _():
            wo_rows(nxt(i)).start()
        own_buf[:, part(i)] = lax.dot_general(
            dy_ref[ALL], w_buf[slot, :, :wo_ref.shape[1]], NT, preferred_element_type=F32).astype(BF16)

    def do_copy(step, mine):
        me = net.c * 4 + net.z
        other = lax.rem(me + step, 8)
        slot = me if mine else lax.rem(me + 8 - step, 8)
        return pltpu.make_async_remote_copy(
            own_buf.at[:, part(other, TRIO * LANES)], do_parts.at[slot], do_send.at[step], do_recv.at[step],
            device_id=net.device(c=lax.div(other, 4), z=lax.rem(other, 4)), device_id_type=pl.DeviceIdType.MESH)

    own_do = pltpu.make_async_copy(own_buf.at[:, part(head, TRIO * LANES)], do_parts.at[head], do_send.at[0])

    def query_row(c, z):
        return c * HALF + z * LANES if z < 2 else BLK + (1 - c) * HALF + (z - 2) * LANES

    def take_do():
        for step in range(1, 8):
            do_copy(step, False).wait_recv()
        for c in range(PAIR):
            for z in range(QUAD):
                for j in range(TRIO):
                    do_buf[j, pl.ds(query_row(c, z), LANES), :] = do_parts[c * 4 + z, :, j * LANES:(j + 1) * LANES]

    every = EVERY

    def chunk(k, base=0):
        return pl.ds(pl.multiple_of(base + k * CHUNK, CHUNK), CHUNK)

    def chunk_rows(k):
        return pltpu.make_async_copy(hd_ref.at[0, every, every, every, every, chunk(k), every], rows_buf, rows_sem)

    def take_positions():
        copy = pltpu.make_async_copy(pos_ref, pos_buf, rows_sem)
        copy.start()
        copy.wait()
        for i in range(PAIR):
            pos_t[i] = pos_buf[i].reshape(LANES, LANES).T

    def angles(k):
        for dev in range(N_DEV):
            column = pos_t[dev // 16, chunk(k), dev % 16 * 8:dev % 16 * 8 + 1]
            cs_buf[dev * CHUNK:(dev + 1) * CHUNK, :] = jnp.broadcast_to(column, (CHUNK, LANES)) * freq_buf[ALL]
        angle = cs_buf[ALL]
        cs_buf[ALL] = jnp.where(low_lanes(angle.shape), jnp.cos(angle), jnp.sin(angle))

    def rotate(v, cs):
        cos, sin = cos_sin(cs)
        return (v * cos + turn(v) * sin).astype(BF16)

    def project(k):
        chunk_rows(k).wait()
        n_rows = N_DEV * CHUNK
        kv = jnp.dot(rows_buf[ALL].reshape(n_rows, -1), wkv_buf[ALL], preferred_element_type=F32)
        key = rotate(kv[:, :LANES], cs_buf[ALL])
        value = kv[:, LANES:].astype(BF16)
        for cp in range(8):
            for z in range(QUAD):
                block = 2 * cp + z if z < 2 else 28 - 2 * cp + z
                rows = slice((cp * 4 + z) * CHUNK, (cp * 4 + z + 1) * CHUNK)
                k_buf[chunk(k, block * LANES), :] = key[rows]
                v_buf[chunk(k, block * LANES), :] = value[rows]
        mine, cs = rows_buf[net.y, net.x].reshape(LANES, -1), cs_buf[part(quarter, LANES), :]
        q = jnp.dot(mine, wq_buf[ALL], preferred_element_type=F32)
        for j in range(TRIO):
            p = rotate(q[:, j * LANES:(j + 1) * LANES], cs)
            for c in range(PAIR):
                for z in range(QUAD):
                    rows = slice((c * 4 + z) * CHUNK, (c * 4 + z + 1) * CHUNK)
                    q_buf[j, chunk(k, query_row(c, z)), :] = p[rows]
                    if j == 0:
                        own_cs[chunk(k, c * BLK + z * LANES), :] = cs[rows]

    def local(p, i, src, rows=pl.ds(0, QROWS)):
        return pltpu.make_async_copy(src, g_ref.at[p, net.c, net.z, net.y, net.x, rows, :], lsem.at[p, i])

    def step_pieces(step):
        head, half = lax.div(step, 8), odd(lax.div(step, 4))
        out_piece = jnp.where(head == 0, O_PIECES[0], O_PIECES[0] + 2 + head)
        return [local(p, side, piece_buf.at[i, head, rows], rows) for i, p in ((0, head), (1, out_piece))
                for side, (_, rows) in enumerate(attn.sides(half))]

    def key_copies(rows):
        for i, moved in enumerate(('x', 'y', 'xy')):
            x, y = (1 - at if name in moved else at for name, at in (('x', net.x), ('y', net.y)))
            yield pltpu.make_async_remote_copy(
                dkv_buf.at[y * 2 + x, :, rows], peer_buf.at[i, :, rows], psend.at[i], precv.at[i],
                device_id=net.device(x=x, y=y), device_id_type=pl.DeviceIdType.MESH)

    def add_peers():
        for copy in key_copies(pl.ds(0, QROWS)):
            copy.wait_recv()
        total = dkv_buf[quarter].astype(F32)
        for i in range(TRIO):
            total = total + peer_buf[i].astype(F32)
        total = total.astype(BF16)
        cos, sin = cos_sin(own_cs[ALL])
        dk = total[0].astype(F32)
        piece_buf[0, 0] = (dk * cos - turn(dk) * sin).astype(BF16)
        piece_buf[0, 1] = total[1]
        kv = [local(KEY_PIECE + i, 0, piece_buf.at[0, i]) for i in range(PAIR)]
        start_all(kv)
        wait_all(kv)

    def view(u):
        p, k = lax.div(u, UPP), lax.rem(u, UPP)
        two = half_of(k)
        rows = part(odd(two) * 4 + half_of(two) * 2 + odd(k), QROWS // UPP)
        return lambda c, x, y, z: g_ref.at[p, c, z, y, x, rows, :]

    def place(n):
        return lax.div(n, N_TILE) * PER_PIECE + lax.rem(n, N_TILE) * 2 + net.c

    def keep_tile(n, slot):
        return pltpu.make_async_copy(obuf.at[slot], t_ref.at[place(n)], osem.at[slot])

    def give_tile(n, slot):
        return pltpu.make_async_remote_copy(
            obuf.at[slot], t_ref.at[place(n)], tsend.at[slot], trecv.at[n],
            device_id=net.device(c=1 - net.c), device_id_type=pl.DeviceIdType.MESH)

    def of_output(p):
        return (p == O_PIECES[0]) | (p == O_PIECES[1])

    def operand(n):
        which, slot = of_output(lax.div(n, N_TILE)).astype(jnp.int32), odd(n)
        return pltpu.make_async_copy(
            hd_ref.at[which, every, every, every, every, every, part(lax.rem(n, N_TILE), BLK)], abuf.at[slot], asem.at[slot])

    def piece(p):
        return piece_copies(g_ref, gbuf, gsem, p, net.c, odd(p))

    n_own = IN_GATHER * N_TILE

    def tile(n, carry):
        slot = lax.rem(n, TRIO)
        p = lax.div(n, N_TILE)

        @pl.when(lax.rem(n, N_TILE) == 0)
        def _():
            wait_piece(gbuf, gsem, odd(p))
        operand(n).wait()

        @pl.when(nxt(n) < n_own)
        def _():
            operand(nxt(n)).start()

        @pl.when(n >= 3)
        def _():
            keep_tile(n, slot).wait()
            give_tile(n, slot).wait_send()
        for output in (False, True):
            @pl.when(of_output(p) == output)
            def _(output=output):
                obuf[slot] = tile_product(abuf[odd(n)].reshape(SEQ, BLK), gbuf[odd(p)], output)
        keep_tile(n, slot).start()
        give_tile(n, slot).start()
        return carry

    kv = wk_ref.shape[1]
    groups = (((0, 1, 2), own_buf, slice(0, TRIO * kv)), ((KEY_PIECE, KEY_PIECE + 1), own_buf, slice(TRIO * kv, 5 * kv)),
              (O_PIECES[:1], oo_buf, slice(0, kv)), (O_PIECES[1:2], oo_buf, slice(kv, PAIR * kv)), (O_PIECES[2:], o_ref, slice(0, kv)))

    def start_own(i):
        rows = pl.ds(pl.multiple_of(net.c * BLK + net.z * LANES, LANES), LANES)
        pieces, dst, cols = groups[i]
        for k, p in enumerate(pieces):
            for g in range(8):
                col = cols.start // LANES + (TRIO * g + k if len(pieces) == 3 else 8 * k + g)
                pltpu.make_async_copy(
                    g_ref.at[p, g // 4, g % 4, net.y, net.x, rows, :], dst.at[:, pl.ds(col * LANES, LANES)], rsem.at[i]).start()

    def wait_own(i):
        _, dst, cols = groups[i]
        pltpu.make_async_copy(dst.at[:, cols], dst.at[:, cols], rsem.at[i]).wait()

    def weight_rows(turn, i):
        slot = odd(i)
        if turn == 0:
            places = ((wq_ref, part(i), 0, TRIO * kv),)
        else:
            places = [(src, part(i * 2 + j), (j * 2 + k) * kv, kv) for j in range(PAIR) for k, src in enumerate((wk_ref, wv_ref))]
        return [pltpu.make_async_copy(src.at[rows, :], w_buf.at[slot, :, pl.ds(at, width)], wsem.at[slot, j])
                for j, (src, rows, at, width) in enumerate(places)]

    def norm_grad(turn, i, n_steps):
        slot = odd(i)
        wait_all(weight_rows(turn, i))

        @pl.when(nxt(i) < n_steps)
        def _():
            start_all(weight_rows(turn, nxt(i)))
        if turn == 0:
            dn_buf[:, part(i)] = lax.dot_general(
                own_buf[:, :TRIO * kv], w_buf[slot, :, :TRIO * kv], NT, preferred_element_type=F32)
            return
        for j in range(PAIR):
            block = i * 2 + j
            dn = dn_buf[:, part(block)] + lax.dot_general(
                own_buf[:, TRIO * kv:], w_buf[slot, :, pl.ds(j * PAIR * kv, PAIR * kv)], NT, preferred_element_type=F32)
            dn_buf[:, part(block)] = dn
            x_hat = x_ref[:, part(block)].astype(F32) * inv_rms()
            total = jnp.sum(dn * x_hat, **BY_COLUMN)
            for k in range(PAIR):
                part_buf[pl.ds(block * 2 + k, 1), :] = total[:, k * LANES:(k + 1) * LANES]

    column = (net.y * PAIR + net.x) * PAIR + net.c

    def share(src, dst, slot, n, sem, device):
        def send(step, carry):
            pltpu.make_async_remote_copy(
                src, dst.at[slot], gain_send.at[sem], gain_recv.at[sem],
                device_id=device(lax.rem(slot + step, n)), device_id_type=pl.DeviceIdType.MESH).start()
            return carry

        mine = pltpu.make_async_copy(src, dst.at[slot], rows_sem)
        mine.start()
        mine.wait()
        lax.fori_loop(1, n, send, 0)

    def shared(dst, n, sem):
        rest = dst.at[pl.ds(1, n - 1)]
        return pltpu.make_async_remote_copy(
            rest, rest, gain_send.at[sem], gain_recv.at[sem],
            device_id=net.device(c=1 - net.c), device_id_type=pl.DeviceIdType.MESH)

    def gain_column():
        share(part_buf, z_parts, net.z, QUAD, 0, lambda z: net.device(z=z))

    def gain_rest():
        shared(z_parts, QUAD, 0).wait_recv()
        sum_buf[ALL] = jnp.sum(z_parts[ALL], axis=0)
        share(sum_buf, parts, column, 8, 1, lambda k: (net.z, k))

    def input_grad():
        x_hat = x_ref[ALL].astype(F32) * inv_rms()
        d_hat = dn_buf[ALL] * gain_buf[ALL]
        dx_ref[ALL] = (dy_ref[ALL].astype(F32) + inv_rms() * (
            d_hat - x_hat * jnp.mean(d_hat * x_hat, **BY_ROW))).astype(BF16)

    n_cols = x_ref.shape[1] // BLK

    def out_rows(i):
        slot = odd(i)
        head = lax.rem(i, 4) * 6 + lax.div(i, 4)
        return [pltpu.make_async_copy(
            wo_ref.at[part(head + TRIO * j, LANES), :], w_buf.at[slot, j * LANES:(j + 1) * LANES, :wo_ref.shape[1]], wsem.at[slot, j])
            for j in range(PAIR)]

    def out_part(i):
        slot = odd(i)
        wait_all(out_rows(i))

        @pl.when(lax.rem(i, QUAD) < 3)
        def _():
            start_all(out_rows(nxt(i)))
        left = oo_buf[:, part(i)]
        for j in range(n_cols):
            cols = slice(j * BLK, (j + 1) * BLK)
            term = jnp.dot(left, w_buf[slot, :, cols], preferred_element_type=F32)
            before = jnp.where(i == 0, x_ref[:, cols].astype(F32), s_buf[j, :LANES, :])
            s_buf[j, :LANES, :] = before + term

    def body(t, carry):
        n, loaded = carry
        since = t - ATTEND

        @pl.when(t == 1)
        def _():
            wait_all(first)
            wo_rows(zero()).start()
            start_all(weights)

        @pl.when(t == SEND_DO + 1)
        def _():
            own_do.start()
            for step in range(1, 8):
                do_copy(step, True).start()
            wait_all(weights)

        @pl.when((since > 0) & (t <= ATTENDED) & (lax.rem(since, 4) == 0))
        def _():
            wait_all(step_pieces(since - 1))

        @pl.when(t == ATTENDED)
        def _():
            attn.key_grads(dkv_buf)

        @pl.when((t >= ATTENDED) & (t < ATTENDED + N_SEND))
        def _():
            start_all(key_copies(part(t - ATTENDED, QROWS // N_SEND)))

        @pl.when(t == KEYS_IN)
        def _():
            add_peers()
        net_in.tick(t, PAIR * N_IN, view_in)
        net.tick(t - START, N_UNIT, view)
        for s in range(N_STAGE + 2):
            @pl.when(t == s * LAG + 1)
            def _(s=s):
                net_cs.advance(0, 'D', view_cs, s)

        @pl.when((t > 1) & (t <= N_PART + 1))
        def _():
            head_grad(t - 2)

        ahead = t - PROJECT + 1

        @pl.when(ahead == 0)
        def _():
            take_positions()
            angles(0)

        @pl.when((ahead >= 0) & (odd(ahead) == 0) & (ahead < PAIR * N_CHUNK))
        def _():
            chunk_rows(half_of(ahead)).start()

        @pl.when((ahead > 0) & (odd(ahead) == 1) & (ahead < PAIR * N_CHUNK))
        def _():
            project(half_of(ahead))

            @pl.when(half_of(ahead) + 1 < N_CHUNK)
            def _():
                angles(half_of(ahead) + 1)

        @pl.when(t == ATTEND)
        def _():
            own_do.wait()
            take_do()
            operand(zero()).start()
            dk_acc[ALL] = jnp.zeros_like(dk_acc)
            dv_acc[ALL] = jnp.zeros_like(dv_acc)

        @pl.when((t >= ATTEND) & (t < ATTENDED))
        def _():
            attn.step(since)

            @pl.when(lax.rem(since, 4) == 3)
            def _():
                start_all(step_pieces(since))

        complete = jnp.minimum(lax.div(jnp.maximum(t - START - (N_STAGE - 1) * LAG + 1, 0), UPP), IN_GATHER)
        load = (loaded < complete) & (loaded <= lax.div(n, N_TILE) + 1)

        @pl.when(load)
        def _():
            start_all(piece(loaded))

        @pl.when(t == QUERY_IN)
        def _():
            for step in range(1, 8):
                do_copy(step, True).wait_send()

        for turn, (tick, n_steps) in enumerate(((QUERY_IN, N_PART), (OWN_IN, N_PART // 2))):
            @pl.when(t == tick)
            def _(turn=turn):
                start_own(turn)
                start_all(weight_rows(turn, zero()))

            @pl.when(t == tick + 1)
            def _(turn=turn):
                wait_own(turn)

            @pl.when((t > tick) & (t <= tick + n_steps))
            def _(turn=turn, tick=tick, n_steps=n_steps):
                norm_grad(turn, t - tick - 1, n_steps)

        @pl.when(t == OWN_IN + N_PART // 2 + 1)
        def _():
            gain_column()
            input_grad()
            start_own(3)
            start_all(out_rows(jnp.int32(QUAD)))

        @pl.when(t == FIRST_O)
        def _():
            start_own(2)

        @pl.when(t == QUERIES_DONE)
        def _():
            wait_own(2)
            start_all(out_rows(zero()))

        @pl.when(t == OUT_IN)
        def _():
            wait_own(3)
            gain_rest()

        early = (t > QUERIES_DONE) & (t <= QUERIES_DONE + QUAD)

        @pl.when(early | ((t >= OUT_IN) & (t < OUT_IN + QUAD)))
        def _():
            out_part(jnp.where(early, t - QUERIES_DONE - 1, t - OUT_IN + QUAD))

        n_end = jnp.minimum(jnp.minimum(n + 1, loaded * N_TILE), n_own)
        lax.fori_loop(n, n_end, tile, 0)
        return n_end, loaded + load.astype(jnp.int32)

    n, _ = loop(LAST + 1, body, (zero(), zero()))
    start_own(4)
    for j in range(n_cols):
        sum_ref[:, j * BLK:(j + 1) * BLK] = s_buf[j, :LANES, :]
    lax.fori_loop(n, n_own, tile, 0)
    shared(parts, 8, 1).wait_recv()
    dgain_ref[ALL] = jnp.sum(parts[ALL], axis=0)
    for slot in range(TRIO):
        keep_tile(0, slot).wait()
        give_tile(0, slot).wait_send()

    def received(n, carry):
        give_tile(n, 0).wait_recv()
        return carry

    loop(n_own, received, 0)
    wait_own(4)
    for copy in key_copies(pl.ds(0, QROWS)):
        copy.wait_send()
    shared(z_parts, QUAD, 0).wait_send()
    shared(parts, 8, 1).wait_send()


def main(x, dy, gain, pos, freq, w_q, w_k, w_v, w_o):
    model = x.shape[1]
    qkv = w_q.shape[1] + w_k.shape[1] + w_v.shape[1]
    gains = pltpu.VMEM((PAIR * N_PART, LANES), F32)
    queries, keys = pltpu.VMEM((TRIO, QROWS, LANES), BF16), pltpu.VMEM((SEQ, LANES), BF16)
    return pl.pallas_call(
        main_kernel,
        out_shape=[like((PAIR, *GRID) + x.shape, BF16), like((*GRID, 8, LANES), F32),
                   like((N_PIECE, PAIR, QUAD, PAIR, PAIR, QROWS, LANES), BF16), like((N_GATHER, BLK, BLK), F32),
                   like((LANES, model // 3), BF16), like(x.shape, F32), like(x.shape, BF16), like((PAIR * N_PART, LANES), F32)],
        in_specs=[vmem_spec()] * 5 + [any_spec()] * 4,
        out_specs=[any_spec()] * 4 + [vmem_spec()] * 4,
        scratch_shapes=[
            pltpu.VMEM(x.shape, BF16), queries, queries, keys, keys,
            pltpu.VMEM((*GRID, CHUNK, model), BF16), pltpu.VMEM((8, LANES), F32), pltpu.VMEM((1, model), F32), pltpu.VMEM((1, LANES), F32),
            pltpu.VMEM((*GRID, 8, LANES), F32), pltpu.VMEM((PAIR, LANES, LANES), F32), pltpu.VMEM((N_DEV * CHUNK, LANES), F32),
            pltpu.VMEM((QROWS, LANES), F32), pltpu.VMEM((8, LANES, TRIO * LANES), BF16),
            pltpu.VMEM((PAIR, 3, QROWS, LANES), BF16), pltpu.VMEM((LANES, SEQ), F32), pltpu.VMEM((LANES, SEQ), F32),
            pltpu.VMEM((SEQ // BLK, BLK, BLK), F32), pltpu.VMEM((TRIO, BLK, LANES), F32),
            pltpu.VMEM((QUAD, PAIR, QROWS, LANES), BF16), pltpu.VMEM((TRIO, 2, QROWS, LANES), BF16),
            pltpu.VMEM((PAIR, SEQ, BLK), BF16), pltpu.VMEM((PAIR, *GRID, LANES, BLK), BF16), pltpu.VMEM((TRIO, BLK, BLK), F32),
            pltpu.VMEM((LANES, qkv), BF16), pltpu.VMEM((LANES, PAIR * w_k.shape[1]), BF16), pltpu.VMEM((PAIR, HALF, qkv), BF16), pltpu.VMEM(x.shape, F32),
            gains, pltpu.VMEM((QUAD, PAIR * N_PART, LANES), F32), gains, pltpu.VMEM((8, PAIR * N_PART, LANES), F32),
            sems(1, N_STAGE), sems(1, N_STAGE), sems(RING, N_STAGE), sems(RING, N_STAGE),
            sems(TRIO), sems(TRIO), sems(), sems(8), sems(8),
            sems(N_PIECE, 2), sems(PAIR), sems(PAIR), sems(TRIO), sems(TRIO),
            sems(IN_GATHER * N_TILE), sems(TRIO), sems(TRIO), sems(5), sems(PAIR, 4), sems(PAIR), sems(PAIR)],
        compiler_params=pltpu.CompilerParams(collective_id=0, has_side_effects=True, vmem_limit_bytes=VMEM_LIMIT),
    )(x, dy, gain, pos, freq, w_q, w_k, w_v, w_o)


N_LATE = N_PIECE - IN_GATHER
GROUP = IN_GATHER // N_LATE


def finish_kernel(sum_ref, o_ref, dx_ref, dgain_ref, w_ref, hd_ref, g_ref, t_ref,
                  y_ref, dx_out, dgain_out, wq_ref, wk_ref, wv_ref, wo_ref,
                  gbuf, abuf, obuf, cbuf, acc, wbuf, gsem, asem, osem, isem, csem, wsem):
    n_step, group = N_LATE * PER_PIECE, GROUP

    def operand(t):
        return operand_copy(hd_ref, abuf, asem, 1, t, odd(t))

    def cut(t):
        return pl.ds(pl.multiple_of(t * BLK, BLK), BLK)

    def lanes(i):
        return pl.ds(pl.multiple_of(i * LANES, LANES), LANES)

    def to_output(p, t, sub, src, sem):
        j = jnp.where(p == O_PIECES[0], 0, p - O_PIECES[0] - 2)
        return [pltpu.make_async_copy(
            src.at[pl.ds(i * LANES, LANES), :], wo_ref.at[lanes(TRIO * (sub * 4 + i) + j), cut(t)], sem.at[i])
            for i in range(QUAD)]

    def to_input(dst, place, t, sub, src, sem):
        return [pltpu.make_async_copy(
            src.at[:, pl.ds(i * LANES, LANES)], dst.at[cut(t), lanes(place(sub * 4 + i))], sem.at[i]) for i in range(QUAD)]

    def ins(n):
        return [pltpu.make_async_copy(t_ref.at[n * group + i], cbuf.at[lax.rem(n, TRIO), i], isem.at[lax.rem(n, TRIO), i])
                for i in range(group)]

    def start_outs(n):
        for i in range(group):
            m = n * group + i
            p, t, sub = lax.div(m, PER_PIECE), lax.rem(half_of(m), N_TILE), odd(m)
            src, sem = cbuf.at[lax.rem(n, TRIO), i], csem.at[lax.rem(n, TRIO), i]
            for cond, copies in (
                (p < 3, lambda: to_input(wq_ref, lambda g: TRIO * g + p, t, sub, src, sem)),
                (p == KEY_PIECE, lambda: to_input(wk_ref, lambda g: g, t, sub, src, sem)),
                (p == KEY_PIECE + 1, lambda: to_input(wv_ref, lambda g: g, t, sub, src, sem)),
                ((p == O_PIECES[0]) | (p == O_PIECES[1]), lambda: to_output(p, t, sub, src, sem)),
            ):
                @pl.when(cond)
                def _(copies=copies):
                    for c in copies():
                        c.start()

    def wait_outs(n):
        for i in range(group):
            for c in to_output(IN_GATHER, 0, 0, cbuf.at[0, i], csem.at[lax.rem(n, TRIO), i]):
                c.wait()

    def weight(i):
        slot = odd(i)
        return pltpu.make_async_copy(w_ref.at[lanes(TRIO * i + 2), :], wbuf.at[slot], wsem.at[slot])

    for late in range(N_LATE):
        for sub in range(PAIR):
            start_all(piece_copies(g_ref, gbuf, gsem, IN_GATHER + late, sub, late * 2 + sub))
    operand(zero()).start()
    weight(zero()).start()
    acc[ALL] = sum_ref[ALL]
    dx_out[ALL] = dx_ref[ALL]
    dgain_out[ALL] = dgain_ref[ALL]

    def step(n, carry):
        t, late, sub = lax.div(n, PAIR * N_LATE), lax.rem(half_of(n), N_LATE), odd(n)
        p, held = IN_GATHER + late, late * 2 + sub
        slot = lax.rem(n, TRIO)

        @pl.when(n >= 3)
        def _():
            wait_outs(n - 3)
        for c in ins(n):
            c.start()

        @pl.when(n >= 1)
        def _():
            for c in ins(n - 1):
                c.wait()
            start_outs(n - 1)

        @pl.when(held == 0)
        def _():
            operand(t).wait()

            @pl.when(nxt(t) < N_TILE)
            def _():
                operand(nxt(t)).start()

        @pl.when(n < PAIR * N_LATE)
        def _():
            wait_piece(gbuf, gsem, held)

        @pl.when(n >= 3)
        def _():
            for c in to_output(IN_GATHER, 0, 0, obuf.at[0], osem.at[slot]):
                c.wait()
        @pl.when(n < 8)
        def _():
            weight(n).wait()

            @pl.when(n < 7)
            def _():
                weight(n + 1).start()
            acc[ALL] += jnp.dot(o_ref[:, lanes(n)], wbuf[odd(n)], preferred_element_type=F32)
        obuf[slot] = tile_product(abuf[odd(t)], gbuf[held], True)
        for c in to_output(p, t, sub, obuf.at[slot], osem.at[slot]):
            c.start()
        return carry

    loop(n_step, step, 0)
    y_ref[ALL] = acc[ALL].astype(BF16)
    for c in ins(n_step - 1):
        c.wait()
    start_outs(jnp.int32(n_step - 1))
    for n in range(n_step - 3, n_step):
        wait_outs(n)
        for c in to_output(IN_GATHER, 0, 0, obuf.at[0], osem.at[n % 3]):
            c.wait()


def finish(x, o, dx, dgain, w_o, hd, g, tiles):
    model, kv = hd.shape[2], 8 * LANES
    return pl.pallas_call(
        finish_kernel,
        out_shape=[like(x.shape, BF16), like(dx.shape, BF16), like(dgain.shape, F32)]
        + [like((model, n), F32) for n in (TRIO * kv, kv, kv)] + [like((TRIO * kv, model), F32)],
        in_specs=[vmem_spec()] * 4 + [any_spec()] * 4,
        out_specs=[vmem_spec()] * 3 + [any_spec()] * 4,
        scratch_shapes=[pltpu.VMEM((PAIR * N_LATE, SEQ, BLK), BF16), pltpu.VMEM((PAIR, SEQ, BLK), BF16), pltpu.VMEM((TRIO, BLK, BLK), F32),
                        pltpu.VMEM((TRIO, GROUP, BLK, BLK), F32), pltpu.VMEM(x.shape, F32), pltpu.VMEM((PAIR, LANES, model), BF16),
                        sems(PAIR * N_LATE), sems(PAIR), sems(TRIO, 4), sems(TRIO, GROUP), sems(TRIO, GROUP, 4), sems(PAIR)],
        cost_estimate=pl.CostEstimate(flops=4 * SEQ * kv * model, bytes_accessed=250 * 2**20, transcendentals=0),
        compiler_params=pltpu.CompilerParams(vmem_limit_bytes=VMEM_LIMIT),
    )(x, o, dx, dgain, w_o, hd, g, tiles)


def solution(mesh):
    assert mesh.shape['hp'] == 4 and mesh.shape['cp'] == 8

    def device_step(hidden, grad_out, positions, norm_gain, w_q, w_k, w_v, w_o, inv_freq):
        model = hidden.shape[1]
        hd, _, gathered, tiles, o_own, total, dx, gains = main(
            hidden, grad_out, norm_gain, positions, inv_freq, w_q, w_k, w_v, w_o)
        output, grad_hidden, grad_gain, grad_wq, grad_wk, grad_wv, grad_wo = finish(
            total, o_own, dx, gains, w_o, hd.reshape(2, SEQ, model), gathered, tiles)
        grad_gain = grad_gain.reshape(-1)
        return output, grad_hidden, grad_wq, grad_wk, grad_wv, grad_wo, grad_gain

    rows, whole = P(('cp', 'hp'), None), P()
    return jax.shard_map(
        device_step, mesh=mesh,
        in_specs=(rows, rows, P(('cp', 'hp')), whole, whole, whole, whole, whole, whole),
        out_specs=(rows, rows, whole, whole, whole, whole, whole), check_vma=False)
```
